256 devices in a mesh: leaf: 64 (over y, z, core), grid: 4 (over x).
Axes of the slice: x: 4, y: 4, z: 8, core: 2. Of those that a mesh axis runs over, the one named last changes fastest.
Arguments:
- source_leaf: float32 [8, 32768], P(None, ('leaf', 'grid')), may hold values from -6 to 6
- block_leaf: float32 [32768, 128], P(('leaf', 'grid')), may hold values from -0.5 to 0.5
- expand_leaf: float32 [32768, 128], P(('leaf', 'grid')), may hold values from -0.5 to 0.5
- basis_leaf: float32 [32768, 256], P(('leaf', 'grid')), may hold values from -0.25 to 0.25
- pivot_leaf: float32 [32768], P(('leaf', 'grid')), may hold values from -2 to 2
- couple_leaf: float32 [65536, 128], P(('leaf', 'grid')), may hold values from -0.5 to 0.5
- ranks_leaf: int32 [64, 2], replicated, may hold values from 32 to 128
- targets_leaf: int32 [65536], P(('leaf', 'grid')), may hold values from 0 to 16383, as said below
- source_middle: float32 [8, 32768], P(None, ('leaf', 'grid')), may hold values from -6 to 6
- block_middle: float32 [32768, 128], P(('leaf', 'grid')), may hold values from -0.5 to 0.5
- expand_middle: float32 [32768, 128], P(('leaf', 'grid')), may hold values from -0.5 to 0.5
- basis_middle: float32 [32768, 256], P(('leaf', 'grid')), may hold values from -0.0625 to 0.0625
- pivot_middle: float32 [32768], P(('leaf', 'grid')), may hold values from -2 to 2
- couple_middle: float32 [32768, 128], P(('leaf', 'grid')), may hold values from -0.5 to 0.5
- ranks_middle: int32 [4, 2], replicated, may hold values from 32 to 128
- targets_middle: int32 [32768], P(('leaf', 'grid')), may hold values from 0 to 32767, as said below
- source_upper: float32 [8, 32768], P(None, ('leaf', 'grid')), may hold values from -6 to 6
- block_upper: float32 [32768, 128], P(('leaf', 'grid')), may hold values from -0.5 to 0.5
- expand_upper: float32 [32768, 128], P(('leaf', 'grid')), may hold values from -0.5 to 0.5
- basis_upper: float32 [32768, 256], P(('leaf', 'grid')), may hold values from -0.046875 to 0.046875
- pivot_upper: float32 [32768], P(('leaf', 'grid')), may hold values from -2 to 2
- couple_upper: float32 [32768, 128], P(('leaf', 'grid')), may hold values from -0.5 to 0.5
- ranks_upper: int32 [2, 2], replicated, may hold values from 32 to 128
- targets_upper: int32 [32768], P(('leaf', 'grid')), may hold values from 0 to 32767, as said below
- source_root: float32 [8, 32768], P(None, ('leaf', 'grid')), may hold values from -6 to 6
- block_root: float32 [32768, 128], P(('leaf', 'grid')), may hold values from -0.5 to 0.5
- expand_root: float32 [32768, 128], P(('leaf', 'grid')), may hold values from -0.5 to 0.5
- basis_root: float32 [32768, 256], P(('leaf', 'grid')), may hold values from -0.03125 to 0.03125
- pivot_root: float32 [32768], P(('leaf', 'grid')), may hold values from -2 to 2
- ranks_root: int32 [1, 2], replicated, may hold values from 32 to 128
Outputs:
- answer_leaf: float32 [8, 32768], P(None, ('leaf', 'grid'))
- answer_middle: float32 [8, 32768], P(None, ('leaf', 'grid'))
- answer_upper: float32 [8, 32768], P(None, ('leaf', 'grid'))
- answer_root: float32 [8, 32768], P(None, ('leaf', 'grid'))
The draws below stay inside these ranges and needn't reach their ends.
Inputs may be any that keep to these rules, and one draw needn't show every extreme that they name: `targets_leaf`: within one leaf front the 1024 entries are distinct; each names a row of the parent front's row vector of 16384 rows. Split that vector's separator part and its update part each evenly, in order, over the parent's devices (leaf then grid); then the rows of one device name at most 4 rows held by any one of them, and exactly that many for some. `targets_middle`: within one middle front the entries are distinct; each names a row of the parent front's row vector of 32768 rows. Split likewise over the parent's devices, the rows of one device name at most 1 row held by any one of them, and exactly that many for some. `targets_upper`: within one upper front the entries are distinct; each names a row of the root separator. Split evenly in order over all devices, the rows of one device name at most 1 row held by any one of them, and exactly that many for some.
All inputs are finite; a program needn't handle non-finite values.
Results may differ from the reference program's by a relative error of at most 0.0003.
Values sent between devices are 32-bit elements; how exact they have to be, the bound alone decides.
A program may use at most 128 MiB of HBM per device.

```python
import jax
import jax.numpy as jnp
from jax import lax

RHS_COUNT = 8
BLOCK = 128
RANK = 128
TOP_ROWS = 128
SEP_LEAF = 512
UPD_LEAF = 1024
SEP_MID = 8192
SEP_UP = 16384
SEP_ROOT = 32768
N_LEAF = 64
N_GRID = 4


def pick_rows(key, salt, fronts, count, owners, width, pieces, sep_rows):
    base = jax.random.fold_in(key, salt)
    slots_each = pieces * width

    def one_front(front):
        fkey = jax.random.fold_in(base, front)
        order = jax.random.permutation(jax.random.fold_in(fkey, 1), owners)
        slot_keys = jax.vmap(lambda owner: jax.random.fold_in(jax.random.fold_in(fkey, 2), owner))(jnp.arange(owners, dtype=jnp.int32))
        slot_order = jax.vmap(lambda one: jax.random.permutation(one, slots_each))(slot_keys)
        rows = jnp.arange(count, dtype=jnp.int32)
        owner = order[rows % owners]
        slot = slot_order[owner, rows // owners]
        return slot // width * sep_rows + owner * width + slot % width
    picked = jax.vmap(one_front)(jnp.arange(fronts, dtype=jnp.int32))
    return picked.reshape(-1).astype(jnp.int32)


def draw_targets_leaf(key, part):
    return pick_rows(key, 11, N_LEAF, UPD_LEAF, N_LEAF * N_GRID // 4, TOP_ROWS, 2, SEP_MID)


def draw_targets_middle(key, part):
    return pick_rows(key, 12, 4, SEP_MID, N_LEAF * N_GRID // 2, TOP_ROWS, 2, SEP_UP)


def draw_targets_upper(key, part):
    return pick_rows(key, 13, 2, SEP_UP, N_LEAF * N_GRID, TOP_ROWS, 1, SEP_ROOT)


def set_ends(array, own_key, low, top_value):
    longest = array.shape.index(max(array.shape))
    spots = []
    for shift in (0, 1):
        where = [jax.random.randint(jax.random.fold_in(own_key, axis), (), 0, length) for axis, length in enumerate(array.shape)]
        where[longest] = (where[longest] + shift) % array.shape[longest]
        spots.append(tuple(where))
    return array.at[spots[0]].set(low).at[spots[1]].set(top_value)


def level_of(rng, dims, shards, least, high):
    def one(position, blocks):
        heights = jax.random.uniform(jax.random.fold_in(jax.random.fold_in(rng, 6), position), (blocks,), jnp.float32, least / len(shards), high / len(shards))
        return jnp.repeat(jnp.exp(heights), dims[position] // blocks).reshape((-1,) + (1,) * (len(dims) - position - 1))

    factor_of = one(*shards[0])
    for cut in shards[1:]:
        factor_of = factor_of * one(*cut)
    return factor_of


def centred(key, dims, scale, limit, shards=(), held_as=jnp.bfloat16):
    factor_of = level_of(key, dims, shards, -0.22, 0.18) if shards else 1.0
    values = jax.random.normal(key, dims, jnp.float32) * scale * factor_of
    return jnp.minimum(jnp.maximum(values, -limit), limit).astype(held_as)


def setup_inputs(seed: int = 0) -> dict:
    key_list = jax.random.split(jax.random.key(seed), 31)
    return {
        "source_leaf": centred(key_list[0], (RHS_COUNT, N_LEAF * SEP_LEAF), 1.0, 6.0, ((1, 256),), jnp.float32),
        "block_leaf": centred(key_list[1], (N_LEAF * SEP_LEAF, BLOCK), BLOCK ** -0.5, 0.5, ((0, 256),), jnp.float32),
        "expand_leaf": centred(key_list[2], (N_LEAF * SEP_LEAF, RANK), RANK ** -0.5, 0.5, ((0, 256),), jnp.float32),
        "basis_leaf": centred(key_list[3], (N_LEAF * SEP_LEAF, 2 * RANK), SEP_LEAF ** -0.5, 0.25, ((0, 256),), jnp.float32),
        "pivot_leaf": jnp.clip(jax.random.uniform(key_list[4], (N_LEAF * SEP_LEAF,), jnp.float32, -2.0, 2.0) * level_of(key_list[4], (N_LEAF * SEP_LEAF,), ((0, 256),), -0.4, 0.0), -2.0, 2.0),
        "couple_leaf": centred(key_list[5], (N_LEAF * UPD_LEAF, RANK), RANK ** -0.5, 0.5, ((0, 256),), jnp.float32),
        "ranks_leaf": set_ends(jax.random.randint(key_list[6], (N_LEAF, 2), RANK // 4, RANK + 1), jax.random.fold_in(key_list[6], 1), RANK // 4, RANK).astype(jnp.int32),
        "targets_leaf": draw_targets_leaf(jax.random.fold_in(key_list[30], 71), 0),
        "source_middle": centred(key_list[8], (RHS_COUNT, 4 * SEP_MID), 1.0, 6.0, ((1, 256),), jnp.float32),
        "block_middle": centred(key_list[9], (4 * SEP_MID, BLOCK), BLOCK ** -0.5, 0.5, ((0, 256),), jnp.float32),
        "expand_middle": centred(key_list[10], (4 * SEP_MID, RANK), RANK ** -0.5, 0.5, ((0, 256),), jnp.float32),
        "basis_middle": centred(key_list[11], (4 * SEP_MID, 2 * RANK), SEP_MID ** -0.5, 0.0625, ((0, 256),), jnp.float32),
        "pivot_middle": jnp.clip(jax.random.uniform(key_list[12], (4 * SEP_MID,), jnp.float32, -2.0, 2.0) * level_of(key_list[12], (4 * SEP_MID,), ((0, 256),), -0.4, 0.0), -2.0, 2.0),
        "couple_middle": centred(key_list[13], (4 * SEP_MID, RANK), RANK ** -0.5, 0.5, ((0, 256),), jnp.float32),
        "ranks_middle": set_ends(jax.random.randint(key_list[14], (4, 2), RANK // 4, RANK + 1), jax.random.fold_in(key_list[14], 1), RANK // 4, RANK).astype(jnp.int32),
        "targets_middle": draw_targets_middle(jax.random.fold_in(key_list[30], 71), 0),
        "source_upper": centred(key_list[16], (RHS_COUNT, 2 * SEP_UP), 1.0, 6.0, ((1, 256),), jnp.float32),
        "block_upper": centred(key_list[17], (2 * SEP_UP, BLOCK), BLOCK ** -0.5, 0.5, ((0, 256),), jnp.float32),
        "expand_upper": centred(key_list[18], (2 * SEP_UP, RANK), RANK ** -0.5, 0.5, ((0, 256),), jnp.float32),
        "basis_upper": centred(key_list[19], (2 * SEP_UP, 2 * RANK), SEP_UP ** -0.5, 0.046875, ((0, 256),), jnp.float32),
        "pivot_upper": jnp.clip(jax.random.uniform(key_list[20], (2 * SEP_UP,), jnp.float32, -2.0, 2.0) * level_of(key_list[20], (2 * SEP_UP,), ((0, 256),), -0.4, 0.0), -2.0, 2.0),
        "couple_upper": centred(key_list[21], (2 * SEP_UP, RANK), RANK ** -0.5, 0.5, ((0, 256),), jnp.float32),
        "ranks_upper": set_ends(jax.random.randint(key_list[22], (2, 2), RANK // 4, RANK + 1), jax.random.fold_in(key_list[22], 1), RANK // 4, RANK).astype(jnp.int32),
        "targets_upper": draw_targets_upper(jax.random.fold_in(key_list[30], 71), 0),
        "source_root": centred(key_list[24], (RHS_COUNT, SEP_ROOT), 1.0, 6.0, ((1, 256),), jnp.float32),
        "block_root": centred(key_list[25], (SEP_ROOT, BLOCK), BLOCK ** -0.5, 0.5, ((0, 256),), jnp.float32),
        "expand_root": centred(key_list[26], (SEP_ROOT, RANK), RANK ** -0.5, 0.5, ((0, 256),), jnp.float32),
        "basis_root": centred(key_list[27], (SEP_ROOT, 2 * RANK), SEP_ROOT ** -0.5, 0.03125, ((0, 256),), jnp.float32),
        "pivot_root": jnp.clip(jax.random.uniform(key_list[28], (SEP_ROOT,), jnp.float32, -2.0, 2.0) * level_of(key_list[28], (SEP_ROOT,), ((0, 256),), -0.4, 0.0), -2.0, 2.0),
        "ranks_root": jax.random.randint(key_list[29], (1, 2), RANK // 4, RANK + 1).astype(jnp.int32),
    }


HIGH_PRECISION = lax.Precision.HIGHEST


def make_masks(ranks):
    cols = jnp.arange(RANK, dtype=jnp.int32)
    head_mask_grid = (cols[None, :] < ranks[:, 0:1]).astype(jnp.float32)[:, None, :]
    column_mask_grid = (cols[None, :] < ranks[:, 1:2]).astype(jnp.float32)[:, None, :]
    return head_mask_grid, column_mask_grid


def forward(source, inc_sep, block, expand, basis, pivot, ranks, fronts):
    width = source.shape[1] // fronts
    level_batch_index = source.reshape(RHS_COUNT, fronts, width).transpose(1, 0, 2)
    if inc_sep is not None:
        level_batch_index = level_batch_index + inc_sep
    tiles = block.reshape(fronts, width // BLOCK, BLOCK, BLOCK)
    local_portion = jnp.einsum("fanh,fnhk->fank", level_batch_index.reshape(fronts, RHS_COUNT, width // BLOCK, BLOCK), tiles, precision=HIGH_PRECISION).reshape(fronts, RHS_COUNT, width)
    gens = basis.reshape(fronts, width, 2 * RANK)
    query_lookup = gens[:, :, :RANK]
    coupling_right_factor = gens[:, :, RANK:]
    spread_across_rows = expand.reshape(fronts, width, RANK)
    head_mask_grid, column_mask_grid = make_masks(ranks)
    hidden_query_rows = jnp.einsum("mle,meq->mlq", level_batch_index, query_lookup, precision=HIGH_PRECISION) * head_mask_grid
    intermediate_entries = local_portion + jnp.einsum("gdk,gtk->gdt", hidden_query_rows, spread_across_rows, precision=HIGH_PRECISION)
    weight_entries = jnp.einsum("mle,meq->mlq", intermediate_entries, coupling_right_factor, precision=HIGH_PRECISION) * column_mask_grid
    correction_entries = intermediate_entries * pivot.reshape(fronts, 1, width)
    return correction_entries, weight_entries, (tiles, query_lookup, coupling_right_factor, spread_across_rows, head_mask_grid, column_mask_grid)


def flat_index(targets, fronts, parents, total):
    count = targets.shape[0] // fronts
    owner = jnp.arange(fronts, dtype=jnp.int32) // (fronts // parents)
    return (owner[:, None] * total + targets.reshape(fronts, count).astype(jnp.int32)).reshape(-1)


def scatter_up(update, targets, fronts, parents, sep_par, upd_par):
    total = sep_par + upd_par
    flat = flat_index(targets, fronts, parents, total)
    values = update.transpose(1, 0, 2).reshape(RHS_COUNT, -1)
    buffer = jnp.zeros((RHS_COUNT, parents * total), jnp.float32).at[:, flat].add(values)
    buffer = buffer.reshape(RHS_COUNT, parents, total).transpose(1, 0, 2)
    return buffer[:, :, :sep_par], buffer[:, :, sep_par:]


def pull_down(front_rows, targets, fronts, parents):
    total = front_rows.shape[2]
    flat = flat_index(targets, fronts, parents, total)
    whole = front_rows.transpose(1, 0, 2).reshape(RHS_COUNT, parents * total)
    values = jnp.take(whole, flat, axis=1)
    return values.reshape(RHS_COUNT, fronts, -1).transpose(1, 0, 2)


def backward(correction_entries, x_upd, couple, parts, fronts):
    tiles, query_lookup, coupling_right_factor, spread_across_rows, head_mask_grid, column_mask_grid = parts
    width = correction_entries.shape[2]
    remainder_rows = correction_entries
    if x_upd is not None:
        couple_u = couple.reshape(fronts, -1, RANK)
        solve_direction = jnp.einsum("fau,fur->far", x_upd, couple_u, precision=HIGH_PRECISION) * column_mask_grid
        remainder_rows = correction_entries - jnp.einsum("gdk,gtk->gdt", solve_direction, coupling_right_factor, precision=HIGH_PRECISION)
    right_projection = jnp.einsum("mle,meq->mlq", remainder_rows, spread_across_rows, precision=HIGH_PRECISION) * head_mask_grid
    local_portion = jnp.einsum("fanh,fnkh->fank", remainder_rows.reshape(fronts, RHS_COUNT, width // BLOCK, BLOCK), tiles, precision=HIGH_PRECISION).reshape(fronts, RHS_COUNT, width)
    return local_portion + jnp.einsum("gdk,gtk->gdt", right_projection, query_lookup, precision=HIGH_PRECISION)


def reference(source_leaf, block_leaf, expand_leaf, basis_leaf, pivot_leaf, couple_leaf, ranks_leaf, targets_leaf,
              source_middle, block_middle, expand_middle, basis_middle, pivot_middle, couple_middle, ranks_middle, targets_middle,
              source_upper, block_upper, expand_upper, basis_upper, pivot_upper, couple_upper, ranks_upper, targets_upper,
              source_root, block_root, expand_root, basis_root, pivot_root, ranks_root):
    levels = [
        (source_leaf, block_leaf, expand_leaf, basis_leaf, pivot_leaf, couple_leaf, ranks_leaf, targets_leaf),
        (source_middle, block_middle, expand_middle, basis_middle, pivot_middle, couple_middle, ranks_middle, targets_middle),
        (source_upper, block_upper, expand_upper, basis_upper, pivot_upper, couple_upper, ranks_upper, targets_upper),
        (source_root, block_root, expand_root, basis_root, pivot_root, None, ranks_root, None),
    ]
    fronts = [N_LEAF, 4, 2, 1]
    inc_sep = None
    inc_upd = None
    saved = []
    for level in range(4):
        source, block, expand, basis, pivot, couple, ranks, targets = levels[level]
        correction_entries, weight_entries, parts = forward(source, inc_sep, block, expand, basis, pivot, ranks, fronts[level])
        saved.append((correction_entries, parts))
        if level < 3:
            couple_u = couple.reshape(fronts[level], -1, RANK)
            update = -jnp.einsum("far,fur->fau", weight_entries, couple_u, precision=HIGH_PRECISION)
            if inc_upd is not None:
                update = update + inc_upd
            sep_par = levels[level + 1][0].shape[1] // fronts[level + 1]
            upd_par = 0
            if level + 1 < 3:
                upd_par = levels[level + 1][5].shape[0] // fronts[level + 1]
            inc_sep, inc_upd = scatter_up(update, targets, fronts[level], fronts[level + 1], sep_par, upd_par)
            if upd_par == 0:
                inc_upd = None
    answers = [None, None, None, None]
    rows_par = None
    for level in (3, 2, 1, 0):
        correction_entries, parts = saved[level]
        couple = levels[level][5]
        targets = levels[level][7]
        x_upd = None
        if level < 3:
            x_upd = pull_down(rows_par, targets, fronts[level], fronts[level + 1])
        xvals = backward(correction_entries, x_upd, couple, parts, fronts[level])
        answers[level] = xvals.transpose(1, 0, 2).reshape(RHS_COUNT, -1)
        rows_par = xvals if x_upd is None else jnp.concatenate([xvals, x_upd], axis=2)
    return (answers[0], answers[1], answers[2], answers[3])
```

```python
import functools

import jax
import jax.numpy as jnp
from jax import lax
from jax.experimental import pallas as pl
from jax.experimental.pallas import tpu as pltpu
from jax.sharding import PartitionSpec as P

RANK = 128
LANES = 128
NEAR = 8
MESH = pl.DeviceIdType.MESH
F32 = jnp.float32
BF16 = jnp.bfloat16


def once(a, b, ca, cb):
    return lax.dot_general(a, b, (((ca,), (cb,)), ((), ())), preferred_element_type=F32)


def halves(x):
    hi = x.astype(BF16)
    return hi, (x - hi.astype(F32)).astype(BF16)


def stacked(x):
    hi = x.astype(BF16).astype(F32)
    return jnp.concatenate([hi, x - hi], axis=0).astype(BF16)


def times(a, b, cb):
    bh, bl = b
    n = a.shape[0]
    both = once(stacked(a), bh, 1, cb)
    return both[:n] + (both[n:] + once(a.astype(BF16), bl, 1, cb))


def mult(a, b):
    return times(a, halves(b), 0)


def outer(a, b):
    return times(a, halves(b), 1)


def inner(a, b):
    ah, al = halves(a)
    bh, bl = halves(b)
    return once(ah, bh, 0, 0) + (once(al, bh, 0, 0) + once(ah, bl, 0, 0))


def pick(x, onehot):
    n = x.shape[0]
    both = once(stacked(x), onehot, 1, 1)
    return both[:n] + both[n:]


def spread(rows, onehot, groups, count):
    m = groups * count
    wide = onehot.shape[1] // groups
    both = once(stacked(rows.T[:m]), onehot, 1, 0)
    out = None
    for g in range(groups):
        lanes = slice(g * wide, (g + 1) * wide)
        part = both[g * count : (g + 1) * count, lanes] + both[m + g * count : m + (g + 1) * count, lanes]
        out = part if out is None else out + part
    return out


def diagonal(x, groups):
    count, wide = x.shape
    zero = jnp.zeros((count, wide), F32)
    rows = [
        jnp.concatenate([x if h == g else zero for h in range(groups)], axis=1) for g in range(groups)
    ]
    rows.append(jnp.zeros((LANES - groups * count, groups * wide), F32))
    return jnp.concatenate(rows, axis=0)


def kernel(cfg, names, *refs):
    leaves, across, size, ups, count, cap = cfg
    total_devices = leaves * across
    (src, blk, exp, bas, piv, rnk) = [refs[4 * i : 4 * i + 4] for i in range(6)]
    cpl = refs[24:27]
    tgt = refs[27:30]
    outs = refs[30:34]
    m = dict(zip(names, refs[34:-3]))
    send_sem, recv_sem, ready = refs[-3:]
    sems = {}
    parts = {}

    me = lax.axis_index("leaf") * across + lax.axis_index("grid")
    near = me % NEAR
    far = me // NEAR
    nb = [s // NEAR for s in size]
    plane = size[1]
    fars = nb[3]

    def where(peer):
        return (peer // across, peer % across)

    def sem_of(name):
        return sems.setdefault(name, len(sems))

    def remote(a, b, sem, peer):
        return pltpu.make_async_remote_copy(
            src_ref=a,
            dst_ref=b,
            send_sem=send_sem.at[sem],
            recv_sem=recv_sem.at[sem],
            device_id=where(peer),
            device_id_type=MESH,
        )

    def wait_for(part, sem):
        pltpu.make_async_copy(part, part, sem).wait()

    def fan(group, stride, *sets):
        idx = me // stride % group
        base = me - idx * stride
        for name, source, dest, part in sets:
            sem_of(name)
            parts[name] = part

        def body(k, carry):
            q = (idx + k) % group
            for name, source, dest, part in sets:
                remote(source(q), dest(idx), sem_of(name), base + q * stride).start()
            return carry

        lax.fori_loop(1, group, body, 0)

    def arrive(name):
        wait_for(parts[name], recv_sem.at[sem_of(name)])

    def slots(name, group):
        buf = m[name]
        return buf.at[pl.ds(0, group - 1)]

    def spread_own(name, group, stride):
        buf = m[name]
        idx = me // stride % group
        fan(group, stride, (name, lambda q: buf.at[idx], lambda i: buf.at[i], slots(name, group)))

    barrier = pltpu.get_barrier_semaphore()

    def greet_near(sem):
        def body(k, carry):
            peer = far * NEAR + (near + k) % NEAR
            pl.semaphore_signal(sem, inc=1, device_id=where(peer), device_id_type=MESH)
            return carry

        lax.fori_loop(1, NEAR, body, 0)

    def greet_far(k, carry):
        peer = (far + k) % fars * NEAR + near
        pl.semaphore_signal(barrier, inc=1, device_id=where(peer), device_id_type=MESH)
        return carry

    lax.fori_loop(1, fars, greet_far, 0)
    greet_near(barrier)

    col = lax.broadcasted_iota(jnp.int32, (count, RANK), 1)

    def mask(level, which):
        def of(front):
            rank = rnk[level][which, front] if level < 3 else rnk[level][0, which]
            return (col < rank).astype(F32)

        return of

    front = [me // s for s in size]
    head = [mask(level, 0)(front[level]) for level in range(4)]
    side = [mask(level, 1)(front[level]) for level in range(3)]

    def q_of(level):
        return bas[level][:, :RANK]

    def v_of(level):
        return bas[level][:, RANK:]

    def tiles_of(level):
        n = nb[level + 1]
        return NEAR * n // LANES, LANES // n

    four = size[0]
    my4 = me % four
    s0 = src[0][...]
    local0 = mult(s0, blk[0][...])
    m["f1"][my4] = jnp.concatenate([mult(s0, q_of(0)), mult(local0, v_of(0))], axis=0)
    m["c0"][my4] = inner(exp[0][...], v_of(0))

    slice_rows = RANK // NEAR
    root_piv = jnp.broadcast_to(piv[3][...], (LANES, LANES)).T
    crosses = [
        inner(exp[1][...], v_of(1)),
        inner(exp[2][...], v_of(2)),
        inner(exp[3][...] * root_piv, exp[3][...]),
    ]
    for j, cross in enumerate(crosses):
        m["xp"][:, j * slice_rows : (j + 1) * slice_rows, :] = cross.reshape(NEAR, slice_rows, RANK)

    def split_targets(level):
        sep = size[level + 1] * LANES
        t = tgt[level][...]
        upd = t >= sep
        rel = jnp.where(upd, t - sep, t)
        return rel // LANES, rel % LANES + jnp.where(upd, LANES, 0)

    def pack_leaf():
        u = ups[0]
        dst, low = split_targets(0)
        ri = lax.broadcasted_iota(jnp.int32, (u, u), 0)
        ci = lax.broadcasted_iota(jnp.int32, (u, u), 1)
        dst_f = dst.astype(F32)
        dst_c = jnp.sum(jnp.where(ri == ci, jnp.broadcast_to(dst_f, (u, u)), 0.0), axis=1, keepdims=True)
        rank = jnp.sum(
            jnp.where((dst_c == dst_f) & (ri < ci), 1.0, 0.0), axis=0, keepdims=True
        ).astype(jnp.int32)
        slot = rank * plane + dst
        ch, cl = halves(cpl[0][...])
        lowmat = None
        li = lax.broadcasted_iota(jnp.int32, (LANES, u), 0)
        for s in range(cap):
            si = lax.broadcasted_iota(jnp.int32, (plane, u), 0) + s * plane
            hit = (si == slot).astype(F32).astype(BF16)
            lanes = slice(s * RANK, (s + 1) * RANK)
            m["hch"][:, lanes] = once(hit, ch, 1, 0).astype(BF16)
            m["hcl"][:, lanes] = once(hit, cl, 1, 0).astype(BF16)
            mine = jnp.where(li == cap * count + s, low.astype(F32), 0.0).astype(BF16)
            part = once(hit, mine, 1, 1)
            lowmat = part if lowmat is None else lowmat + part
        m["low0"][...] = lowmat

    def pack_couple(level):
        n = nb[level + 1]
        dst, low = split_targets(level)
        slot = dst % NEAR * n + dst // NEAR
        si = lax.broadcasted_iota(jnp.int32, (NEAR * n, LANES), 0)
        h = (si == slot).astype(F32).astype(BF16)
        m["h", level][...] = h
        hi, lo = [once(h, piece, 1, 0) for piece in halves(cpl[level][...])]
        m["pa", level][...] = (hi + lo).reshape(NEAR, n, RANK)
        rows = jnp.broadcast_to(low, (count, LANES)).astype(F32).astype(BF16)
        bi = lax.broadcasted_iota(jnp.int32, (n, LANES), 0) * NEAR
        m["ohr", level][...] = jnp.concatenate(
            [(bi + k == dst).astype(F32) for k in range(NEAR)], axis=1
        ).astype(BF16)
        return once(rows, h, 1, 1)

    low1, low2 = pack_couple(1), pack_couple(2)
    ri = lax.broadcasted_iota(jnp.int32, (count, LANES), 0)
    for t in range(2):
        two = low2[:, t * LANES : (t + 1) * LANES]
        m["lows"][t] = jnp.where(ri == 0, two, jnp.where(ri == 1, low1, 0.0))
    pack_leaf()

    pl.semaphore_wait(barrier, NEAR - 1 + fars - 1)
    greet_near(ready)
    spread_own("f1", four, 1)
    spread_own("c0", four, 1)

    def fan_near(name, source, dest):
        fan(NEAR, 1, (name, source, lambda i: dest.at[i], dest.at[pl.ds(0, NEAR - 1)]))

    m["xra"][near] = m["xp"][near]
    fan_near("xra", lambda q: m["xp"].at[q], m["xra"])
    m["la"][near] = m["lows"][near // 4]
    fan_near("la", lambda q: m["lows"].at[q // 4], m["la"])
    for level in (1, 2):
        pa, ra = m["pa", level], m["ra", level]
        ra[near] = pa[near]
        fan_near(("ra", level), lambda q, pa=pa: pa.at[q], ra)

    def keep(name, value):
        hi, lo = halves(value)
        m[name, "h"][...] = hi
        m[name, "l"][...] = lo

    def kept(name):
        return m[name, "h"][...], m[name, "l"][...]

    for level in (1, 2):
        wv = mult(blk[level][...], v_of(level))
        keep(("qw", level), jnp.concatenate([q_of(level), wv], axis=1))
    wpp = mult(blk[3][...] * piv[3][...], exp[3][...])
    keep(("qw", 3), jnp.concatenate([q_of(3), wpp], axis=1))

    arrive("f1")
    arrive("c0")
    cross0 = jnp.sum(m["c0"][...], axis=0)
    tot = jnp.sum(m["f1"][...], axis=0)
    hq0 = tot[:count] * head[0]
    keep(("cross", 0), cross0)
    w0 = (tot[count:] + times(hq0, kept(("cross", 0)), 0)) * side[0]

    def leaf_rows(a, b):
        ah, al = a
        bh, bl = halves(b)
        out = once(ah, bh, 1, 1) + once(ah, bl, 1, 1)
        return out if al is None else out + once(al, bh, 1, 1)

    place = me % plane

    def send_leaf(rows, got, name):
        m[got][pl.ds(place, 1), :] = m[rows][pl.ds(place, 1), :]
        fan(
            plane,
            1,
            (
                name,
                lambda q: m[rows].at[pl.ds(q, 1)],
                lambda i: m[got].at[pl.ds(i, 1)],
                m[got].at[pl.ds(0, plane - 1)],
            ),
        )

    hc = (m["hch"][...], m["hcl"][...])
    m["s0"][...] = leaf_rows(hc, diagonal(-w0, cap)) + m["low0"][...]
    pl.semaphore_wait(ready, NEAR - 1)
    send_leaf("s0", "r0", "r0")

    z0 = (local0 + outer(hq0, exp[0][...])) * piv[0][...]
    m["zx"][my4] = mult(z0, exp[0][...])
    spread_own("zx", four, 1)

    def store_row(buf, i, row):
        buf[pl.ds(i, 1), :] = row

    def forward_rows(level, table, got, name):
        n = nb[level + 1]
        per = tiles_of(level)[1]
        idx = far % n
        first = near % per * n
        store_row(m[got], idx, m[table][pl.ds(first + idx, 1), :])
        return (
            name,
            lambda q: m[table].at[pl.ds(first + q, 1)],
            lambda i: m[got].at[pl.ds(i, 1)],
            m[got].at[pl.ds(0, n - 1)],
        )

    def transposed(x):
        return jnp.concatenate([x, jnp.zeros((LANES - x.shape[0], LANES), F32)], axis=0).T

    def couple_set(level):
        n = nb[level + 1]
        ra, rb = m["ra", level], m["rb", level]
        idx = far % n
        rb[:, pl.ds(idx, 1), :] = ra[:, pl.ds(idx, 1), :]
        return (
            ("rb", level),
            lambda q: ra.at[:, pl.ds(q, 1)],
            lambda i: rb.at[:, pl.ds(i, 1)],
            rb.at[:, pl.ds(0, n - 1)],
        )

    arrive("xra")
    sums = jnp.sum(m["xra"][...], axis=0)
    for j, n in enumerate((nb[1], nb[2], nb[3])):
        m["xb", j][far % n] = sums[j * slice_rows : (j + 1) * slice_rows]
    spread_own(("xb", 0), nb[1], NEAR)
    arrive("la")
    m["tl"][...] = transposed(m["la"][...].reshape(NEAR * count, LANES))
    for level in (1, 2):
        arrive(("ra", level))
        fan(nb[level + 1], NEAR, forward_rows(level, "tl", ("lb", level), ("lb", level)), couple_set(level))
        spread_own(("xb", level), nb[level + 1], NEAR)

    def build(level):
        n = nb[level + 1]
        wide = 2 * LANES if level == 1 else LANES
        arrive(("lb", level))
        lb = m["lb", level][...]
        lane = lax.broadcasted_iota(jnp.int32, (n, wide), 1).astype(F32)
        at = 2 - level
        hits = [(lane == lb[:, k * count + at : k * count + at + 1]).astype(F32) for k in range(NEAR)]
        m["ohf", level][...] = jnp.concatenate(hits, axis=1).astype(BF16)
        m["ohg", level][...] = jnp.concatenate(hits, axis=0).astype(BF16)
        arrive(("rb", level))
        half = n // 2
        for child in range(2):
            rows = slice(child * half, (child + 1) * half)
            got = m["rb", level][:, rows, :].reshape(NEAR * half, RANK)
            hot = jnp.concatenate([hit[rows] for hit in hits], axis=0).astype(BF16)
            hi, lo = [once(piece, hot, 0, 0) for piece in halves(got)]
            gh, gl = halves(hi + lo)
            out = slice(child * RANK, (child + 1) * RANK)
            m[("g", level), "h"][out, :] = gh
            m[("g", level), "l"][out, :] = gl

    def send_up(level, b, u):
        count_tiles, per = tiles_of(level)
        both = times(b, kept(("qw", level)), 0)
        tile = pick(u, m["h", level][...])
        for t in range(count_tiles):
            m["fs", level][t] = jnp.concatenate(
                [both[:, :RANK], both[:, RANK:], tile[:, t * LANES : (t + 1) * LANES]], axis=0
            )
        fs, fa = m["fs", level], m["fa", level]
        fa[near] = fs[near // per]
        fan_near(("fa", level), lambda q: fs.at[q // per], fa)

    def send_on(level):
        n = nb[level + 1]
        arrive(("fa", level))
        fa = m["fa", level]
        tot = jnp.sum(fa[:, : 2 * count, :], axis=0)
        hq = tot[:count] * head[level]
        w = tot[count:] + times(hq, kept(("cross", level)), 0)
        idx = far % n
        wb = m["wb", level]
        wb[idx] = w
        m["tf", level][...] = transposed(fa[:, 2 * count :, :].reshape(NEAR * count, LANES))
        fan(
            n,
            NEAR,
            (("wb", level), lambda q: wb.at[idx], lambda i: wb.at[i], wb.at[pl.ds(0, n - 1)]),
            forward_rows(level, ("tf", level), ("rf", level), ("rf", level)),
        )
        m["hb", level][far % nb[level]] = hq
        spread_own(("hb", level), nb[level], NEAR)

    def receive_up(level):
        n = nb[level + 1]
        half = n // 2
        arrive(("wb", level))
        wb = m["wb", level]
        ws = []
        for child in range(2):
            mc = mask(level, 1)(front[level + 1] * 2 + child)
            ws.append(jnp.sum(wb[child * half : (child + 1) * half], axis=0) * mc)
        inc = -times(jnp.concatenate(ws, axis=1), kept(("g", level)), 0)
        arrive(("rf", level))
        return inc + spread(m["rf", level][...], m["ohf", level][...], NEAR, count)

    def near_sum(name):
        arrive(name)
        return jnp.sum(m[name][...], axis=0)

    saved = {}

    def solve_front(level, local):
        arrive(("hb", level))
        hq = jnp.sum(m["hb", level][...], axis=0)
        z = (local + outer(hq, exp[level][...])) * piv[level][...]
        saved[level] = z
        m["za", level][near] = mult(z, exp[level][...])
        spread_own(("za", level), NEAR, 1)

    def pass_zp(level):
        m["zb", level][far % nb[level]] = near_sum(("za", level))
        spread_own(("zb", level), nb[level], NEAR)

    def base_of(level, zp):
        return outer(saved[level], blk[level][...]) + outer(zp * head[level], q_of(level))

    def tail_of(level, wv):
        qm = q_of(level) * jnp.broadcast_to(head[level][:1], (LANES, RANK))
        keep(("t", level), wv + times(qm, kept(("cross", level)), 0))

    def wv_of(level):
        qh, ql = kept(("qw", level))
        return qh[:, RANK:].astype(F32) + ql[:, RANK:].astype(F32)

    arrive("r0")
    r0 = m["r0"][...]
    lane = lax.broadcasted_iota(jnp.int32, (plane, 2 * LANES), 1).astype(F32)
    at = cap * count
    m["oh0"][...] = jnp.concatenate(
        [(lane == r0[:, at + s : at + s + 1]).astype(F32) for s in range(cap)], axis=1
    ).astype(BF16)
    inc = spread(r0, m["oh0"][...], cap, count)
    b1 = src[1][...] + inc[:, :LANES]
    send_up(1, b1, inc[:, LANES:])

    arrive(("xb", 0))
    m["xg1"][near] = jnp.sum(m["xb", 0][...], axis=0)
    spread_own("xg1", NEAR, 1)
    local1 = mult(b1, blk[1][...])
    saved[0] = z0
    arrive("zx")
    base0 = base_of(0, jnp.sum(m["zx"][...], axis=0))
    build(1)
    arrive("xg1")
    keep(("cross", 1), m["xg1"][...].reshape(RANK, RANK))
    send_on(1)

    arrive(("xb", 1))
    arrive(("xb", 2))
    m["xg2"][near] = jnp.concatenate([jnp.sum(m["xb", j][...], axis=0) for j in (1, 2)], axis=0)
    spread_own("xg2", NEAR, 1)
    tail_of(0, mult(blk[0][...], v_of(0)))
    tail_of(1, wv_of(1))

    inc = receive_up(1)
    b2 = src[2][...] + inc[:, :LANES]
    send_up(2, b2, inc[:, LANES:])

    local2 = mult(b2, blk[2][...])
    arrive("xg2")
    keep(("cross", 2), m["xg2"][:, :slice_rows, :].reshape(RANK, RANK))
    keep(("cross", 3), m["xg2"][:, slice_rows:, :].reshape(RANK, RANK))
    build(2)
    send_on(2)
    solve_front(1, local1)
    tail_of(2, wv_of(2))

    b3 = src[3][...] + receive_up(2)
    both = times(b3, kept(("qw", 3)), 0)
    m["fa", 3][near] = jnp.concatenate([both[:, :RANK], both[:, RANK:]], axis=0)
    spread_own(("fa", 3), NEAR, 1)
    local3 = mult(b3, blk[3][...]) * piv[3][...]
    solve_front(2, local2)
    pass_zp(1)
    tot = near_sum(("fa", 3))
    hq = tot[:count] * head[3]
    rp = tot[count:] + times(hq, kept(("cross", 3)), 0)
    m["fb"][far] = jnp.concatenate([rp, hq], axis=0)
    spread_own("fb", fars, NEAR)
    early = outer(local3, blk[3][...])
    pass_zp(2)
    arrive(("zb", 1))
    base1 = base_of(1, jnp.sum(m["zb", 1][...], axis=0))
    arrive("fb")
    tot = jnp.sum(m["fb"][...], axis=0)
    ends = jnp.concatenate([tot[:count] * head[3], tot[count:]], axis=1)
    x = early + times(ends, kept(("qw", 3)), 1)

    def send_down(level, full):
        count_tiles, per = tiles_of(level)
        sp = times(full, kept(("g", level)), 1)
        tile = pick(full, m["ohg", level][...])
        for t in range(count_tiles):
            m["bs", level][t] = jnp.concatenate(
                [sp[:, :RANK], sp[:, RANK:], tile[:, t * LANES : (t + 1) * LANES]], axis=0
            )
        bs, ba = m["bs", level], m["ba", level]
        ba[near] = bs[near // per]
        fan_near(("ba", level), lambda q: bs.at[q // per], ba)

    def send_further(level):
        n = nb[level + 1]
        half = n // 2
        arrive(("ba", level))
        ba = m["ba", level]
        tot = jnp.sum(ba[:, : 2 * count, :], axis=0)
        two, sb = m["two", level], m["sb", level]
        two[0] = tot[:count]
        two[1] = tot[count:]
        idx = far % n
        sb[idx] = two[idx // half]
        m["td", level][...] = transposed(ba[:, 2 * count :, :].reshape(NEAR * count, LANES))
        fan(
            n,
            NEAR,
            (("sb", level), lambda q: two.at[q // half], lambda i: sb.at[i], sb.at[pl.ds(0, n - 1)]),
            forward_rows(level, ("td", level), ("rd", level), ("rd", level)),
        )

    def receive_down(level, base):
        arrive(("sb", level))
        s = jnp.sum(m["sb", level][...], axis=0) * side[level]
        x = base - times(s, kept(("t", level)), 1)
        arrive(("rd", level))
        xu = spread(m["rd", level][...], m["ohr", level][...], NEAR, count)
        return x, xu

    send_down(2, x)
    outs[3][...] = x
    arrive(("zb", 2))
    base2 = base_of(2, jnp.sum(m["zb", 2][...], axis=0))
    send_further(2)
    x, xu = receive_down(2, base2)
    send_down(1, jnp.concatenate([x, xu], axis=1))
    outs[2][...] = x
    send_further(1)
    x, xu = receive_down(1, base1)
    m["s0b"][...] = leaf_rows((m["oh0"][...], None), diagonal(jnp.concatenate([x, xu], axis=1), cap))
    send_leaf("s0b", "r0b", "r0b")
    outs[1][...] = x
    arrive("r0b")
    rows = stacked(m["r0b"][...].T[: cap * count])
    half = cap * count
    first = once(rows, m["hch"][...], 1, 0)
    second = once(rows[:half], m["hcl"][...], 1, 0)
    s = None
    for g in range(cap):
        lanes = slice(g * RANK, (g + 1) * RANK)
        up, down = slice(g * count, (g + 1) * count), slice(half + g * count, half + (g + 1) * count)
        part = first[up, lanes] + (first[down, lanes] + second[up, lanes])
        s = part if s is None else s + part
    m["xs"][my4] = s
    spread_own("xs", four, 1)
    arrive("xs")
    s = jnp.sum(m["xs"][...], axis=0) * side[0]
    outs[0][...] = base0 - times(s, kept(("t", 0)), 1)

    for name, part in parts.items():
        wait_for(part, send_sem.at[sem_of(name)])


def solution(mesh):
    leaves, across = mesh.shape["leaf"], mesh.shape["grid"]

    def shards(*args):
        levels = [args[8 * i : 8 * i + 8] for i in range(3)]
        root = args[24:30]
        (sl, bl, el, qs, pv, cl, rk, tg) = zip(*levels)
        src = list(sl) + [root[0]]
        blk = list(bl) + [root[1]]
        exp = list(el) + [root[2]]
        bas = list(qs) + [root[3]]
        piv = [v.reshape(1, -1) for v in list(pv) + [root[4]]]
        rnk = [r.T for r in rk] + [root[5]]
        tgt = [t.reshape(1, -1) for t in tg]
        count = src[0].shape[0]
        ups = [t.shape[1] for t in tgt]
        fronts = [r.shape[0] for r in rk] + [root[5].shape[0]]
        size = [leaves * across // f for f in fronts]
        cap = ups[0] // size[1]
        nb = [s // NEAR for s in size]
        for v in src:
            assert v.shape == (NEAR, LANES)
        assert ups[1:] == [LANES, LANES] and cap * (count + 1) <= LANES
        assert size[2] == 2 * size[1] and size[3] == 2 * size[2] and size[1] % NEAR == 0
        assert NEAR * nb[2] == LANES and NEAR * nb[3] == 2 * LANES
        vm = lambda *s: pltpu.VMEM(s, F32)
        bits = lambda *s: pltpu.VMEM(s, BF16)
        piece = RANK // NEAR
        bufs = {
            "f1": vm(size[0], 2 * count, LANES),
            "c0": vm(size[0], RANK, RANK),
            "zx": vm(size[0], count, LANES),
            "xs": vm(size[0], count, LANES),
            "xp": vm(NEAR, 3 * piece, RANK),
            "xra": vm(NEAR, 3 * piece, RANK),
            "xg1": vm(NEAR, piece, RANK),
            "xg2": vm(NEAR, 2 * piece, RANK),
            "lows": vm(2, count, LANES),
            "la": vm(NEAR, count, LANES),
            "tl": vm(LANES, LANES),
            "hch": bits(size[1], cap * RANK),
            "hcl": bits(size[1], cap * RANK),
            "low0": vm(size[1], LANES),
            "oh0": bits(size[1], cap * 2 * LANES),
            "fb": vm(nb[3], 2 * count, LANES),
        }
        for name in ("s0", "r0", "s0b", "r0b"):
            bufs[name] = vm(size[1], LANES)
        for j in range(3):
            bufs["xb", j] = vm(nb[j + 1], piece, RANK)
        for i in range(4):
            for half in "hl":
                bufs[("cross", i), half] = bits(RANK, RANK)
                bufs[("qw", i), half] = bits(LANES, 2 * RANK)
                bufs[("t", i), half] = bits(LANES, RANK)
        bufs["fa", 3] = vm(NEAR, 2 * count, LANES)
        for i in (1, 2):
            n = nb[i + 1]
            wide = 2 * LANES if i == 1 else LANES
            tiles = NEAR * n // LANES
            bufs["h", i] = bits(NEAR * n, LANES)
            bufs["ohr", i] = bits(n, NEAR * LANES)
            bufs["ohf", i] = bits(n, NEAR * wide)
            bufs["ohg", i] = bits(NEAR * n, wide)
            bufs["pa", i] = vm(NEAR, n, RANK)
            bufs["ra", i] = vm(NEAR, n, RANK)
            bufs["rb", i] = vm(NEAR, n, RANK)
            bufs["lb", i] = vm(n, LANES)
            for half in "hl":
                bufs[("g", i), half] = bits(2 * RANK, wide)
            bufs["fs", i] = vm(tiles, 3 * count, LANES)
            bufs["fa", i] = vm(NEAR, 3 * count, LANES)
            bufs["bs", i] = vm(tiles, 3 * count, LANES)
            bufs["ba", i] = vm(NEAR, 3 * count, LANES)
            bufs["tf", i] = vm(LANES, LANES)
            bufs["td", i] = vm(LANES, LANES)
            bufs["rf", i] = vm(n, LANES)
            bufs["rd", i] = vm(n, LANES)
            bufs["wb", i] = vm(n, count, LANES)
            bufs["sb", i] = vm(n, count, LANES)
            bufs["two", i] = vm(2, count, LANES)
            bufs["hb", i] = vm(nb[i], count, LANES)
            bufs["za", i] = vm(NEAR, count, LANES)
            bufs["zb", i] = vm(nb[i], count, LANES)
        scratch = list(bufs.values())
        scratch += [
            pltpu.SemaphoreType.DMA((48,)),
            pltpu.SemaphoreType.DMA((48,)),
            pltpu.SemaphoreType.REGULAR,
        ]
        vspec = pl.BlockSpec(memory_space=pltpu.VMEM)
        sspec = pl.BlockSpec(memory_space=pltpu.SMEM)
        return pl.pallas_call(
            functools.partial(kernel, (leaves, across, size, ups, count, cap), list(bufs)),
            out_shape=[jax.ShapeDtypeStruct(v.shape, F32) for v in src],
            in_specs=[vspec] * 20 + [sspec] * 4 + [vspec] * 6,
            out_specs=[vspec] * 4,
            scratch_shapes=scratch,
            compiler_params=pltpu.CompilerParams(
                collective_id=0, has_side_effects=True, vmem_limit_bytes=60 * 1024 * 1024
            ),
        )(*src, *blk, *exp, *bas, *piv, *rnk, *cl, *tgt)

    spread_axes = ("leaf", "grid")
    level = (P(None, spread_axes), P(spread_axes, None), P(spread_axes, None), P(spread_axes, None), P(spread_axes))
    mid = level + (P(spread_axes, None), P(), P(spread_axes))
    return jax.shard_map(
        shards,
        mesh=mesh,
        in_specs=mid * 3 + level + (P(),),
        out_specs=(P(None, spread_axes),) * 4,
        check_vma=False,
    )
```

```python
import functools

import jax
import jax.numpy as jnp
from jax import lax
from jax.experimental import pallas as pl
from jax.experimental.pallas import tpu as pltpu
from jax.sharding import PartitionSpec as P

RANK = 128
LANES = 128
NEAR = 8
LOGICAL = pl.DeviceIdType.LOGICAL
F32 = jnp.float32
BF16 = jnp.bfloat16


def once(a, b, ca, cb):
    return lax.dot_general(a, b, (((ca,), (cb,)), ((), ())), preferred_element_type=F32)


def halves(x):
    hi = x.astype(BF16)
    return hi, (x - hi.astype(F32)).astype(BF16)


def stacked(x):
    hi = x.astype(BF16).astype(F32)
    return jnp.concatenate([hi, x - hi], axis=0).astype(BF16)


def times(a, b, cb):
    bh, bl = b
    n = a.shape[0]
    both = once(stacked(a), bh, 1, cb)
    return both[:n] + (both[n:] + once(a.astype(BF16), bl, 1, cb))


def mult(a, b):
    return times(a, halves(b), 0)


def outer(a, b):
    return times(a, halves(b), 1)


def inner(a, b):
    ah, al = halves(a)
    bh, bl = halves(b)
    return once(ah, bh, 0, 0) + (once(al, bh, 0, 0) + once(ah, bl, 0, 0))


def pick(x, onehot):
    n = x.shape[0]
    both = once(stacked(x), onehot, 1, 1)
    return both[:n] + both[n:]


def spread(rows, onehot, groups, count):
    m = groups * count
    wide = onehot.shape[1] // groups
    both = once(stacked(rows.T[:m]), onehot, 1, 0)
    out = None
    for g in range(groups):
        lanes = slice(g * wide, (g + 1) * wide)
        part = both[g * count : (g + 1) * count, lanes] + both[m + g * count : m + (g + 1) * count, lanes]
        out = part if out is None else out + part
    return out


def diagonal(x, groups):
    count, wide = x.shape
    zero = jnp.zeros((count, wide), F32)
    rows = [
        jnp.concatenate([x if h == g else zero for h in range(groups)], axis=1) for g in range(groups)
    ]
    rows.append(jnp.zeros((LANES - groups * count, groups * wide), F32))
    return jnp.concatenate(rows, axis=0)


def kernel(cfg, names, *refs):
    leaves, across, size, ups, count, cap = cfg
    total_devices = leaves * across
    (src, blk, exp, bas, piv, rnk) = [refs[4 * i : 4 * i + 4] for i in range(6)]
    cpl = refs[24:27]
    tgt = refs[27:30]
    outs = refs[30:34]
    m = dict(zip(names, refs[34:-3]))
    send_sem, recv_sem, ready = refs[-3:]
    sems = {}
    parts = {}

    me = lax.axis_index("leaf") * across + lax.axis_index("grid")
    near = me % NEAR
    far = me // NEAR
    nb = [s // NEAR for s in size]
    plane = size[1]
    fars = nb[3]

    def sem_of(name):
        return sems.setdefault(name, len(sems))

    def remote(a, b, sem, peer):
        return pltpu.make_async_remote_copy(
            src_ref=a,
            dst_ref=b,
            send_sem=send_sem.at[sem],
            recv_sem=recv_sem.at[sem],
            device_id=peer,
            device_id_type=LOGICAL,
        )

    def wait_for(part, sem):
        pltpu.make_async_copy(part, part, sem).wait()

    ring = nb[1]

    def farthest(n):
        return sorted(range(n), key=lambda d: -min(d, n - d))

    def fan(group, stride, *sets):
        idx = me // stride % group
        base = me - idx * stride
        for name, source, dest, part in sets:
            sem_of(name)
            parts[name] = part

        def go(q):
            for name, source, dest, part in sets:
                remote(source(q), dest(idx), sem_of(name), base + q * stride).start()

        if stride == NEAR:
            rows = group // ring
            for dy in farthest(rows):
                line = (idx // ring + dy) % rows * ring
                for dz in farthest(ring):
                    if dy or dz:
                        go(line + (idx + dz) % ring)
        elif group == plane:
            for dz in farthest(ring)[:-1]:
                line = (idx // NEAR + dz) % ring * NEAR

                def body(k, carry, line=line):
                    go(line + k)
                    return carry

                lax.fori_loop(0, NEAR, body, 0, unroll=True)
            for k in range(1, NEAR):
                go(idx // NEAR * NEAR + (idx + k) % NEAR)
        elif group == NEAR:
            for dx in farthest(across):
                for dc in (1, 0):
                    if dx or dc:
                        go((idx // across + dc) % 2 * across + (idx + dx) % across)
        else:
            for d in farthest(group)[:-1]:
                go((idx + d) % group)

    def arrive(name):
        wait_for(parts[name], recv_sem.at[sem_of(name)])

    def slots(name, group):
        buf = m[name]
        return buf.at[pl.ds(0, group - 1)]

    def spread_own(name, group, stride):
        buf = m[name]
        idx = me // stride % group
        fan(group, stride, (name, lambda q: buf.at[idx], lambda i: buf.at[i], slots(name, group)))

    barrier = pltpu.get_barrier_semaphore()

    def greet_near(sem):
        def body(k, carry):
            peer = far * NEAR + (near + k) % NEAR
            pl.semaphore_signal(sem, inc=1, device_id=peer, device_id_type=LOGICAL)
            return carry

        lax.fori_loop(1, NEAR, body, 0)

    def greet_far(k, carry):
        peer = (far + k) % fars * NEAR + near
        pl.semaphore_signal(barrier, inc=1, device_id=peer, device_id_type=LOGICAL)
        return carry

    lax.fori_loop(1, fars, greet_far, 0)
    greet_near(barrier)

    col = lax.broadcasted_iota(jnp.int32, (count, RANK), 1)

    def mask(level, which):
        def of(front):
            rank = rnk[level][which, front] if level < 2 else rnk[level][front, which]
            return (col < rank).astype(F32)

        return of

    front = [me // s for s in size]
    head = [mask(level, 0)(front[level]) for level in range(4)]
    side = [mask(level, 1)(front[level]) for level in range(3)]

    def q_of(level):
        return bas[level][:, :RANK]

    def v_of(level):
        return bas[level][:, RANK:]

    def tiles_of(level):
        n = nb[level + 1]
        return NEAR * n // LANES, LANES // n

    four = size[0]
    my4 = me % four
    s0 = src[0][...]
    local0 = mult(s0, blk[0][...])
    m["f1"][my4] = mult(s0, q_of(0))
    m["c0"][my4] = inner(exp[0][...], v_of(0))

    slice_rows = RANK // NEAR
    root_piv = jnp.broadcast_to(piv[3][...], (LANES, LANES)).T
    crosses = [
        inner(exp[1][...], v_of(1)),
        inner(exp[2][...], v_of(2)),
        inner(exp[3][...] * root_piv, exp[3][...]),
    ]
    for j, cross in enumerate(crosses):
        buf, at = (m["xp1"], 0) if j == 0 else (m["xp2"], (j - 1) * slice_rows)
        buf[:, at : at + slice_rows, :] = cross.reshape(NEAR, slice_rows, RANK)

    def split_targets(level):
        sep = size[level + 1] * LANES
        t = tgt[level][...]
        upd = t >= sep
        rel = jnp.where(upd, t - sep, t)
        return rel // LANES, rel % LANES + jnp.where(upd, LANES, 0)

    def pack_leaf():
        u = ups[0]
        dst, low = split_targets(0)
        ri = lax.broadcasted_iota(jnp.int32, (u, u), 0)
        ci = lax.broadcasted_iota(jnp.int32, (u, u), 1)
        dst_f = dst.astype(F32)
        dst_c = jnp.sum(jnp.where(ri == ci, jnp.broadcast_to(dst_f, (u, u)), 0.0), axis=1, keepdims=True)
        rank = jnp.sum(
            jnp.where((dst_c == dst_f) & (ri < ci), 1.0, 0.0), axis=0, keepdims=True
        ).astype(jnp.int32)
        slot = rank * plane + dst
        ch, cl = halves(cpl[0][...])
        lowmat = None
        li = lax.broadcasted_iota(jnp.int32, (LANES, u), 0)
        for s in range(cap):
            si = lax.broadcasted_iota(jnp.int32, (plane, u), 0) + s * plane
            hit = (si == slot).astype(F32).astype(BF16)
            lanes = slice(s * RANK, (s + 1) * RANK)
            m["hch"][:, lanes] = once(hit, ch, 1, 0).astype(BF16)
            m["hcl"][:, lanes] = once(hit, cl, 1, 0).astype(BF16)
            mine = jnp.where(li == cap * count + s, low.astype(F32), 0.0).astype(BF16)
            part = once(hit, mine, 1, 1)
            lowmat = part if lowmat is None else lowmat + part
        m["low0"][...] = lowmat

    def pack_couple(level):
        n = nb[level + 1]
        dst, low = split_targets(level)
        slot = dst % NEAR * n + dst // NEAR
        si = lax.broadcasted_iota(jnp.int32, (NEAR * n, LANES), 0)
        h = (si == slot).astype(F32).astype(BF16)
        m["h", level][...] = h
        hi, lo = [once(h, piece, 1, 0) for piece in halves(cpl[level][...])]
        m["pa", level][...] = (hi + lo).reshape(NEAR, n, RANK)
        rows = jnp.broadcast_to(low, (count, LANES)).astype(F32).astype(BF16)
        bi = lax.broadcasted_iota(jnp.int32, (n, LANES), 0) * NEAR
        m["ohr", level][...] = jnp.concatenate(
            [(bi + k == dst).astype(F32) for k in range(NEAR)], axis=1
        ).astype(BF16)
        return once(rows, h, 1, 1)

    low1, low2 = pack_couple(1), pack_couple(2)
    ri = lax.broadcasted_iota(jnp.int32, (count, LANES), 0)
    for t in range(2):
        two = low2[:, t * LANES : (t + 1) * LANES]
        m["lows"][t] = jnp.where(ri == 0, two, jnp.where(ri == 1, low1, 0.0))
    pack_leaf()

    pl.semaphore_wait(barrier, NEAR - 1 + fars - 1)
    greet_near(ready)
    spread_own("f1", four, 1)

    def fan_near(name, source, dest):
        fan(NEAR, 1, (name, source, lambda i: dest.at[i], dest.at[pl.ds(0, NEAR - 1)]))

    def scatter_near(name, source):
        m[name][near] = m[source][near]
        fan_near(name, lambda q: m[source].at[q], m[name])

    scatter_near("xr1", "xp1")
    m["la"][near] = m["lows"][near // 4]
    fan_near("la", lambda q: m["lows"].at[q // 4], m["la"])
    scatter_near(("ra", 1), ("pa", 1))

    def keep(name, value):
        hi, lo = halves(value)
        m[name, "h"][...] = hi
        m[name, "l"][...] = lo

    def kept(name):
        return m[name, "h"][...], m[name, "l"][...]

    for level in (1, 2):
        wv = mult(blk[level][...], v_of(level))
        keep(("qw", level), jnp.concatenate([q_of(level), wv], axis=1))
    wpp = mult(blk[3][...] * piv[3][...], exp[3][...])
    keep(("qw", 3), jnp.concatenate([q_of(3), wpp], axis=1))

    arrive("f1")
    hq0 = jnp.sum(m["f1"][...], axis=0) * head[0]
    y0 = local0 + outer(hq0, exp[0][...])
    m["fv"][my4] = mult(y0, v_of(0))
    spread_own("fv", four, 1)
    scatter_near(("ra", 2), ("pa", 2))
    scatter_near("xr2", "xp2")
    z0 = y0 * piv[0][...]
    m["zx"][my4] = mult(z0, exp[0][...])
    arrive("xr1")
    m["xb1"][far % ring] = jnp.sum(m["xr1"][...], axis=0)
    spread_own("xb1", ring, NEAR)
    arrive("fv")
    w0 = jnp.sum(m["fv"][...], axis=0) * side[0]

    def leaf_rows(a, b):
        ah, al = a
        bh, bl = halves(b)
        out = once(ah, bh, 1, 1) + once(ah, bl, 1, 1)
        return out if al is None else out + once(al, bh, 1, 1)

    place = me % plane

    def send_leaf(rows, got, name):
        m[got][pl.ds(place, 1), :] = m[rows][pl.ds(place, 1), :]
        fan(
            plane,
            1,
            (
                name,
                lambda q: m[rows].at[pl.ds(q, 1)],
                lambda i: m[got].at[pl.ds(i, 1)],
                m[got].at[pl.ds(0, plane - 1)],
            ),
        )

    hc = (m["hch"][...], m["hcl"][...])
    m["s0"][...] = leaf_rows(hc, diagonal(-w0, cap)) + m["low0"][...]
    pl.semaphore_wait(ready, NEAR - 1)
    send_leaf("s0", "r0", "r0")

    def store_row(buf, i, row):
        buf[pl.ds(i, 1), :] = row

    def forward_rows(level, table, got, name):
        n = nb[level + 1]
        per = tiles_of(level)[1]
        idx = far % n
        first = near % per * n
        store_row(m[got], idx, m[table][pl.ds(first + idx, 1), :])
        return (
            name,
            lambda q: m[table].at[pl.ds(first + q, 1)],
            lambda i: m[got].at[pl.ds(i, 1)],
            m[got].at[pl.ds(0, n - 1)],
        )

    def transposed(x):
        return jnp.concatenate([x, jnp.zeros((LANES - x.shape[0], LANES), F32)], axis=0).T

    def couple_set(level):
        n = nb[level + 1]
        ra, rb = m["ra", level], m["rb", level]
        idx = far % n
        rb[:, pl.ds(idx, 1), :] = ra[:, pl.ds(idx, 1), :]
        return (
            ("rb", level),
            lambda q: ra.at[:, pl.ds(q, 1)],
            lambda i: rb.at[:, pl.ds(i, 1)],
            rb.at[:, pl.ds(0, n - 1)],
        )

    arrive("la")
    m["tl"][...] = transposed(m["la"][...].reshape(NEAR * count, LANES))
    for level in (1, 2):
        arrive(("ra", level))
        fan(nb[level + 1], NEAR, forward_rows(level, "tl", ("lb", level), ("lb", level)), couple_set(level))
    arrive("xr2")
    m["xb2"][far % ring] = jnp.sum(m["xr2"][...], axis=0)
    spread_own("xb2", ring, NEAR)
    arrive("xb1")
    m["xg1"][near] = jnp.sum(m["xb1"][...], axis=0)
    spread_own("xg1", NEAR, 1)
    spread_own("zx", four, 1)
    spread_own("c0", four, 1)

    def build(level):
        n = nb[level + 1]
        wide = 2 * LANES if level == 1 else LANES
        arrive(("lb", level))
        lb = m["lb", level][...]
        lane = lax.broadcasted_iota(jnp.int32, (n, wide), 1).astype(F32)
        at = 2 - level
        hits = [(lane == lb[:, k * count + at : k * count + at + 1]).astype(F32) for k in range(NEAR)]
        m["ohf", level][...] = jnp.concatenate(hits, axis=1).astype(BF16)
        m["ohg", level][...] = jnp.concatenate(hits, axis=0).astype(BF16)
        arrive(("rb", level))
        half = n // 2
        for child in range(2):
            rows = slice(child * half, (child + 1) * half)
            got = m["rb", level][:, rows, :].reshape(NEAR * half, RANK)
            hot = jnp.concatenate([hit[rows] for hit in hits], axis=0).astype(BF16)
            hi, lo = [once(piece, hot, 0, 0) for piece in halves(got)]
            gh, gl = halves(hi + lo)
            out = slice(child * RANK, (child + 1) * RANK)
            m[("g", level), "h"][out, :] = gh
            m[("g", level), "l"][out, :] = gl

    def send_up(level, b, u):
        count_tiles, per = tiles_of(level)
        both = times(b, kept(("qw", level)), 0)
        tile = pick(u, m["h", level][...])
        for t in range(count_tiles):
            m["fs", level][t] = jnp.concatenate(
                [both[:, :RANK], both[:, RANK:], tile[:, t * LANES : (t + 1) * LANES]], axis=0
            )
        fs, fa = m["fs", level], m["fa", level]
        fa[near] = fs[near // per]
        fan_near(("fa", level), lambda q: fs.at[q // per], fa)

    def send_far(level, kind, first, second, tiles):
        n = nb[level + 1]
        half = n // 2
        per = tiles_of(level)[1]
        idx = far % n
        table, source, got = m["t" + kind, level], m[kind + "s", level], m[kind + "b", level]
        table[...] = transposed(tiles[:, 2 * count :, :].reshape(NEAR * count, LANES))
        source[:half, :count, :] = jnp.broadcast_to(first[None], (half, count, RANK))
        source[half:, :count, :] = jnp.broadcast_to(second[None], (half, count, RANK))
        source[:, count, :] = table[pl.ds(pl.multiple_of(near % per * n, 8), n), :]
        used = pl.ds(0, count + 1)
        got[idx, : count + 1, :] = source[idx, : count + 1, :]
        fan(
            n,
            NEAR,
            (
                (kind, level),
                lambda q: source.at[q, used],
                lambda i: got.at[i, used],
                got.at[pl.ds(0, n - 1), used],
            ),
        )

    def send_on(level):
        arrive(("fa", level))
        fa = m["fa", level]
        tot = jnp.sum(fa[:, : 2 * count, :], axis=0)
        hq = tot[:count] * head[level]
        w = tot[count:] + times(hq, kept(("cross", level)), 0)
        send_far(level, "w", w, w, fa)
        m["hb", level][far % nb[level]] = hq
        spread_own(("hb", level), nb[level], NEAR)

    def receive_up(level):
        n = nb[level + 1]
        half = n // 2
        arrive(("w", level))
        wb = m["wb", level]
        ws = []
        for child in range(2):
            mc = mask(level, 1)(front[level + 1] * 2 + child)
            ws.append(jnp.sum(wb[child * half : (child + 1) * half, :count, :], axis=0) * mc)
        inc = -times(jnp.concatenate(ws, axis=1), kept(("g", level)), 0)
        return inc + spread(wb[:, count, :], m["ohf", level][...], NEAR, count)

    def near_sum(name):
        arrive(name)
        return jnp.sum(m[name][...], axis=0)

    saved = {}

    def solve_front(level, local):
        arrive(("hb", level))
        hq = jnp.sum(m["hb", level][...], axis=0)
        z = (local + outer(hq, exp[level][...])) * piv[level][...]
        saved[level] = z
        m["za", level][near] = mult(z, exp[level][...])
        spread_own(("za", level), NEAR, 1)

    def pass_zp(level):
        m["zb", level][far % nb[level]] = near_sum(("za", level))
        spread_own(("zb", level), nb[level], NEAR)

    def base_of(level, zp):
        return outer(saved[level], blk[level][...]) + outer(zp * head[level], q_of(level))

    def tail_of(level, wv):
        qm = q_of(level) * jnp.broadcast_to(head[level][:1], (LANES, RANK))
        keep(("t", level), wv + times(qm, kept(("cross", level)), 0))

    def wv_of(level):
        qh, ql = kept(("qw", level))
        return qh[:, RANK:].astype(F32) + ql[:, RANK:].astype(F32)

    arrive("r0")
    r0 = m["r0"][...]
    lane = lax.broadcasted_iota(jnp.int32, (plane, 2 * LANES), 1).astype(F32)
    at = cap * count
    m["oh0"][...] = jnp.concatenate(
        [(lane == r0[:, at + s : at + s + 1]).astype(F32) for s in range(cap)], axis=1
    ).astype(BF16)
    inc = spread(r0, m["oh0"][...], cap, count)
    b1 = src[1][...] + inc[:, :LANES]
    send_up(1, b1, inc[:, LANES:])

    local1 = mult(b1, blk[1][...])
    saved[0] = z0
    arrive("zx")
    base0 = base_of(0, jnp.sum(m["zx"][...], axis=0))
    build(1)
    arrive("xg1")
    keep(("cross", 1), m["xg1"][...].reshape(RANK, RANK))
    arrive("xb2")
    m["xy"][me // plane] = jnp.sum(m["xb2"][...], axis=0)
    spread_own("xy", total_devices // plane, plane)
    send_on(1)

    arrive("xy")
    pair = me // plane // 2 * 2
    m["xg2"][near, :slice_rows, :] = jnp.sum(m["xy"][pl.ds(pair, 2), :slice_rows, :], axis=0)
    m["xg2"][near, slice_rows:, :] = jnp.sum(m["xy"][:, slice_rows:, :], axis=0)
    spread_own("xg2", NEAR, 1)
    tail_of(1, wv_of(1))

    inc = receive_up(1)
    b2 = src[2][...] + inc[:, :LANES]
    send_up(2, b2, inc[:, LANES:])

    local2 = mult(b2, blk[2][...])
    build(2)
    arrive("xg2")
    keep(("cross", 2), m["xg2"][:, :slice_rows, :].reshape(RANK, RANK))
    send_on(2)
    keep(("cross", 3), m["xg2"][:, slice_rows:, :].reshape(RANK, RANK))
    root_qm = q_of(3) * jnp.broadcast_to(head[3][:1], (LANES, RANK))
    root_t = wv_of(3) + times(root_qm, kept(("cross", 3)), 0)
    keep(("qt", 3), jnp.concatenate([root_qm, root_t], axis=1))
    solve_front(1, local1)
    tail_of(2, wv_of(2))

    b3 = src[3][...] + receive_up(2)
    both = times(b3, kept(("qt", 3)), 0)
    m["fa", 3][near] = jnp.concatenate([both[:, :RANK], both[:, RANK:]], axis=0)
    spread_own(("fa", 3), NEAR, 1)
    local3 = mult(b3, blk[3][...]) * piv[3][...]
    solve_front(2, local2)
    pass_zp(1)
    m["fb"][far] = near_sum(("fa", 3))
    spread_own("fb", fars, NEAR)
    arrive("c0")
    keep(("cross", 0), jnp.sum(m["c0"][...], axis=0))
    tail_of(0, mult(blk[0][...], v_of(0)))
    early = outer(local3, blk[3][...])
    pass_zp(2)
    arrive(("zb", 1))
    base1 = base_of(1, jnp.sum(m["zb", 1][...], axis=0))
    arrive("fb")
    tot = jnp.sum(m["fb"][...], axis=0)
    ends = jnp.concatenate([tot[count:] * head[3], tot[:count]], axis=1)
    x = early + times(ends, kept(("qw", 3)), 1)

    def send_down(level, full):
        count_tiles, per = tiles_of(level)
        sp = times(full, kept(("g", level)), 1)
        tile = pick(full, m["ohg", level][...])
        for t in range(count_tiles):
            m["bs", level][t] = jnp.concatenate(
                [sp[:, :RANK], sp[:, RANK:], tile[:, t * LANES : (t + 1) * LANES]], axis=0
            )
        bs, ba = m["bs", level], m["ba", level]
        ba[near] = bs[near // per]
        fan_near(("ba", level), lambda q: bs.at[q // per], ba)

    def send_further(level):
        arrive(("ba", level))
        ba = m["ba", level]
        tot = jnp.sum(ba[:, : 2 * count, :], axis=0)
        send_far(level, "s", tot[:count], tot[count:], ba)

    def receive_down(level, base):
        arrive(("s", level))
        sb = m["sb", level]
        s = jnp.sum(sb[:, :count, :], axis=0) * side[level]
        x = base - times(s, kept(("t", level)), 1)
        xu = spread(sb[:, count, :], m["ohr", level][...], NEAR, count)
        return x, xu

    send_down(2, x)
    outs[3][...] = x
    arrive(("zb", 2))
    base2 = base_of(2, jnp.sum(m["zb", 2][...], axis=0))
    send_further(2)
    x, xu = receive_down(2, base2)
    send_down(1, jnp.concatenate([x, xu], axis=1))
    outs[2][...] = x
    send_further(1)
    x, xu = receive_down(1, base1)
    m["s0b"][...] = leaf_rows((m["oh0"][...], None), diagonal(jnp.concatenate([x, xu], axis=1), cap))
    send_leaf("s0b", "r0b", "r0b")
    outs[1][...] = x
    arrive("r0b")
    rows = stacked(m["r0b"][...].T[: cap * count])
    half = cap * count
    first = once(rows, m["hch"][...], 1, 0)
    second = once(rows[:half], m["hcl"][...], 1, 0)
    s = None
    for g in range(cap):
        lanes = slice(g * RANK, (g + 1) * RANK)
        up, down = slice(g * count, (g + 1) * count), slice(half + g * count, half + (g + 1) * count)
        part = first[up, lanes] + (first[down, lanes] + second[up, lanes])
        s = part if s is None else s + part
    m["xs"][my4] = s
    spread_own("xs", four, 1)
    arrive("xs")
    s = jnp.sum(m["xs"][...], axis=0) * side[0]
    outs[0][...] = base0 - times(s, kept(("t", 0)), 1)

    for name, part in parts.items():
        wait_for(part, send_sem.at[sem_of(name)])


def solution(mesh):
    leaves, across = mesh.shape["leaf"], mesh.shape["grid"]

    def shards(*args):
        levels = [args[8 * i : 8 * i + 8] for i in range(3)]
        root = args[24:30]
        (sl, bl, el, qs, pv, cl, rk, tg) = zip(*levels)
        src = list(sl) + [root[0]]
        blk = list(bl) + [root[1]]
        exp = list(el) + [root[2]]
        bas = list(qs) + [root[3]]
        piv = [v.reshape(1, -1) for v in list(pv) + [root[4]]]
        rnk = [rk[0].T, rk[1].T, rk[2], root[5]]
        tgt = [t.reshape(1, -1) for t in tg]
        count = src[0].shape[0]
        ups = [t.shape[1] for t in tgt]
        fronts = [r.shape[0] for r in rk] + [root[5].shape[0]]
        size = [leaves * across // f for f in fronts]
        cap = ups[0] // size[1]
        nb = [s // NEAR for s in size]
        for v in src:
            assert v.shape == (NEAR, LANES)
        assert ups[1:] == [LANES, LANES] and cap * (count + 1) <= LANES
        assert nb[1] == 8 and across == 4 and size[0] == across
        assert size[2] == 2 * size[1] and size[3] == 2 * size[2] and size[1] % NEAR == 0
        assert NEAR * nb[2] == LANES and NEAR * nb[3] == 2 * LANES
        vm = lambda *s: pltpu.VMEM(s, F32)
        bits = lambda *s: pltpu.VMEM(s, BF16)
        piece = RANK // NEAR
        bufs = {
            "f1": vm(size[0], count, LANES),
            "fv": vm(size[0], count, LANES),
            "c0": vm(size[0], RANK, RANK),
            "zx": vm(size[0], count, LANES),
            "xs": vm(size[0], count, LANES),
            "xp1": vm(NEAR, piece, RANK),
            "xr1": vm(NEAR, piece, RANK),
            "xp2": vm(NEAR, 2 * piece, RANK),
            "xr2": vm(NEAR, 2 * piece, RANK),
            "xb1": vm(nb[1], piece, RANK),
            "xb2": vm(nb[1], 2 * piece, RANK),
            "xy": vm(nb[3] // nb[1], 2 * piece, RANK),
            "xg1": vm(NEAR, piece, RANK),
            "xg2": vm(NEAR, 2 * piece, RANK),
            "lows": vm(2, count, LANES),
            "la": vm(NEAR, count, LANES),
            "tl": vm(LANES, LANES),
            "hch": bits(size[1], cap * RANK),
            "hcl": bits(size[1], cap * RANK),
            "low0": vm(size[1], LANES),
            "oh0": bits(size[1], cap * 2 * LANES),
            "fb": vm(nb[3], 2 * count, LANES),
        }
        for name in ("s0", "r0", "s0b", "r0b"):
            bufs[name] = vm(size[1], LANES)
        for i in range(4):
            for half in "hl":
                bufs[("cross", i), half] = bits(RANK, RANK)
                bufs[("qw", i), half] = bits(LANES, 2 * RANK)
                bufs[("t", i), half] = bits(LANES, RANK)
                bufs[("qt", i), half] = bits(LANES, 2 * RANK)
        bufs["fa", 3] = vm(NEAR, 2 * count, LANES)
        for i in (1, 2):
            n = nb[i + 1]
            wide = 2 * LANES if i == 1 else LANES
            tiles = NEAR * n // LANES
            bufs["h", i] = bits(NEAR * n, LANES)
            bufs["ohr", i] = bits(n, NEAR * LANES)
            bufs["ohf", i] = bits(n, NEAR * wide)
            bufs["ohg", i] = bits(NEAR * n, wide)
            bufs["pa", i] = vm(NEAR, n, RANK)
            bufs["ra", i] = vm(NEAR, n, RANK)
            bufs["rb", i] = vm(NEAR, n, RANK)
            bufs["lb", i] = vm(n, LANES)
            for half in "hl":
                bufs[("g", i), half] = bits(2 * RANK, wide)
            bufs["fs", i] = vm(tiles, 3 * count, LANES)
            bufs["fa", i] = vm(NEAR, 3 * count, LANES)
            bufs["bs", i] = vm(tiles, 3 * count, LANES)
            bufs["ba", i] = vm(NEAR, 3 * count, LANES)
            for kind in "ws":
                bufs["t" + kind, i] = vm(LANES, LANES)
                bufs[kind + "s", i] = vm(n, 2 * count, LANES)
                bufs[kind + "b", i] = vm(n, 2 * count, LANES)
            bufs["hb", i] = vm(nb[i], count, LANES)
            bufs["za", i] = vm(NEAR, count, LANES)
            bufs["zb", i] = vm(nb[i], count, LANES)
        scratch = list(bufs.values())
        scratch += [
            pltpu.SemaphoreType.DMA((48,)),
            pltpu.SemaphoreType.DMA((48,)),
            pltpu.SemaphoreType.REGULAR,
        ]
        vspec = pl.BlockSpec(memory_space=pltpu.VMEM)
        sspec = pl.BlockSpec(memory_space=pltpu.SMEM)
        return pl.pallas_call(
            functools.partial(kernel, (leaves, across, size, ups, count, cap), list(bufs)),
            out_shape=[jax.ShapeDtypeStruct(v.shape, F32) for v in src],
            in_specs=[vspec] * 20 + [sspec] * 4 + [vspec] * 6,
            out_specs=[vspec] * 4,
            scratch_shapes=scratch,
            compiler_params=pltpu.CompilerParams(
                collective_id=0, has_side_effects=True, vmem_limit_bytes=60 * 1024 * 1024
            ),
        )(*src, *blk, *exp, *bas, *piv, *rnk, *cl, *tgt)

    spread_axes = ("leaf", "grid")
    level = (P(None, spread_axes), P(spread_axes, None), P(spread_axes, None), P(spread_axes, None), P(spread_axes))
    mid = level + (P(spread_axes, None), P(), P(spread_axes))
    return jax.shard_map(
        shards,
        mesh=mesh,
        in_specs=mid * 3 + level + (P(),),
        out_specs=(P(None, spread_axes),) * 4,
        check_vma=False,
    )
```

```python
import functools

import jax
import jax.numpy as jnp
from jax import lax
from jax.experimental import pallas as pl
from jax.experimental.pallas import tpu as pltpu
from jax.sharding import PartitionSpec as P

RANK = 128
LANES = 128
NEAR = 8
LOGICAL = pl.DeviceIdType.LOGICAL
F32 = jnp.float32
BF16 = jnp.bfloat16


def once(a, b, ca, cb):
    return lax.dot_general(a, b, (((ca,), (cb,)), ((), ())), preferred_element_type=F32)


def halves(x):
    hi = x.astype(BF16)
    return hi, (x - hi.astype(F32)).astype(BF16)


def stacked(x):
    hi = x.astype(BF16).astype(F32)
    return jnp.concatenate([hi, x - hi], axis=0).astype(BF16)


def times(a, b, cb):
    bh, bl = b
    n = a.shape[0]
    both = once(stacked(a), bh, 1, cb)
    return both[:n] + (both[n:] + once(a.astype(BF16), bl, 1, cb))


def mult(a, b):
    return times(a, halves(b), 0)


def outer(a, b):
    return times(a, halves(b), 1)


def inner(a, b):
    ah, al = halves(a)
    bh, bl = halves(b)
    return once(ah, bh, 0, 0) + (once(al, bh, 0, 0) + once(ah, bl, 0, 0))


def pick(x, onehot):
    n = x.shape[0]
    both = once(stacked(x), onehot, 1, 1)
    return both[:n] + both[n:]


def spread(rows, onehot, groups, count):
    m = groups * count
    wide = onehot.shape[1] // groups
    both = once(stacked(rows.T[:m]), onehot, 1, 0)
    out = None
    for g in range(groups):
        lanes = slice(g * wide, (g + 1) * wide)
        part = both[g * count : (g + 1) * count, lanes] + both[m + g * count : m + (g + 1) * count, lanes]
        out = part if out is None else out + part
    return out


def diagonal(x, groups, again=1):
    count, wide = x.shape
    zero = jnp.zeros((count, wide), F32)
    rows = [
        jnp.concatenate([x if h == g else zero for h in range(groups)], axis=1) for g in range(groups)
    ]
    rows = rows * again
    left = LANES - len(rows) * count
    if left:
        rows.append(jnp.zeros((left, groups * wide), F32))
    return jnp.concatenate(rows, axis=0)


def kernel(cfg, names, *refs):
    leaves, across, size, ups, count, cap = cfg
    total_devices = leaves * across
    given, rnk, out = refs[:26], refs[26:30], refs[30]
    outs = [out.at[pl.ds(i * count, count)] for i in range(4)]
    m = dict(zip(names, refs[31:-4]))
    send_sem, recv_sem, load_sem, ready = refs[-4:]
    held = [m["in", i] for i in range(26)]
    (src, blk, exp, bas, piv) = [held[4 * i : 4 * i + 4] for i in range(5)]
    cpl, tgt = held[20:23], held[23:26]
    loads = [pltpu.make_async_copy(given[i], held[i], load_sem.at[i]) for i in range(26)]
    sems = {}
    parts = {}

    me = lax.axis_index("leaf") * across + lax.axis_index("grid")
    near = me % NEAR
    far = me // NEAR
    nb = [s // NEAR for s in size]
    plane = size[1]
    fars = nb[3]

    def sem_of(name):
        return sems.setdefault(name, len(sems))

    def remote(a, b, sem, peer):
        return pltpu.make_async_remote_copy(
            src_ref=a,
            dst_ref=b,
            send_sem=send_sem.at[sem],
            recv_sem=recv_sem.at[sem],
            device_id=peer,
            device_id_type=LOGICAL,
        )

    def wait_for(part, sem):
        pltpu.make_async_copy(part, part, sem).wait()

    ring = nb[1]

    def farthest(n):
        return sorted(range(n), key=lambda d: -min(d, n - d))

    def fan(group, stride, *sets):
        idx = me // stride % group
        base = me - idx * stride
        for name, source, dest, part in sets:
            sem_of(name)
            parts[name] = part

        def go(q):
            for name, source, dest, part in sets:
                remote(source(q), dest(idx), sem_of(name), base + q * stride).start()

        if stride == NEAR:
            rows = group // ring
            for dy in farthest(rows):
                line = (idx // ring + dy) % rows * ring
                for dz in farthest(ring):
                    if dy or dz:
                        go(line + (idx + dz) % ring)
        elif group == plane:
            for dz in farthest(ring)[:-1]:
                line = (idx // NEAR + dz) % ring * NEAR

                def body(k, carry, line=line):
                    go(line + k)
                    return carry

                lax.fori_loop(0, NEAR, body, 0, unroll=True)
            for k in range(1, NEAR):
                go(idx // NEAR * NEAR + (idx + k) % NEAR)
        elif group == NEAR:
            for dx in farthest(across):
                for dc in (1, 0):
                    if dx or dc:
                        go((idx // across + dc) % 2 * across + (idx + dx) % across)
        else:
            for d in farthest(group)[:-1]:
                go((idx + d) % group)

    def arrive(name):
        wait_for(parts[name], recv_sem.at[sem_of(name)])

    def slots(name, group):
        buf = m[name]
        return buf.at[pl.ds(0, group - 1)]

    def spread_own(name, group, stride):
        buf = m[name]
        idx = me // stride % group
        fan(group, stride, (name, lambda q: buf.at[idx], lambda i: buf.at[i], slots(name, group)))

    barrier = pltpu.get_barrier_semaphore()

    def greet_near(sem):
        def body(k, carry):
            peer = far * NEAR + (near + k) % NEAR
            pl.semaphore_signal(sem, inc=1, device_id=peer, device_id_type=LOGICAL)
            return carry

        lax.fori_loop(1, NEAR, body, 0)

    def greet_far(k, carry):
        peer = (far + k) % fars * NEAR + near
        pl.semaphore_signal(barrier, inc=1, device_id=peer, device_id_type=LOGICAL)
        return carry

    lax.fori_loop(1, fars, greet_far, 0)
    greet_near(barrier)
    soon = (0, 12)
    rest = [i for i in range(26) if i not in soon]
    for i in soon + tuple(rest):
        loads[i].start()

    col = lax.broadcasted_iota(jnp.int32, (count, RANK), 1)

    def mask(level, which):
        def of(front):
            rank = rnk[level][which, front] if level < 2 else rnk[level][front, which]
            return (col < rank).astype(F32)

        return of

    front = [me // s for s in size]
    head = [mask(level, 0)(front[level]) for level in range(4)]
    side = [mask(level, 1)(front[level]) for level in range(3)]

    def q_of(level):
        return bas[level][:, :RANK]

    def v_of(level):
        return bas[level][:, RANK:]

    def tiles_of(level):
        n = nb[level + 1]
        return NEAR * n // LANES, LANES // n

    four = size[0]
    my4 = me % four
    for i in soon:
        loads[i].wait()
    s0 = src[0][...]
    m["f1"][my4] = mult(s0, q_of(0))
    pl.semaphore_wait(barrier, NEAR - 1 + fars - 1)
    greet_near(ready)
    spread_own("f1", four, 1)
    for i in rest:
        loads[i].wait()
    local0 = mult(s0, blk[0][...])
    m["c0"][my4] = inner(exp[0][...], v_of(0))

    slice_rows = RANK // NEAR
    root_piv = jnp.broadcast_to(piv[3][...], (LANES, LANES)).T
    crosses = [
        inner(exp[1][...], v_of(1)),
        inner(exp[2][...], v_of(2)),
        inner(exp[3][...] * root_piv, exp[3][...]),
    ]
    for j, cross in enumerate(crosses):
        buf, at = (m["xp1"], 0) if j == 0 else (m["xp2"], (j - 1) * slice_rows)
        buf[:, at : at + slice_rows, :] = cross.reshape(NEAR, slice_rows, RANK)

    def split_targets(level):
        sep = size[level + 1] * LANES
        t = tgt[level][...]
        upd = t >= sep
        rel = jnp.where(upd, t - sep, t)
        return rel // LANES, rel % LANES + jnp.where(upd, LANES, 0)

    def pack_leaf():
        u = ups[0]
        dst, low = split_targets(0)
        ri = lax.broadcasted_iota(jnp.int32, (u, u), 0)
        ci = lax.broadcasted_iota(jnp.int32, (u, u), 1)
        dst_f = dst.astype(F32)
        dst_c = jnp.sum(jnp.where(ri == ci, jnp.broadcast_to(dst_f, (u, u)), 0.0), axis=1, keepdims=True)
        rank = jnp.sum(
            jnp.where((dst_c == dst_f) & (ri < ci), 1.0, 0.0), axis=0, keepdims=True
        ).astype(jnp.int32)
        slot = rank * plane + dst
        ch, cl = halves(cpl[0][...])
        lowmat = None
        li = lax.broadcasted_iota(jnp.int32, (LANES, u), 0)
        for s in range(cap):
            si = lax.broadcasted_iota(jnp.int32, (plane, u), 0) + s * plane
            hit = (si == slot).astype(F32).astype(BF16)
            lanes = slice(s * RANK, (s + 1) * RANK)
            high, low_part = once(hit, ch, 1, 0), once(hit, cl, 1, 0)
            m["hch"][:, lanes] = high.astype(BF16)
            m["hcl"][:, lanes] = low_part.astype(BF16)
            m["hx"][my4, s * plane : (s + 1) * plane, :] = high + low_part
            mine = jnp.where(li == cap * count + s, low.astype(F32), 0.0).astype(BF16)
            part = once(hit, mine, 1, 1)
            lowmat = part if lowmat is None else lowmat + part
        m["low0"][...] = lowmat

    def pack_couple(level):
        n = nb[level + 1]
        dst, low = split_targets(level)
        slot = dst % NEAR * n + dst // NEAR
        si = lax.broadcasted_iota(jnp.int32, (NEAR * n, LANES), 0)
        h = (si == slot).astype(F32).astype(BF16)
        m["h", level][...] = h
        hi, lo = [once(h, piece, 1, 0) for piece in halves(cpl[level][...])]
        m["pa", level][...] = (hi + lo).reshape(NEAR, n, RANK)
        rows = jnp.broadcast_to(low, (count, LANES)).astype(F32).astype(BF16)
        bi = lax.broadcasted_iota(jnp.int32, (n, LANES), 0) * NEAR
        m["ohr", level][...] = jnp.concatenate(
            [(bi + k == dst).astype(F32) for k in range(NEAR)], axis=1
        ).astype(BF16)
        return once(rows, h, 1, 1)

    low1, low2 = pack_couple(1), pack_couple(2)
    ri = lax.broadcasted_iota(jnp.int32, (count, LANES), 0)
    for t in range(2):
        two = low2[:, t * LANES : (t + 1) * LANES]
        m["lows"][t] = jnp.where(ri == 0, two, jnp.where(ri == 1, low1, 0.0))
    pack_leaf()

    def fan_near(name, source, dest):
        fan(NEAR, 1, (name, source, lambda i: dest.at[i], dest.at[pl.ds(0, NEAR - 1)]))

    def scatter_near(name, source):
        m[name][near] = m[source][near]
        fan_near(name, lambda q: m[source].at[q], m[name])

    scatter_near("xr1", "xp1")
    m["la"][near] = m["lows"][near // 4]
    fan_near("la", lambda q: m["lows"].at[q // 4], m["la"])
    scatter_near(("ra", 1), ("pa", 1))

    def keep(name, value):
        hi, lo = halves(value)
        m[name, "h"][...] = hi
        m[name, "l"][...] = lo

    def kept(name):
        return m[name, "h"][...], m[name, "l"][...]

    for level in (1, 2):
        wv = mult(blk[level][...], v_of(level))
        keep(("qw", level), jnp.concatenate([q_of(level), wv], axis=1))
    wpp = mult(blk[3][...] * piv[3][...], exp[3][...])
    keep(("qw", 3), jnp.concatenate([q_of(3), wpp], axis=1))

    arrive("f1")
    hq0 = jnp.sum(m["f1"][...], axis=0) * head[0]
    y0 = local0 + outer(hq0, exp[0][...])
    m["fv"][my4] = mult(y0, v_of(0))
    spread_own("fv", four, 1)
    scatter_near(("ra", 2), ("pa", 2))
    scatter_near("xr2", "xp2")
    z0 = y0 * piv[0][...]
    m["zx"][my4] = mult(z0, exp[0][...])
    arrive("xr1")
    m["xb1"][far % ring] = jnp.sum(m["xr1"][...], axis=0)
    spread_own("xb1", ring, NEAR)
    arrive("fv")
    w0 = jnp.sum(m["fv"][...], axis=0) * side[0]

    def leaf_rows(a, b):
        ah, al = a
        bh, bl = halves(b)
        out = once(ah, bh, 1, 1) + once(ah, bl, 1, 1)
        return out if al is None else out + once(al, bh, 1, 1)

    place = me % plane

    def send_leaf(rows, got, row):
        m[got][pl.ds(place, 1), :] = m[rows][pl.ds(row(place), 1), :]
        fan(
            plane,
            1,
            (
                got,
                lambda q: m[rows].at[pl.ds(row(q), 1)],
                lambda i: m[got].at[pl.ds(i, 1)],
                m[got].at[pl.ds(0, plane - 1)],
            ),
        )

    hc = (m["hch"][...], m["hcl"][...])
    m["s0"][...] = leaf_rows(hc, diagonal(-w0, cap)) + m["low0"][...]
    pl.semaphore_wait(ready, NEAR - 1)
    send_leaf("s0", "r0", lambda q: q)

    def store_row(buf, i, row):
        buf[pl.ds(i, 1), :] = row

    def forward_rows(level, table, got, name):
        n = nb[level + 1]
        per = tiles_of(level)[1]
        idx = far % n
        first = near % per * n
        store_row(m[got], idx, m[table][pl.ds(first + idx, 1), :])
        return (
            name,
            lambda q: m[table].at[pl.ds(first + q, 1)],
            lambda i: m[got].at[pl.ds(i, 1)],
            m[got].at[pl.ds(0, n - 1)],
        )

    def transposed(x):
        return jnp.concatenate([x, jnp.zeros((LANES - x.shape[0], LANES), F32)], axis=0).T

    def couple_set(level):
        n = nb[level + 1]
        ra, rb = m["ra", level], m["rb", level]
        idx = far % n
        rb[:, pl.ds(idx, 1), :] = ra[:, pl.ds(idx, 1), :]
        return (
            ("rb", level),
            lambda q: ra.at[:, pl.ds(q, 1)],
            lambda i: rb.at[:, pl.ds(i, 1)],
            rb.at[:, pl.ds(0, n - 1)],
        )

    arrive("la")
    m["tl"][...] = transposed(m["la"][...].reshape(NEAR * count, LANES))
    for level in (1, 2):
        arrive(("ra", level))
        fan(nb[level + 1], NEAR, forward_rows(level, "tl", ("lb", level), ("lb", level)), couple_set(level))
    arrive("xr2")
    m["xb2"][far % ring] = jnp.sum(m["xr2"][...], axis=0)
    spread_own("xb2", ring, NEAR)
    arrive("xb1")
    m["xg1"][near] = jnp.sum(m["xb1"][...], axis=0)
    spread_own("xg1", NEAR, 1)
    spread_own("zx", four, 1)
    spread_own("c0", four, 1)

    def build(level):
        n = nb[level + 1]
        wide = 2 * LANES if level == 1 else LANES
        arrive(("lb", level))
        lb = m["lb", level][...]
        lane = lax.broadcasted_iota(jnp.int32, (n, wide), 1).astype(F32)
        at = 2 - level
        hits = [(lane == lb[:, k * count + at : k * count + at + 1]).astype(F32) for k in range(NEAR)]
        m["ohf", level][...] = jnp.concatenate(hits, axis=1).astype(BF16)
        m["ohg", level][...] = jnp.concatenate(hits, axis=0).astype(BF16)
        arrive(("rb", level))
        half = n // 2
        for child in range(2):
            rows = slice(child * half, (child + 1) * half)
            got = m["rb", level][:, rows, :].reshape(NEAR * half, RANK)
            hot = jnp.concatenate([hit[rows] for hit in hits], axis=0).astype(BF16)
            hi, lo = [once(piece, hot, 0, 0) for piece in halves(got)]
            gh, gl = halves(hi + lo)
            out = slice(child * RANK, (child + 1) * RANK)
            m[("g", level), "h"][out, :] = gh
            m[("g", level), "l"][out, :] = gl

    def send_up(level, b, u):
        count_tiles, per = tiles_of(level)
        both = times(b, kept(("qw", level)), 0)
        tile = pick(u, m["h", level][...])
        for t in range(count_tiles):
            m["fs", level][t] = jnp.concatenate(
                [both[:, :RANK], both[:, RANK:], tile[:, t * LANES : (t + 1) * LANES]], axis=0
            )
        fs, fa = m["fs", level], m["fa", level]
        fa[near] = fs[near // per]
        fan_near(("fa", level), lambda q: fs.at[q // per], fa)

    def send_far(level, kind, first, second, tiles):
        n = nb[level + 1]
        half = n // 2
        per = tiles_of(level)[1]
        idx = far % n
        table, source, got = m["t" + kind, level], m[kind + "s", level], m[kind + "b", level]
        table[...] = transposed(tiles[:, 2 * count :, :].reshape(NEAR * count, LANES))
        source[:half, :count, :] = jnp.broadcast_to(first[None], (half, count, RANK))
        source[half:, :count, :] = jnp.broadcast_to(second[None], (half, count, RANK))
        source[:, count, :] = table[pl.ds(pl.multiple_of(near % per * n, 8), n), :]
        used = pl.ds(0, count + 1)
        got[idx, : count + 1, :] = source[idx, : count + 1, :]
        fan(
            n,
            NEAR,
            (
                (kind, level),
                lambda q: source.at[q, used],
                lambda i: got.at[i, used],
                got.at[pl.ds(0, n - 1), used],
            ),
        )

    def send_on(level):
        arrive(("fa", level))
        fa = m["fa", level]
        tot = jnp.sum(fa[:, : 2 * count, :], axis=0)
        hq = tot[:count] * head[level]
        w = tot[count:] + times(hq, kept(("cross", level)), 0)
        send_far(level, "w", w, w, fa)
        m["hb", level][far % nb[level]] = hq
        spread_own(("hb", level), nb[level], NEAR)

    def receive_up(level):
        n = nb[level + 1]
        half = n // 2
        arrive(("w", level))
        wb = m["wb", level]
        ws = []
        for child in range(2):
            mc = mask(level, 1)(front[level + 1] * 2 + child)
            ws.append(jnp.sum(wb[child * half : (child + 1) * half, :count, :], axis=0) * mc)
        inc = -times(jnp.concatenate(ws, axis=1), kept(("g", level)), 0)
        return inc + spread(wb[:, count, :], m["ohf", level][...], NEAR, count)

    def near_sum(name):
        arrive(name)
        return jnp.sum(m[name][...], axis=0)

    saved = {}

    def solve_front(level, local):
        arrive(("hb", level))
        hq = jnp.sum(m["hb", level][...], axis=0)
        z = (local + outer(hq, exp[level][...])) * piv[level][...]
        saved[level] = z
        m["za", level][near] = mult(z, exp[level][...])
        spread_own(("za", level), NEAR, 1)

    def pass_zp(level):
        m["zb", level][far % nb[level]] = near_sum(("za", level))
        spread_own(("zb", level), nb[level], NEAR)

    def base_of(level, zp):
        return outer(saved[level], blk[level][...]) + outer(zp * head[level], q_of(level))

    def tail_of(level, wv):
        qm = q_of(level) * jnp.broadcast_to(head[level][:1], (LANES, RANK))
        keep(("t", level), wv + times(qm, kept(("cross", level)), 0))

    def wv_of(level):
        qh, ql = kept(("qw", level))
        return qh[:, RANK:].astype(F32) + ql[:, RANK:].astype(F32)

    arrive("r0")
    r0 = m["r0"][...]
    lane = lax.broadcasted_iota(jnp.int32, (plane, 2 * LANES), 1).astype(F32)
    at = cap * count
    m["oh0"][...] = jnp.concatenate(
        [(lane == r0[:, at + s : at + s + 1]).astype(F32) for s in range(cap)], axis=1
    ).astype(BF16)
    inc = spread(r0, m["oh0"][...], cap, count)
    b1 = src[1][...] + inc[:, :LANES]
    send_up(1, b1, inc[:, LANES:])

    local1 = mult(b1, blk[1][...])
    saved[0] = z0
    arrive("zx")
    base0 = base_of(0, jnp.sum(m["zx"][...], axis=0))
    build(1)
    arrive("xg1")
    keep(("cross", 1), m["xg1"][...].reshape(RANK, RANK))
    arrive("xb2")
    m["xy"][me // plane] = jnp.sum(m["xb2"][...], axis=0)
    spread_own("xy", total_devices // plane, plane)
    send_on(1)

    arrive("xy")
    pair = me // plane // 2 * 2
    m["xg2"][near, :slice_rows, :] = jnp.sum(m["xy"][pl.ds(pair, 2), :slice_rows, :], axis=0)
    m["xg2"][near, slice_rows:, :] = jnp.sum(m["xy"][:, slice_rows:, :], axis=0)
    spread_own("xg2", NEAR, 1)
    tail_of(1, wv_of(1))

    inc = receive_up(1)
    b2 = src[2][...] + inc[:, :LANES]
    send_up(2, b2, inc[:, LANES:])

    local2 = mult(b2, blk[2][...])
    build(2)
    arrive("xg2")
    keep(("cross", 2), m["xg2"][:, :slice_rows, :].reshape(RANK, RANK))
    send_on(2)
    spread_own("hx", four, 1)
    keep(("cross", 3), m["xg2"][:, slice_rows:, :].reshape(RANK, RANK))
    root_qm = q_of(3) * jnp.broadcast_to(head[3][:1], (LANES, RANK))
    root_t = wv_of(3) + times(root_qm, kept(("cross", 3)), 0)
    keep(("qt", 3), jnp.concatenate([root_qm, root_t], axis=1))
    solve_front(1, local1)
    tail_of(2, wv_of(2))

    b3 = src[3][...] + receive_up(2)
    both = times(b3, kept(("qt", 3)), 0)
    core = near // across
    m["fs3"][0] = both[:, :RANK]
    m["fs3"][1] = both[:, RANK:]
    m["fa", 3][near] = m["fs3"][core]
    fan_near(("fa", 3), lambda q: m["fs3"].at[q // across], m["fa", 3])
    local3 = mult(b3, blk[3][...]) * piv[3][...]
    solve_front(2, local2)
    pass_zp(1)
    m["fb"][far] = near_sum(("fa", 3))
    spread_own("fb", fars, NEAR)
    arrive("c0")
    keep(("cross", 0), jnp.sum(m["c0"][...], axis=0))
    tail_of(0, mult(blk[0][...], v_of(0)))
    arrive("hx")
    for k in range(four):
        at = slice(k * cap * plane, (k + 1) * cap * plane)
        m["hxh"][at, :], m["hxl"][at, :] = halves(m["hx"][k])
    early = outer(local3, blk[3][...])
    pass_zp(2)
    arrive(("zb", 1))
    base1 = base_of(1, jnp.sum(m["zb", 1][...], axis=0))
    arrive("fb")
    m["fc"][core] = jnp.sum(m["fb"][...], axis=0)
    spread_own("fc", 2, across)
    arrive("fc")
    ends = jnp.concatenate([m["fc"][1] * head[3], m["fc"][0]], axis=1)
    x = early + times(ends, kept(("qw", 3)), 1)

    def send_down(level, full):
        count_tiles, per = tiles_of(level)
        sp = times(full, kept(("g", level)), 1)
        tile = pick(full, m["ohg", level][...])
        for t in range(count_tiles):
            m["bs", level][t] = jnp.concatenate(
                [sp[:, :RANK], sp[:, RANK:], tile[:, t * LANES : (t + 1) * LANES]], axis=0
            )
        bs, ba = m["bs", level], m["ba", level]
        ba[near] = bs[near // per]
        fan_near(("ba", level), lambda q: bs.at[q // per], ba)

    def send_further(level):
        arrive(("ba", level))
        ba = m["ba", level]
        tot = jnp.sum(ba[:, : 2 * count, :], axis=0)
        send_far(level, "s", tot[:count], tot[count:], ba)

    def receive_down(level, base):
        arrive(("s", level))
        sb = m["sb", level]
        s = jnp.sum(sb[:, :count, :], axis=0) * side[level]
        x = base - times(s, kept(("t", level)), 1)
        xu = spread(sb[:, count, :], m["ohr", level][...], NEAR, count)
        return x, xu

    send_down(2, x)
    outs[3][...] = x
    arrive(("zb", 2))
    base2 = base_of(2, jnp.sum(m["zb", 2][...], axis=0))
    send_further(2)
    x, xu = receive_down(2, base2)
    send_down(1, jnp.concatenate([x, xu], axis=1))
    outs[2][...] = x
    send_further(1)
    x, xu = receive_down(1, base1)
    full = diagonal(jnp.concatenate([x, xu], axis=1), cap, four)
    rows = leaf_rows((m["oh0"][...], None), full)
    ri = lax.broadcasted_iota(jnp.int32, (plane, LANES), 0)
    li = lax.broadcasted_iota(jnp.int32, (plane, LANES), 1)
    rows = jnp.where(li // (cap * count) == ri % four, rows, 0.0)
    rows = rows + pltpu.roll(rows, plane - 1, 0)
    m["s0b"][...] = rows + pltpu.roll(rows, plane - 2, 0)
    send_leaf("s0b", "r0b", lambda q: q // four * four)
    outs[1][...] = x
    arrive("r0b")
    rows = transposed(m["r0b"][...])
    pieces = [rows[g * count : (g + 1) * count] for g in range(four * cap)]
    pairs = [pieces[2 * g] + pltpu.roll(pieces[2 * g + 1], plane, 1) for g in range(four * cap // 2)]
    s = times(jnp.concatenate(pairs, axis=1), (m["hxh"][...], m["hxl"][...]), 0) * side[0]
    outs[0][...] = base0 - times(s, kept(("t", 0)), 1)

    for name, part in parts.items():
        wait_for(part, send_sem.at[sem_of(name)])


def solution(mesh):
    leaves, across = mesh.shape["leaf"], mesh.shape["grid"]

    def shards(*args):
        levels = [args[8 * i : 8 * i + 8] for i in range(3)]
        root = args[24:30]
        (sl, bl, el, qs, pv, cl, rk, tg) = zip(*levels)
        src = list(sl) + [root[0]]
        blk = list(bl) + [root[1]]
        exp = list(el) + [root[2]]
        bas = list(qs) + [root[3]]
        piv = [v.reshape(1, -1) for v in list(pv) + [root[4]]]
        rnk = [rk[0].T, rk[1].T, rk[2], root[5]]
        tgt = [t.reshape(1, -1) for t in tg]
        count = src[0].shape[0]
        ups = [t.shape[1] for t in tgt]
        fronts = [r.shape[0] for r in rk] + [root[5].shape[0]]
        size = [leaves * across // f for f in fronts]
        cap = ups[0] // size[1]
        nb = [s // NEAR for s in size]
        for v in src:
            assert v.shape == (NEAR, LANES)
        assert ups[1:] == [LANES, LANES] and cap * (count + 1) <= LANES
        assert 2 * size[1] == LANES and size[0] * cap * count == LANES
        assert nb[1] == 8 and across == 4 and size[0] == across
        assert size[2] == 2 * size[1] and size[3] == 2 * size[2] and size[1] % NEAR == 0
        assert NEAR * nb[2] == LANES and NEAR * nb[3] == 2 * LANES
        vm = lambda *s: pltpu.VMEM(s, F32)
        bits = lambda *s: pltpu.VMEM(s, BF16)
        piece = RANK // NEAR
        bufs = {
            "f1": vm(size[0], count, LANES),
            "fv": vm(size[0], count, LANES),
            "c0": vm(size[0], RANK, RANK),
            "zx": vm(size[0], count, LANES),
            "xp1": vm(NEAR, piece, RANK),
            "xr1": vm(NEAR, piece, RANK),
            "xp2": vm(NEAR, 2 * piece, RANK),
            "xr2": vm(NEAR, 2 * piece, RANK),
            "xb1": vm(nb[1], piece, RANK),
            "xb2": vm(nb[1], 2 * piece, RANK),
            "xy": vm(nb[3] // nb[1], 2 * piece, RANK),
            "xg1": vm(NEAR, piece, RANK),
            "xg2": vm(NEAR, 2 * piece, RANK),
            "lows": vm(2, count, LANES),
            "la": vm(NEAR, count, LANES),
            "tl": vm(LANES, LANES),
            "hch": bits(size[1], cap * RANK),
            "hcl": bits(size[1], cap * RANK),
            "low0": vm(size[1], LANES),
            "oh0": bits(size[1], cap * 2 * LANES),
            "fb": vm(nb[3], count, LANES),
            "fs3": vm(2, count, LANES),
            "fc": vm(2, count, LANES),
            "hx": vm(size[0], cap * size[1], RANK),
            "hxh": bits(size[0] * cap * size[1], RANK),
            "hxl": bits(size[0] * cap * size[1], RANK),
        }
        for name in ("s0", "r0", "s0b", "r0b"):
            bufs[name] = vm(size[1], LANES)
        for i in range(4):
            for half in "hl":
                bufs[("cross", i), half] = bits(RANK, RANK)
                bufs[("qw", i), half] = bits(LANES, 2 * RANK)
                bufs[("t", i), half] = bits(LANES, RANK)
                bufs[("qt", i), half] = bits(LANES, 2 * RANK)
        bufs["fa", 3] = vm(NEAR, count, LANES)
        for i in (1, 2):
            n = nb[i + 1]
            wide = 2 * LANES if i == 1 else LANES
            tiles = NEAR * n // LANES
            bufs["h", i] = bits(NEAR * n, LANES)
            bufs["ohr", i] = bits(n, NEAR * LANES)
            bufs["ohf", i] = bits(n, NEAR * wide)
            bufs["ohg", i] = bits(NEAR * n, wide)
            bufs["pa", i] = vm(NEAR, n, RANK)
            bufs["ra", i] = vm(NEAR, n, RANK)
            bufs["rb", i] = vm(NEAR, n, RANK)
            bufs["lb", i] = vm(n, LANES)
            for half in "hl":
                bufs[("g", i), half] = bits(2 * RANK, wide)
            bufs["fs", i] = vm(tiles, 3 * count, LANES)
            bufs["fa", i] = vm(NEAR, 3 * count, LANES)
            bufs["bs", i] = vm(tiles, 3 * count, LANES)
            bufs["ba", i] = vm(NEAR, 3 * count, LANES)
            for kind in "ws":
                bufs["t" + kind, i] = vm(LANES, LANES)
                bufs[kind + "s", i] = vm(n, 2 * count, LANES)
                bufs[kind + "b", i] = vm(n, 2 * count, LANES)
            bufs["hb", i] = vm(nb[i], count, LANES)
            bufs["za", i] = vm(NEAR, count, LANES)
            bufs["zb", i] = vm(nb[i], count, LANES)
        arrays = [*src, *blk, *exp, *bas, *piv, *cl, *tgt]
        for i, v in enumerate(arrays):
            bufs["in", i] = pltpu.VMEM(v.shape, v.dtype)
        scratch = list(bufs.values())
        scratch += [
            pltpu.SemaphoreType.DMA((48,)),
            pltpu.SemaphoreType.DMA((48,)),
            pltpu.SemaphoreType.DMA((26,)),
            pltpu.SemaphoreType.REGULAR,
        ]
        vspec = pl.BlockSpec(memory_space=pltpu.VMEM)
        sspec = pl.BlockSpec(memory_space=pltpu.SMEM)
        whole = pl.pallas_call(
            functools.partial(kernel, (leaves, across, size, ups, count, cap), list(bufs)),
            out_shape=jax.ShapeDtypeStruct((4 * count, LANES), F32),
            in_specs=[pl.BlockSpec(memory_space=pl.ANY)] * 26 + [sspec] * 4,
            out_specs=vspec,
            scratch_shapes=scratch,
            compiler_params=pltpu.CompilerParams(
                collective_id=0, has_side_effects=True, vmem_limit_bytes=60 * 1024 * 1024
            ),
        )(*arrays, *rnk)
        return tuple(whole[i * count : (i + 1) * count] for i in range(4))

    spread_axes = ("leaf", "grid")
    level = (P(None, spread_axes), P(spread_axes, None), P(spread_axes, None), P(spread_axes, None), P(spread_axes))
    mid = level + (P(spread_axes, None), P(), P(spread_axes))
    return jax.shard_map(
        shards,
        mesh=mesh,
        in_specs=mid * 3 + level + (P(),),
        out_specs=(P(None, spread_axes),) * 4,
        check_vma=False,
    )
```

```python
import functools

import jax
import jax.numpy as jnp
from jax import lax
from jax.experimental import pallas as pl
from jax.experimental.pallas import tpu as pltpu
from jax.sharding import PartitionSpec as P

RANK = 128
LANES = 128
NEAR = 8
LOGICAL = pl.DeviceIdType.LOGICAL
F32 = jnp.float32
BF16 = jnp.bfloat16


def once(a, b, ca, cb):
    return lax.dot_general(a, b, (((ca,), (cb,)), ((), ())), preferred_element_type=F32)


def halves(x):
    hi = x.astype(BF16)
    return hi, (x - hi.astype(F32)).astype(BF16)


def stacked(x):
    hi = x.astype(BF16).astype(F32)
    return jnp.concatenate([hi, x - hi], axis=0).astype(BF16)


def times(a, b, cb):
    bh, bl = b
    n = a.shape[0]
    both = once(stacked(a), bh, 1, cb)
    return both[:n] + (both[n:] + once(a.astype(BF16), bl, 1, cb))


def mult(a, b):
    return times(a, halves(b), 0)


def outer(a, b):
    return times(a, halves(b), 1)


def inner(a, b):
    ah, al = halves(a)
    bh, bl = halves(b)
    return once(ah, bh, 0, 0) + (once(al, bh, 0, 0) + once(ah, bl, 0, 0))


def pick(x, onehot):
    n = x.shape[0]
    both = once(stacked(x), onehot, 1, 1)
    return both[:n] + both[n:]


def spread(rows, onehot, groups, count):
    m = groups * count
    wide = onehot.shape[1] // groups
    both = once(stacked(rows.T[:m]), onehot, 1, 0)
    out = None
    for g in range(groups):
        lanes = slice(g * wide, (g + 1) * wide)
        part = both[g * count : (g + 1) * count, lanes] + both[m + g * count : m + (g + 1) * count, lanes]
        out = part if out is None else out + part
    return out


def diagonal(x, groups, again=1):
    count, wide = x.shape
    zero = jnp.zeros((count, wide), F32)
    rows = [
        jnp.concatenate([x if h == g else zero for h in range(groups)], axis=1) for g in range(groups)
    ]
    rows = rows * again
    left = LANES - len(rows) * count
    if left:
        rows.append(jnp.zeros((left, groups * wide), F32))
    return jnp.concatenate(rows, axis=0)


def kernel(cfg, names, *refs):
    leaves, across, size, ups, count, cap = cfg
    total_devices = leaves * across
    count_in = 30
    given, out = refs[:count_in], refs[count_in]
    outs = [out.at[pl.ds(i * count, count)] for i in range(4)]
    m = dict(zip(names, refs[count_in + 1 : -4]))
    send_sem, recv_sem, load_sem, ready = refs[-4:]
    held = [m["in", i] for i in range(count_in)]
    (src, blk, exp, bas, piv) = [held[4 * i : 4 * i + 4] for i in range(5)]
    cpl, tgt, rnk = held[20:23], held[23:26], held[26:30]
    loads = [pltpu.make_async_copy(given[i], held[i], load_sem.at[i]) for i in range(count_in)]
    sems = {}
    parts = {}

    me = lax.axis_index("leaf") * across + lax.axis_index("grid")
    near = me % NEAR
    far = me // NEAR
    nb = [s // NEAR for s in size]
    plane = size[1]
    fars = nb[3]

    def sem_of(name):
        return sems.setdefault(name, len(sems))

    def remote(a, b, sem, peer):
        return pltpu.make_async_remote_copy(
            src_ref=a,
            dst_ref=b,
            send_sem=send_sem.at[sem],
            recv_sem=recv_sem.at[sem],
            device_id=peer,
            device_id_type=LOGICAL,
        )

    def wait_for(part, sem):
        pltpu.make_async_copy(part, part, sem).wait()

    ring = nb[1]

    def farthest(n):
        return sorted(range(n), key=lambda d: -min(d, n - d))

    def fan(group, stride, *sets):
        idx = me // stride % group
        base = me - idx * stride
        for name, source, dest, part in sets:
            sem_of(name)
            parts[name] = part

        def go(q):
            for name, source, dest, part in sets:
                remote(source(q), dest(idx), sem_of(name), base + q * stride).start()

        if stride == NEAR:
            rows = group // ring
            for dy in farthest(rows):
                line = (idx // ring + dy) % rows * ring
                for dz in farthest(ring):
                    if dy or dz:
                        go(line + (idx + dz) % ring)
        elif group == plane:
            for dz in farthest(ring)[:-1]:
                line = (idx // NEAR + dz) % ring * NEAR

                def body(k, carry, line=line):
                    go(line + k)
                    return carry

                lax.fori_loop(0, NEAR, body, 0, unroll=True)
            for k in range(1, NEAR):
                go(idx // NEAR * NEAR + (idx + k) % NEAR)
        elif group == NEAR:
            for dx in farthest(across):
                for dc in (1, 0):
                    if dx or dc:
                        go((idx // across + dc) % 2 * across + (idx + dx) % across)
        else:
            for d in farthest(group)[:-1]:
                go((idx + d) % group)

    def arrive(name):
        wait_for(parts[name], recv_sem.at[sem_of(name)])

    def slots(name, group):
        buf = m[name]
        return buf.at[pl.ds(0, group - 1)]

    def spread_own(name, group, stride):
        buf = m[name]
        idx = me // stride % group
        fan(group, stride, (name, lambda q: buf.at[idx], lambda i: buf.at[i], slots(name, group)))

    barrier = pltpu.get_barrier_semaphore()

    def greet_near(sem):
        def body(k, carry):
            peer = far * NEAR + (near + k) % NEAR
            pl.semaphore_signal(sem, inc=1, device_id=peer, device_id_type=LOGICAL)
            return carry

        lax.fori_loop(1, NEAR, body, 0)

    def greet_far(k, carry):
        peer = (far + k) % fars * NEAR + near
        pl.semaphore_signal(barrier, inc=1, device_id=peer, device_id_type=LOGICAL)
        return carry

    lax.fori_loop(1, fars, greet_far, 0)
    greet_near(barrier)
    soon = (0, 12)
    rest = [i for i in range(count_in) if i not in soon]
    for i in soon + tuple(rest):
        loads[i].start()

    def mask(level, which, front):
        ranks = rnk[level][...].astype(F32)
        axis = 1 if level < 2 else 0
        line = ranks[which : which + 1, :] if level < 2 else ranks[:, which : which + 1]
        here = lax.broadcasted_iota(jnp.int32, line.shape, axis) == front
        rank = jnp.sum(jnp.where(here, line, 0.0), axis=axis, keepdims=True)
        col = lax.broadcasted_iota(jnp.int32, (count, RANK), 1).astype(F32)
        return (col < rank).astype(F32)

    def q_of(level):
        return bas[level][:, :RANK]

    def v_of(level):
        return bas[level][:, RANK:]

    def tiles_of(level):
        n = nb[level + 1]
        return NEAR * n // LANES, LANES // n

    four = size[0]
    my4 = me % four
    for i in soon:
        loads[i].wait()
    s0 = src[0][...]
    m["f1"][my4] = mult(s0, q_of(0))
    pl.semaphore_wait(barrier, NEAR - 1 + fars - 1)
    greet_near(ready)
    spread_own("f1", four, 1)
    for i in rest:
        loads[i].wait()
    front = [me // n for n in size]
    head = [mask(level, 0, front[level]) for level in range(4)]
    side = [mask(level, 1, front[level]) for level in range(3)]
    below = [None] + [
        [mask(level, 1, front[level + 1] * 2 + child) for child in range(2)] for level in (1, 2)
    ]
    local0 = mult(s0, blk[0][...])
    m["c0"][my4] = inner(exp[0][...], v_of(0))

    slice_rows = RANK // NEAR
    root_piv = jnp.broadcast_to(piv[3][...], (LANES, LANES)).T
    crosses = [
        inner(exp[1][...], v_of(1)),
        inner(exp[2][...], v_of(2)),
        inner(exp[3][...] * root_piv, exp[3][...]),
    ]
    for j, cross in enumerate(crosses):
        buf, at = (m["xp1"], 0) if j == 0 else (m["xp2"], (j - 1) * slice_rows)
        buf[:, at : at + slice_rows, :] = cross.reshape(NEAR, slice_rows, RANK)

    def split_targets(level):
        sep = size[level + 1] * LANES
        t = tgt[level][...]
        upd = t >= sep
        rel = jnp.where(upd, t - sep, t)
        return rel // LANES, rel % LANES + jnp.where(upd, LANES, 0)

    def pack_leaf():
        u = ups[0]
        dst, low = split_targets(0)
        ri = lax.broadcasted_iota(jnp.int32, (u, u), 0)
        ci = lax.broadcasted_iota(jnp.int32, (u, u), 1)
        dst_f = dst.astype(F32)
        dst_c = jnp.sum(jnp.where(ri == ci, jnp.broadcast_to(dst_f, (u, u)), 0.0), axis=1, keepdims=True)
        rank = jnp.sum(
            jnp.where((dst_c == dst_f) & (ri < ci), 1.0, 0.0), axis=0, keepdims=True
        ).astype(jnp.int32)
        slot = rank * plane + dst
        ch, cl = halves(cpl[0][...])
        lowmat = None
        li = lax.broadcasted_iota(jnp.int32, (LANES, u), 0)
        for s in range(cap):
            si = lax.broadcasted_iota(jnp.int32, (plane, u), 0) + s * plane
            hit = (si == slot).astype(F32).astype(BF16)
            lanes = slice(s * RANK, (s + 1) * RANK)
            high, low_part = once(hit, ch, 1, 0), once(hit, cl, 1, 0)
            m["hch"][:, lanes] = high.astype(BF16)
            m["hcl"][:, lanes] = low_part.astype(BF16)
            m["hx"][my4, s * plane : (s + 1) * plane, :] = high + low_part
            mine = jnp.where(li == cap * count + s, low.astype(F32), 0.0).astype(BF16)
            part = once(hit, mine, 1, 1)
            lowmat = part if lowmat is None else lowmat + part
        m["low0"][...] = lowmat

    def pack_couple(level):
        n = nb[level + 1]
        dst, low = split_targets(level)
        slot = dst % NEAR * n + dst // NEAR
        si = lax.broadcasted_iota(jnp.int32, (NEAR * n, LANES), 0)
        h = (si == slot).astype(F32).astype(BF16)
        m["h", level][...] = h
        hi, lo = [once(h, piece, 1, 0) for piece in halves(cpl[level][...])]
        m["pa", level][...] = (hi + lo).reshape(NEAR, n, RANK)
        rows = jnp.broadcast_to(low, (count, LANES)).astype(F32).astype(BF16)
        bi = lax.broadcasted_iota(jnp.int32, (n, LANES), 0) * NEAR
        m["ohr", level][...] = jnp.concatenate(
            [(bi + k == dst).astype(F32) for k in range(NEAR)], axis=1
        ).astype(BF16)
        return once(rows, h, 1, 1)

    low1, low2 = pack_couple(1), pack_couple(2)
    ri = lax.broadcasted_iota(jnp.int32, (count, LANES), 0)
    for t in range(2):
        two = low2[:, t * LANES : (t + 1) * LANES]
        m["lows"][t] = jnp.where(ri == 0, two, jnp.where(ri == 1, low1, 0.0))
    pack_leaf()

    def fan_near(name, source, dest):
        fan(NEAR, 1, (name, source, lambda i: dest.at[i], dest.at[pl.ds(0, NEAR - 1)]))

    def scatter_near(name, source):
        m[name][near] = m[source][near]
        fan_near(name, lambda q: m[source].at[q], m[name])

    scatter_near("xr1", "xp1")
    m["la"][near] = m["lows"][near // 4]
    fan_near("la", lambda q: m["lows"].at[q // 4], m["la"])
    scatter_near(("ra", 1), ("pa", 1))

    def keep(name, value):
        hi, lo = halves(value)
        m[name, "h"][...] = hi
        m[name, "l"][...] = lo

    def kept(name):
        return m[name, "h"][...], m[name, "l"][...]

    for level in (1, 2):
        wv = mult(blk[level][...], v_of(level))
        keep(("qw", level), jnp.concatenate([q_of(level), wv], axis=1))
    wpp = mult(blk[3][...] * piv[3][...], exp[3][...])
    keep(("qw", 3), jnp.concatenate([q_of(3), wpp], axis=1))

    arrive("f1")
    hq0 = jnp.sum(m["f1"][...], axis=0) * head[0]
    y0 = local0 + outer(hq0, exp[0][...])
    m["fv"][my4] = mult(y0, v_of(0))
    spread_own("fv", four, 1)
    scatter_near(("ra", 2), ("pa", 2))
    scatter_near("xr2", "xp2")
    z0 = y0 * piv[0][...]
    m["zx"][my4] = mult(z0, exp[0][...])
    arrive("xr1")
    m["xb1"][far % ring] = jnp.sum(m["xr1"][...], axis=0)
    spread_own("xb1", ring, NEAR)
    arrive("fv")
    w0 = jnp.sum(m["fv"][...], axis=0) * side[0]

    def leaf_rows(a, b):
        ah, al = a
        bh, bl = halves(b)
        out = once(ah, bh, 1, 1) + once(ah, bl, 1, 1)
        return out if al is None else out + once(al, bh, 1, 1)

    place = me % plane

    def send_leaf(rows, got, row):
        m[got][pl.ds(place, 1), :] = m[rows][pl.ds(row(place), 1), :]
        fan(
            plane,
            1,
            (
                got,
                lambda q: m[rows].at[pl.ds(row(q), 1)],
                lambda i: m[got].at[pl.ds(i, 1)],
                m[got].at[pl.ds(0, plane - 1)],
            ),
        )

    hc = (m["hch"][...], m["hcl"][...])
    m["s0"][...] = leaf_rows(hc, diagonal(-w0, cap)) + m["low0"][...]
    pl.semaphore_wait(ready, NEAR - 1)
    send_leaf("s0", "r0", lambda q: q)

    def store_row(buf, i, row):
        buf[pl.ds(i, 1), :] = row

    def forward_rows(level, table, got, name):
        n = nb[level + 1]
        per = tiles_of(level)[1]
        idx = far % n
        first = near % per * n
        store_row(m[got], idx, m[table][pl.ds(first + idx, 1), :])
        return (
            name,
            lambda q: m[table].at[pl.ds(first + q, 1)],
            lambda i: m[got].at[pl.ds(i, 1)],
            m[got].at[pl.ds(0, n - 1)],
        )

    def transposed(x):
        return jnp.concatenate([x, jnp.zeros((LANES - x.shape[0], LANES), F32)], axis=0).T

    def couple_set(level):
        n = nb[level + 1]
        ra, rb = m["ra", level], m["rb", level]
        idx = far % n
        rb[:, pl.ds(idx, 1), :] = ra[:, pl.ds(idx, 1), :]
        return (
            ("rb", level),
            lambda q: ra.at[:, pl.ds(q, 1)],
            lambda i: rb.at[:, pl.ds(i, 1)],
            rb.at[:, pl.ds(0, n - 1)],
        )

    arrive("la")
    m["tl"][...] = transposed(m["la"][...].reshape(NEAR * count, LANES))
    for level in (1, 2):
        arrive(("ra", level))
        fan(nb[level + 1], NEAR, forward_rows(level, "tl", ("lb", level), ("lb", level)), couple_set(level))
    arrive("xr2")
    m["xb2"][far % ring] = jnp.sum(m["xr2"][...], axis=0)
    spread_own("xb2", ring, NEAR)
    arrive("xb1")
    m["xg1"][near] = jnp.sum(m["xb1"][...], axis=0)
    spread_own("xg1", NEAR, 1)
    spread_own("zx", four, 1)
    spread_own("c0", four, 1)

    def build(level):
        n = nb[level + 1]
        wide = 2 * LANES if level == 1 else LANES
        arrive(("lb", level))
        lb = m["lb", level][...]
        lane = lax.broadcasted_iota(jnp.int32, (n, wide), 1).astype(F32)
        at = 2 - level
        hits = [(lane == lb[:, k * count + at : k * count + at + 1]).astype(F32) for k in range(NEAR)]
        m["ohf", level][...] = jnp.concatenate(hits, axis=1).astype(BF16)
        m["ohg", level][...] = jnp.concatenate(hits, axis=0).astype(BF16)
        arrive(("rb", level))
        half = n // 2
        for child in range(2):
            rows = slice(child * half, (child + 1) * half)
            got = m["rb", level][:, rows, :].reshape(NEAR * half, RANK)
            hot = jnp.concatenate([hit[rows] for hit in hits], axis=0).astype(BF16)
            hi, lo = [once(piece, hot, 0, 0) for piece in halves(got)]
            gh, gl = halves(hi + lo)
            out = slice(child * RANK, (child + 1) * RANK)
            m[("g", level), "h"][out, :] = gh
            m[("g", level), "l"][out, :] = gl

    def send_up(level, b, u):
        count_tiles, per = tiles_of(level)
        both = times(b, kept(("qw", level)), 0)
        tile = pick(u, m["h", level][...])
        for t in range(count_tiles):
            m["fs", level][t] = jnp.concatenate(
                [both[:, :RANK], both[:, RANK:], tile[:, t * LANES : (t + 1) * LANES]], axis=0
            )
        fs, fa = m["fs", level], m["fa", level]
        fa[near] = fs[near // per]
        fan_near(("fa", level), lambda q: fs.at[q // per], fa)

    def rows_of(level, kind, tiles):
        n = nb[level + 1]
        table = m["t" + kind, level]
        table[...] = transposed(tiles.reshape(NEAR * count, LANES))
        return table[pl.ds(pl.multiple_of(near % tiles_of(level)[1] * n, 8), n), :]

    def send_far(level, kind, first, second, rows):
        n = nb[level + 1]
        half = n // 2
        idx = far % n
        source, got = m[kind + "s", level], m[kind + "b", level]
        source[:half, :count, :] = jnp.broadcast_to(first[None], (half, count, RANK))
        source[half:, :count, :] = jnp.broadcast_to(second[None], (half, count, RANK))
        source[:, count, :] = rows
        used = pl.ds(0, count + 1)
        got[idx, : count + 1, :] = source[idx, : count + 1, :]
        fan(
            n,
            NEAR,
            (
                (kind, level),
                lambda q: source.at[q, used],
                lambda i: got.at[i, used],
                got.at[pl.ds(0, n - 1), used],
            ),
        )

    def send_on(level):
        arrive(("fa", level))
        fa = m["fa", level]
        tot = jnp.sum(fa[:, : 2 * count, :], axis=0)
        hq = tot[:count] * head[level]
        w = tot[count:] + times(hq, kept(("cross", level)), 0)
        send_far(level, "w", w, w, rows_of(level, "w", fa[:, 2 * count :, :]))
        m["hb", level][far % nb[level]] = hq
        spread_own(("hb", level), nb[level], NEAR)

    def receive_up(level):
        n = nb[level + 1]
        half = n // 2
        arrive(("w", level))
        wb = m["wb", level]
        ws = []
        for child in range(2):
            mc = below[level][child]
            ws.append(jnp.sum(wb[child * half : (child + 1) * half, :count, :], axis=0) * mc)
        inc = -times(jnp.concatenate(ws, axis=1), kept(("g", level)), 0)
        return inc + spread(wb[:, count, :], m["ohf", level][...], NEAR, count)

    def near_sum(name):
        arrive(name)
        return jnp.sum(m[name][...], axis=0)

    def send_down(level, full):
        count_tiles, per = tiles_of(level)
        sp = times(full, kept(("g", level)), 1)
        tile = pick(full, m["ohg", level][...])
        for t in range(count_tiles):
            m["bs", level][t] = jnp.concatenate(
                [sp[:, :RANK], sp[:, RANK:], tile[:, t * LANES : (t + 1) * LANES]], axis=0
            )
        bs, ba = m["bs", level], m["ba", level]
        ba[near] = bs[near // per]
        fan_near(("ba", level), lambda q: bs.at[q // per], ba)

    def send_further(level):
        arrive(("ba", level))
        ba = m["ba", level]
        tot = jnp.sum(ba[:, : 2 * count, :], axis=0)
        send_far(level, "s", tot[:count], tot[count:], rows_of(level, "s", ba[:, 2 * count :, :]))

    def receive_down(level, base):
        arrive(("s", level))
        sb = m["sb", level]
        s = jnp.sum(sb[:, :count, :], axis=0) * side[level]
        x = base - times(s, kept(("t", level)), 1)
        xu = spread(sb[:, count, :], m["ohr", level][...], NEAR, count)
        return x, xu

    saved = {}

    def solve_front(level, local):
        arrive(("hb", level))
        hq = jnp.sum(m["hb", level][...], axis=0)
        z = (local + outer(hq, exp[level][...])) * piv[level][...]
        saved[level] = z
        m["za", level][near] = mult(z, exp[level][...])
        spread_own(("za", level), NEAR, 1)

    def pass_zp(level):
        m["zb", level][far % nb[level]] = near_sum(("za", level))
        spread_own(("zb", level), nb[level], NEAR)

    def base_of(level, zp):
        return outer(saved[level], blk[level][...]) + outer(zp * head[level], q_of(level))

    def tail_of(level, wv):
        qm = q_of(level) * jnp.broadcast_to(head[level][:1], (LANES, RANK))
        keep(("t", level), wv + times(qm, kept(("cross", level)), 0))

    def wv_of(level):
        qh, ql = kept(("qw", level))
        return qh[:, RANK:].astype(F32) + ql[:, RANK:].astype(F32)

    arrive("r0")
    r0 = m["r0"][...]
    lane = lax.broadcasted_iota(jnp.int32, (plane, 2 * LANES), 1).astype(F32)
    at = cap * count
    m["oh0"][...] = jnp.concatenate(
        [(lane == r0[:, at + s : at + s + 1]).astype(F32) for s in range(cap)], axis=1
    ).astype(BF16)
    inc = spread(r0, m["oh0"][...], cap, count)
    b1 = src[1][...] + inc[:, :LANES]
    send_up(1, b1, inc[:, LANES:])

    local1 = mult(b1, blk[1][...])
    saved[0] = z0
    arrive("zx")
    base0 = base_of(0, jnp.sum(m["zx"][...], axis=0))
    build(1)
    arrive("xg1")
    keep(("cross", 1), m["xg1"][...].reshape(RANK, RANK))
    build(2)
    kh, kl = kept(("qw", 3))
    hot, gh, gl = m["ohg", 2][...], *kept(("g", 2))
    m["kp"][...] = (once(hot, kh, 1, 0) + once(hot, kl, 1, 0)).reshape(NEAR, fars, 2 * RANK)
    scatter_near("kr", "kp")
    arrive("xb2")
    m["xy"][me // plane] = jnp.sum(m["xb2"][...], axis=0)
    spread_own("xy", total_devices // plane, plane)
    send_on(1)
    both = once(gh, kh, 1, 0) + (once(gl, kh, 1, 0) + once(gh, kl, 1, 0))
    m["yp"][...] = both.reshape(NEAR, 2 * RANK // NEAR, 2 * RANK)
    scatter_near("yr", "yp")

    arrive("xy")
    pair = me // plane // 2 * 2
    m["xg2"][near, :slice_rows, :] = jnp.sum(m["xy"][pl.ds(pair, 2), :slice_rows, :], axis=0)
    m["xg2"][near, slice_rows:, :] = jnp.sum(m["xy"][:, slice_rows:, :], axis=0)
    spread_own("xg2", NEAR, 1)
    tail_of(1, wv_of(1))

    inc = receive_up(1)
    b2 = src[2][...] + inc[:, :LANES]
    send_up(2, b2, inc[:, LANES:])

    local2 = mult(b2, blk[2][...])
    arrive("xg2")
    keep(("cross", 2), m["xg2"][:, :slice_rows, :].reshape(RANK, RANK))
    send_on(2)
    m["yg"][near] = near_sum("yr")
    spread_own("yg", NEAR, 1)
    keep(("cross", 3), m["xg2"][:, slice_rows:, :].reshape(RANK, RANK))
    root_qm = q_of(3) * jnp.broadcast_to(head[3][:1], (LANES, RANK))
    root_t = wv_of(3) + times(root_qm, kept(("cross", 3)), 0)
    keep(("qt", 3), jnp.concatenate([root_qm, root_t], axis=1))
    solve_front(1, local1)
    tail_of(2, wv_of(2))

    b3 = src[3][...] + receive_up(2)
    both = times(b3, kept(("qt", 3)), 0)
    core = near // across
    m["fs3"][0] = both[:, :RANK]
    m["fs3"][1] = both[:, RANK:]
    m["fa", 3][near] = m["fs3"][core]
    fan_near(("fa", 3), lambda q: m["fs3"].at[q // across], m["fa", 3])
    early = outer(mult(b3, blk[3][...]) * piv[3][...], blk[3][...])
    send_down(2, early)
    solve_front(2, local2)
    pass_zp(1)
    m["fb"][far] = near_sum(("fa", 3))
    spread_own("fb", fars, NEAR)
    arrive("c0")
    keep(("cross", 0), jnp.sum(m["c0"][...], axis=0))
    tail_of(0, mult(blk[0][...], v_of(0)))
    arrive(("ba", 2))
    ba = m["ba", 2]
    sums = jnp.sum(ba[:, : 2 * count, :], axis=0)
    early_rows = rows_of(2, "s", ba[:, 2 * count :, :])
    pass_zp(2)
    arrive("yg")
    arrive("kr")
    keep("ka", m["kr"][...].reshape(NEAR * fars, 2 * RANK))
    keep("y", m["yg"][...].reshape(2 * RANK, 2 * RANK))
    arrive(("zb", 1))
    base1 = base_of(1, jnp.sum(m["zb", 1][...], axis=0))
    arrive("fb")
    m["fc"][core] = jnp.sum(m["fb"][...], axis=0)
    spread_own("fc", 2, across)
    arrive("fc")
    ends = jnp.concatenate([m["fc"][1] * head[3], m["fc"][0]], axis=1)
    sums = jnp.concatenate([sums[:count], sums[count:]], axis=1) + times(ends, kept("y"), 1)
    late = times(ends, kept("ka"), 1)
    per = LANES // fars
    late = [
        pltpu.roll(late[:, k // per * LANES : (k // per + 1) * LANES], (LANES - k % per * fars) % LANES, 1)
        for k in range(NEAR)
    ]
    late = transposed(jnp.concatenate(late, axis=0))[:fars]
    send_far(2, "s", sums[:, :RANK], sums[:, RANK:], early_rows + late)
    spread_own("hx", four, 1)
    outs[3][...] = early + times(ends, kept(("qw", 3)), 1)

    arrive(("zb", 2))
    base2 = base_of(2, jnp.sum(m["zb", 2][...], axis=0))
    x, xu = receive_down(2, base2)
    send_down(1, jnp.concatenate([x, xu], axis=1))
    outs[2][...] = x
    send_further(1)
    arrive("hx")
    for k in range(four):
        at = slice(k * cap * plane, (k + 1) * cap * plane)
        m["hxh"][at, :], m["hxl"][at, :] = halves(m["hx"][k])
    x, xu = receive_down(1, base1)
    full = diagonal(jnp.concatenate([x, xu], axis=1), cap, four)
    rows = leaf_rows((m["oh0"][...], None), full)
    ri = lax.broadcasted_iota(jnp.int32, (plane, LANES), 0)
    li = lax.broadcasted_iota(jnp.int32, (plane, LANES), 1)
    rows = jnp.where(li // (cap * count) == ri % four, rows, 0.0)
    rows = rows + pltpu.roll(rows, plane - 1, 0)
    m["s0b"][...] = rows + pltpu.roll(rows, plane - 2, 0)
    send_leaf("s0b", "r0b", lambda q: q // four * four)
    outs[1][...] = x
    arrive("r0b")
    rows = transposed(m["r0b"][...])
    pieces = [rows[g * count : (g + 1) * count] for g in range(four * cap)]
    pairs = [pieces[2 * g] + pltpu.roll(pieces[2 * g + 1], plane, 1) for g in range(four * cap // 2)]
    s = times(jnp.concatenate(pairs, axis=1), (m["hxh"][...], m["hxl"][...]), 0) * side[0]
    outs[0][...] = base0 - times(s, kept(("t", 0)), 1)

    for name, part in parts.items():
        wait_for(part, send_sem.at[sem_of(name)])


def solution(mesh):
    leaves, across = mesh.shape["leaf"], mesh.shape["grid"]

    def shards(*args):
        levels = [args[8 * i : 8 * i + 8] for i in range(3)]
        root = args[24:30]
        (sl, bl, el, qs, pv, cl, rk, tg) = zip(*levels)
        src = list(sl) + [root[0]]
        blk = list(bl) + [root[1]]
        exp = list(el) + [root[2]]
        bas = list(qs) + [root[3]]
        piv = [v.reshape(1, -1) for v in list(pv) + [root[4]]]
        rnk = [rk[0].T, rk[1].T, rk[2], root[5]]
        tgt = [t.reshape(1, -1) for t in tg]
        count = src[0].shape[0]
        ups = [t.shape[1] for t in tgt]
        fronts = [r.shape[0] for r in rk] + [root[5].shape[0]]
        size = [leaves * across // f for f in fronts]
        cap = ups[0] // size[1]
        nb = [s // NEAR for s in size]
        for v in src:
            assert v.shape == (NEAR, LANES)
        assert ups[1:] == [LANES, LANES] and cap * (count + 1) <= LANES
        assert 2 * size[1] == LANES and size[0] * cap * count == LANES
        assert nb[1] == 8 and across == 4 and size[0] == across
        assert size[2] == 2 * size[1] and size[3] == 2 * size[2] and size[1] % NEAR == 0
        assert NEAR * nb[2] == LANES and NEAR * nb[3] == 2 * LANES
        vm = lambda *s: pltpu.VMEM(s, F32)
        bits = lambda *s: pltpu.VMEM(s, BF16)
        piece = RANK // NEAR
        bufs = {
            "f1": vm(size[0], count, LANES),
            "fv": vm(size[0], count, LANES),
            "c0": vm(size[0], RANK, RANK),
            "zx": vm(size[0], count, LANES),
            "xp1": vm(NEAR, piece, RANK),
            "xr1": vm(NEAR, piece, RANK),
            "xp2": vm(NEAR, 2 * piece, RANK),
            "xr2": vm(NEAR, 2 * piece, RANK),
            "xb1": vm(nb[1], piece, RANK),
            "xb2": vm(nb[1], 2 * piece, RANK),
            "xy": vm(nb[3] // nb[1], 2 * piece, RANK),
            "xg1": vm(NEAR, piece, RANK),
            "xg2": vm(NEAR, 2 * piece, RANK),
            "lows": vm(2, count, LANES),
            "la": vm(NEAR, count, LANES),
            "tl": vm(LANES, LANES),
            "hch": bits(size[1], cap * RANK),
            "hcl": bits(size[1], cap * RANK),
            "low0": vm(size[1], LANES),
            "oh0": bits(size[1], cap * 2 * LANES),
            "fb": vm(nb[3], count, LANES),
            "fs3": vm(2, count, LANES),
            "kp": vm(NEAR, nb[3], 2 * RANK),
            "kr": vm(NEAR, nb[3], 2 * RANK),
            "yp": vm(NEAR, 2 * RANK // NEAR, 2 * RANK),
            "yr": vm(NEAR, 2 * RANK // NEAR, 2 * RANK),
            "yg": vm(NEAR, 2 * RANK // NEAR, 2 * RANK),
            "fc": vm(2, count, LANES),
            "hx": vm(size[0], cap * size[1], RANK),
            "hxh": bits(size[0] * cap * size[1], RANK),
            "hxl": bits(size[0] * cap * size[1], RANK),
        }
        for name in ("s0", "r0", "s0b", "r0b"):
            bufs[name] = vm(size[1], LANES)
        for half in "hl":
            bufs["ka", half] = bits(NEAR * nb[3], 2 * RANK)
            bufs["y", half] = bits(2 * RANK, 2 * RANK)
        for i in range(4):
            for half in "hl":
                bufs[("cross", i), half] = bits(RANK, RANK)
                bufs[("qw", i), half] = bits(LANES, 2 * RANK)
                bufs[("t", i), half] = bits(LANES, RANK)
                bufs[("qt", i), half] = bits(LANES, 2 * RANK)
        bufs["fa", 3] = vm(NEAR, count, LANES)
        for i in (1, 2):
            n = nb[i + 1]
            wide = 2 * LANES if i == 1 else LANES
            tiles = NEAR * n // LANES
            bufs["h", i] = bits(NEAR * n, LANES)
            bufs["ohr", i] = bits(n, NEAR * LANES)
            bufs["ohf", i] = bits(n, NEAR * wide)
            bufs["ohg", i] = bits(NEAR * n, wide)
            bufs["pa", i] = vm(NEAR, n, RANK)
            bufs["ra", i] = vm(NEAR, n, RANK)
            bufs["rb", i] = vm(NEAR, n, RANK)
            bufs["lb", i] = vm(n, LANES)
            for half in "hl":
                bufs[("g", i), half] = bits(2 * RANK, wide)
            bufs["fs", i] = vm(tiles, 3 * count, LANES)
            bufs["fa", i] = vm(NEAR, 3 * count, LANES)
            bufs["bs", i] = vm(tiles, 3 * count, LANES)
            bufs["ba", i] = vm(NEAR, 3 * count, LANES)
            for kind in "ws":
                bufs["t" + kind, i] = vm(LANES, LANES)
                bufs[kind + "s", i] = vm(n, 2 * count, LANES)
                bufs[kind + "b", i] = vm(n, 2 * count, LANES)
            bufs["hb", i] = vm(nb[i], count, LANES)
            bufs["za", i] = vm(NEAR, count, LANES)
            bufs["zb", i] = vm(nb[i], count, LANES)
        arrays = [*src, *blk, *exp, *bas, *piv, *cl, *tgt, *rnk]
        for i, v in enumerate(arrays):
            bufs["in", i] = pltpu.VMEM(v.shape, v.dtype)
        scratch = list(bufs.values())
        scratch += [
            pltpu.SemaphoreType.DMA((48,)),
            pltpu.SemaphoreType.DMA((48,)),
            pltpu.SemaphoreType.DMA((30,)),
            pltpu.SemaphoreType.REGULAR,
        ]
        vspec = pl.BlockSpec(memory_space=pltpu.VMEM)
        whole = pl.pallas_call(
            functools.partial(kernel, (leaves, across, size, ups, count, cap), list(bufs)),
            out_shape=jax.ShapeDtypeStruct((4 * count, LANES), F32),
            in_specs=[pl.BlockSpec(memory_space=pl.ANY)] * 30,
            out_specs=vspec,
            scratch_shapes=scratch,
            compiler_params=pltpu.CompilerParams(
                collective_id=0, has_side_effects=True, vmem_limit_bytes=60 * 1024 * 1024
            ),
        )(*arrays)
        return tuple(whole[i * count : (i + 1) * count] for i in range(4))

    spread_axes = ("leaf", "grid")
    level = (P(None, spread_axes), P(spread_axes, None), P(spread_axes, None), P(spread_axes, None), P(spread_axes))
    mid = level + (P(spread_axes, None), P(), P(spread_axes))
    return jax.shard_map(
        shards,
        mesh=mesh,
        in_specs=mid * 3 + level + (P(),),
        out_specs=(P(None, spread_axes),) * 4,
        check_vma=False,
    )
```

```python
import functools

import jax
import jax.numpy as jnp
from jax import lax
from jax.experimental import pallas as pl
from jax.experimental.pallas import tpu as pltpu
from jax.sharding import PartitionSpec as P

RANK = 128
LANES = 128
NEAR = 8
LOGICAL = pl.DeviceIdType.LOGICAL
F32 = jnp.float32
BF16 = jnp.bfloat16


def once(a, b, ca, cb):
    return lax.dot_general(a, b, (((ca,), (cb,)), ((), ())), preferred_element_type=F32)


def halves(x):
    hi = x.astype(BF16)
    return hi, (x - hi.astype(F32)).astype(BF16)


def stacked(x):
    hi = x.astype(BF16).astype(F32)
    return jnp.concatenate([hi, x - hi], axis=0).astype(BF16)


def times(a, b, cb):
    bh, bl = b
    n = a.shape[0]
    both = once(stacked(a), bh, 1, cb)
    return both[:n] + (both[n:] + once(a.astype(BF16), bl, 1, cb))


def mult(a, b):
    return times(a, halves(b), 0)


def outer(a, b):
    return times(a, halves(b), 1)


def inner(a, b):
    ah, al = halves(a)
    bh, bl = halves(b)
    return once(ah, bh, 0, 0) + (once(al, bh, 0, 0) + once(ah, bl, 0, 0))


def pick(x, onehot):
    n = x.shape[0]
    both = once(stacked(x), onehot, 1, 1)
    return both[:n] + both[n:]


def spread(rows, onehot, groups, count):
    m = groups * count
    wide = onehot.shape[1] // groups
    both = once(stacked(rows.T[:m]), onehot, 1, 0)
    out = None
    for g in range(groups):
        lanes = slice(g * wide, (g + 1) * wide)
        part = both[g * count : (g + 1) * count, lanes] + both[m + g * count : m + (g + 1) * count, lanes]
        out = part if out is None else out + part
    return out


def diagonal(x, groups, again=1):
    count, wide = x.shape
    zero = jnp.zeros((count, wide), F32)
    rows = [
        jnp.concatenate([x if h == g else zero for h in range(groups)], axis=1) for g in range(groups)
    ]
    rows = rows * again
    left = LANES - len(rows) * count
    if left:
        rows.append(jnp.zeros((left, groups * wide), F32))
    return jnp.concatenate(rows, axis=0)


def kernel(cfg, names, *refs):
    leaves, across, size, ups, count, cap = cfg
    total_devices = leaves * across
    count_in = 30
    given, out = refs[:count_in], refs[count_in]
    outs = [out.at[pl.ds(i * count, count)] for i in range(4)]
    m = dict(zip(names, refs[count_in + 1 : -4]))
    send_sem, recv_sem, load_sem, ready = refs[-4:]
    held = [m["in", i] for i in range(count_in)]
    (src, blk, exp, bas, piv) = [held[4 * i : 4 * i + 4] for i in range(5)]
    cpl, tgt, rnk = held[20:23], held[23:26], held[26:30]
    loads = [pltpu.make_async_copy(given[i], held[i], load_sem.at[i]) for i in range(count_in)]
    sems = {}
    parts = {}

    me = lax.axis_index("leaf") * across + lax.axis_index("grid")
    near = me % NEAR
    far = me // NEAR
    nb = [s // NEAR for s in size]
    plane = size[1]
    fars = nb[3]

    def sem_of(name):
        return sems.setdefault(name, len(sems))

    def remote(a, b, sem, peer):
        return pltpu.make_async_remote_copy(
            src_ref=a,
            dst_ref=b,
            send_sem=send_sem.at[sem],
            recv_sem=recv_sem.at[sem],
            device_id=peer,
            device_id_type=LOGICAL,
        )

    def wait_for(part, sem):
        pltpu.make_async_copy(part, part, sem).wait()

    ring = nb[1]

    def farthest(n):
        return sorted(range(n), key=lambda d: -min(d, n - d))

    def fan(group, stride, *sets):
        idx = me // stride % group
        base = me - idx * stride
        for name, source, dest, part in sets:
            sem_of(name)
            parts[name] = part

        def go(q):
            for name, source, dest, part in sets:
                remote(source(q), dest(idx), sem_of(name), base + q * stride).start()

        if stride == NEAR:
            rows = group // ring
            for dy in farthest(rows):
                line = (idx // ring + dy) % rows * ring
                for dz in farthest(ring):
                    if dy or dz:
                        go(line + (idx + dz) % ring)
        elif group == plane:
            for dz in farthest(ring)[:-1]:
                line = (idx // NEAR + dz) % ring * NEAR

                def body(k, carry, line=line):
                    go(line + k)
                    return carry

                lax.fori_loop(0, NEAR, body, 0, unroll=True)
            for k in range(1, NEAR):
                go(idx // NEAR * NEAR + (idx + k) % NEAR)
        elif group == NEAR:
            for dx in farthest(across):
                for dc in (1, 0):
                    if dx or dc:
                        go((idx // across + dc) % 2 * across + (idx + dx) % across)
        else:
            for d in farthest(group)[:-1]:
                go((idx + d) % group)

    def arrive(name):
        wait_for(parts[name], recv_sem.at[sem_of(name)])

    def slots(name, group):
        buf = m[name]
        return buf.at[pl.ds(0, group - 1)]

    def spread_own(name, group, stride):
        buf = m[name]
        idx = me // stride % group
        fan(group, stride, (name, lambda q: buf.at[idx], lambda i: buf.at[i], slots(name, group)))

    barrier = pltpu.get_barrier_semaphore()

    def greet_near(sem):
        def body(k, carry):
            peer = far * NEAR + (near + k) % NEAR
            pl.semaphore_signal(sem, inc=1, device_id=peer, device_id_type=LOGICAL)
            return carry

        lax.fori_loop(1, NEAR, body, 0)

    def greet_far(k, carry):
        peer = (far + k) % fars * NEAR + near
        pl.semaphore_signal(barrier, inc=1, device_id=peer, device_id_type=LOGICAL)
        return carry

    lax.fori_loop(1, fars, greet_far, 0)
    greet_near(barrier)
    soon = (0, 12)
    rest = [i for i in range(count_in) if i not in soon]
    for i in soon + tuple(rest):
        loads[i].start()

    def mask(level, which, front):
        ranks = rnk[level][...].astype(F32)
        axis = 1 if level < 2 else 0
        line = ranks[which : which + 1, :] if level < 2 else ranks[:, which : which + 1]
        here = lax.broadcasted_iota(jnp.int32, line.shape, axis) == front
        rank = jnp.sum(jnp.where(here, line, 0.0), axis=axis, keepdims=True)
        col = lax.broadcasted_iota(jnp.int32, (count, RANK), 1).astype(F32)
        return (col < rank).astype(F32)

    def q_of(level):
        return bas[level][:, :RANK]

    def v_of(level):
        return bas[level][:, RANK:]

    def tiles_of(level):
        n = nb[level + 1]
        return NEAR * n // LANES, LANES // n

    four = size[0]
    my4 = me % four
    for i in soon:
        loads[i].wait()
    s0 = src[0][...]
    m["f1"][my4] = mult(s0, q_of(0))
    pl.semaphore_wait(barrier, NEAR - 1 + fars - 1)
    greet_near(ready)
    spread_own("f1", four, 1)
    for i in rest:
        loads[i].wait()
    front = [me // n for n in size]
    head = [mask(level, 0, front[level]) for level in range(4)]
    side = [mask(level, 1, front[level]) for level in range(3)]
    below = [None] + [
        [mask(level, 1, front[level + 1] * 2 + child) for child in range(2)] for level in (1, 2)
    ]
    local0 = mult(s0, blk[0][...])
    m["c0"][my4] = inner(exp[0][...], v_of(0))

    slice_rows = RANK // NEAR
    root_piv = jnp.broadcast_to(piv[3][...], (LANES, LANES)).T
    crosses = [
        inner(exp[1][...], v_of(1)),
        inner(exp[2][...], v_of(2)),
        inner(exp[3][...] * root_piv, exp[3][...]),
    ]
    for j, cross in enumerate(crosses):
        buf, at = (m["xp1"], 0) if j == 0 else (m["xp2"], (j - 1) * slice_rows)
        buf[:, at : at + slice_rows, :] = cross.reshape(NEAR, slice_rows, RANK)

    def split_targets(level):
        sep = size[level + 1] * LANES
        t = tgt[level][...]
        upd = t >= sep
        rel = jnp.where(upd, t - sep, t)
        return rel // LANES, rel % LANES + jnp.where(upd, LANES, 0)

    def pack_leaf():
        u = ups[0]
        dst, low = split_targets(0)
        ri = lax.broadcasted_iota(jnp.int32, (u, u), 0)
        ci = lax.broadcasted_iota(jnp.int32, (u, u), 1)
        dst_f = dst.astype(F32)
        dst_c = jnp.sum(jnp.where(ri == ci, jnp.broadcast_to(dst_f, (u, u)), 0.0), axis=1, keepdims=True)
        rank = jnp.sum(
            jnp.where((dst_c == dst_f) & (ri < ci), 1.0, 0.0), axis=0, keepdims=True
        ).astype(jnp.int32)
        slot = rank * plane + dst
        ch, cl = halves(cpl[0][...])
        lowmat = None
        li = lax.broadcasted_iota(jnp.int32, (LANES, u), 0)
        for s in range(cap):
            si = lax.broadcasted_iota(jnp.int32, (plane, u), 0) + s * plane
            hit = (si == slot).astype(F32).astype(BF16)
            lanes = slice(s * RANK, (s + 1) * RANK)
            high, low_part = once(hit, ch, 1, 0), once(hit, cl, 1, 0)
            m["hch"][:, lanes] = high.astype(BF16)
            m["hcl"][:, lanes] = low_part.astype(BF16)
            m["hx"][my4, s * plane : (s + 1) * plane, :] = high + low_part
            mine = jnp.where(li == cap * count + s, low.astype(F32), 0.0).astype(BF16)
            part = once(hit, mine, 1, 1)
            lowmat = part if lowmat is None else lowmat + part
        m["low0"][...] = lowmat

    def pack_couple(level):
        n = nb[level + 1]
        dst, low = split_targets(level)
        slot = dst % NEAR * n + dst // NEAR
        si = lax.broadcasted_iota(jnp.int32, (NEAR * n, LANES), 0)
        h = (si == slot).astype(F32).astype(BF16)
        m["h", level][...] = h
        hi, lo = [once(h, piece, 1, 0) for piece in halves(cpl[level][...])]
        m["pa", level][...] = (hi + lo).reshape(NEAR, n, RANK)
        rows = jnp.broadcast_to(low, (count, LANES)).astype(F32).astype(BF16)
        bi = lax.broadcasted_iota(jnp.int32, (n, LANES), 0) * NEAR
        m["ohr", level][...] = jnp.concatenate(
            [(bi + k == dst).astype(F32) for k in range(NEAR)], axis=1
        ).astype(BF16)
        return once(rows, h, 1, 1)

    low1, low2 = pack_couple(1), pack_couple(2)
    ri = lax.broadcasted_iota(jnp.int32, (count, LANES), 0)
    for t in range(2):
        two = low2[:, t * LANES : (t + 1) * LANES]
        m["lows"][t] = jnp.where(ri == 0, two, jnp.where(ri == 1, low1, 0.0))
    pack_leaf()

    def fan_near(name, source, dest):
        fan(NEAR, 1, (name, source, lambda i: dest.at[i], dest.at[pl.ds(0, NEAR - 1)]))

    def scatter_near(name, source):
        m[name][near] = m[source][near]
        fan_near(name, lambda q: m[source].at[q], m[name])

    scatter_near("xr1", "xp1")
    m["la"][near] = m["lows"][near // 4]
    fan_near("la", lambda q: m["lows"].at[q // 4], m["la"])
    scatter_near(("ra", 1), ("pa", 1))

    def keep(name, value):
        hi, lo = halves(value)
        m[name, "h"][...] = hi
        m[name, "l"][...] = lo

    def kept(name):
        return m[name, "h"][...], m[name, "l"][...]

    for level in (1, 2):
        wv = mult(blk[level][...], v_of(level))
        keep(("qw", level), jnp.concatenate([q_of(level), wv], axis=1))
    wpp = mult(blk[3][...] * piv[3][...], exp[3][...])
    keep(("qw", 3), jnp.concatenate([q_of(3), wpp], axis=1))

    arrive("f1")
    hq0 = jnp.sum(m["f1"][...], axis=0) * head[0]
    y0 = local0 + outer(hq0, exp[0][...])
    m["fv"][my4] = mult(y0, v_of(0))
    spread_own("fv", four, 1)
    scatter_near(("ra", 2), ("pa", 2))
    scatter_near("xr2", "xp2")
    z0 = y0 * piv[0][...]
    m["zx"][my4] = mult(z0, exp[0][...])
    arrive("xr1")
    m["xb1"][far % ring] = jnp.sum(m["xr1"][...], axis=0)
    spread_own("xb1", ring, NEAR)
    arrive("fv")
    w0 = jnp.sum(m["fv"][...], axis=0) * side[0]

    def leaf_rows(a, b):
        ah, al = a
        bh, bl = halves(b)
        out = once(ah, bh, 1, 1) + once(ah, bl, 1, 1)
        return out if al is None else out + once(al, bh, 1, 1)

    place = me % plane

    def send_leaf(rows, got, row):
        m[got][pl.ds(place, 1), :] = m[rows][pl.ds(row(place), 1), :]
        fan(
            plane,
            1,
            (
                got,
                lambda q: m[rows].at[pl.ds(row(q), 1)],
                lambda i: m[got].at[pl.ds(i, 1)],
                m[got].at[pl.ds(0, plane - 1)],
            ),
        )

    hc = (m["hch"][...], m["hcl"][...])
    m["s0"][...] = leaf_rows(hc, diagonal(-w0, cap)) + m["low0"][...]
    pl.semaphore_wait(ready, NEAR - 1)
    send_leaf("s0", "r0", lambda q: q)

    def store_row(buf, i, row):
        buf[pl.ds(i, 1), :] = row

    def forward_rows(level, table, got, name):
        n = nb[level + 1]
        per = tiles_of(level)[1]
        idx = far % n
        first = near % per * n
        store_row(m[got], idx, m[table][pl.ds(first + idx, 1), :])
        return (
            name,
            lambda q: m[table].at[pl.ds(first + q, 1)],
            lambda i: m[got].at[pl.ds(i, 1)],
            m[got].at[pl.ds(0, n - 1)],
        )

    def transposed(x):
        return jnp.concatenate([x, jnp.zeros((LANES - x.shape[0], LANES), F32)], axis=0).T

    def couple_set(level):
        n = nb[level + 1]
        ra, rb = m["ra", level], m["rb", level]
        idx = far % n
        rb[:, pl.ds(idx, 1), :] = ra[:, pl.ds(idx, 1), :]
        return (
            ("rb", level),
            lambda q: ra.at[:, pl.ds(q, 1)],
            lambda i: rb.at[:, pl.ds(i, 1)],
            rb.at[:, pl.ds(0, n - 1)],
        )

    arrive("la")
    m["tl"][...] = transposed(m["la"][...].reshape(NEAR * count, LANES))
    for level in (1, 2):
        arrive(("ra", level))
        fan(nb[level + 1], NEAR, forward_rows(level, "tl", ("lb", level), ("lb", level)), couple_set(level))
    arrive("xr2")
    m["xb2"][far % ring] = jnp.sum(m["xr2"][...], axis=0)
    spread_own("xb2", ring, NEAR)
    arrive("xb1")
    m["xg1"][near] = jnp.sum(m["xb1"][...], axis=0)
    spread_own("xg1", NEAR, 1)
    spread_own("zx", four, 1)
    spread_own("c0", four, 1)

    def build(level):
        n = nb[level + 1]
        wide = 2 * LANES if level == 1 else LANES
        arrive(("lb", level))
        lb = m["lb", level][...]
        lane = lax.broadcasted_iota(jnp.int32, (n, wide), 1).astype(F32)
        at = 2 - level
        hits = [(lane == lb[:, k * count + at : k * count + at + 1]).astype(F32) for k in range(NEAR)]
        m["ohf", level][...] = jnp.concatenate(hits, axis=1).astype(BF16)
        m["ohg", level][...] = jnp.concatenate(hits, axis=0).astype(BF16)
        arrive(("rb", level))
        half = n // 2
        for child in range(2):
            rows = slice(child * half, (child + 1) * half)
            got = m["rb", level][:, rows, :].reshape(NEAR * half, RANK)
            hot = jnp.concatenate([hit[rows] for hit in hits], axis=0).astype(BF16)
            hi, lo = [once(piece, hot, 0, 0) for piece in halves(got)]
            gh, gl = halves(hi + lo)
            out = slice(child * RANK, (child + 1) * RANK)
            m[("g", level), "h"][out, :] = gh
            m[("g", level), "l"][out, :] = gl

    def send_up(level, b, u):
        count_tiles, per = tiles_of(level)
        both = times(b, kept(("qw", level)), 0)
        tile = pick(u, m["h", level][...])
        for t in range(count_tiles):
            m["fs", level][t] = jnp.concatenate(
                [both[:, :RANK], both[:, RANK:], tile[:, t * LANES : (t + 1) * LANES]], axis=0
            )
        fs, fa = m["fs", level], m["fa", level]
        fa[near] = fs[near // per]
        fan_near(("fa", level), lambda q: fs.at[q // per], fa)

    def rows_of(level, kind, tiles):
        n = nb[level + 1]
        table = m["t" + kind, level]
        table[...] = transposed(tiles.reshape(NEAR * count, LANES))
        return table[pl.ds(pl.multiple_of(near % tiles_of(level)[1] * n, 8), n), :]

    def send_far(level, kind, first, second, rows):
        n = nb[level + 1]
        half = n // 2
        idx = far % n
        source, got = m[kind + "s", level], m[kind + "b", level]
        source[:half, :count, :] = jnp.broadcast_to(first[None], (half, count, RANK))
        source[half:, :count, :] = jnp.broadcast_to(second[None], (half, count, RANK))
        source[:, count, :] = rows
        used = pl.ds(0, count + 1)
        got[idx, : count + 1, :] = source[idx, : count + 1, :]
        fan(
            n,
            NEAR,
            (
                (kind, level),
                lambda q: source.at[q, used],
                lambda i: got.at[i, used],
                got.at[pl.ds(0, n - 1), used],
            ),
        )

    def send_on(level):
        arrive(("fa", level))
        fa = m["fa", level]
        tot = jnp.sum(fa[:, : 2 * count, :], axis=0)
        hq = tot[:count] * head[level]
        w = tot[count:] + times(hq, kept(("cross", level)), 0)
        rows = rows_of(level, "w", fa[:, 2 * count :, :])
        send_far(level, "w", w, w, rows)
        m["hb", level][far % nb[level]] = hq
        spread_own(("hb", level), nb[level], NEAR)
        return rows

    def sums_up(level):
        half = nb[level + 1] // 2
        arrive(("w", level))
        wb = m["wb", level]
        ws = [
            jnp.sum(wb[child * half : (child + 1) * half, :count, :], axis=0) * below[level][child]
            for child in range(2)
        ]
        return jnp.concatenate(ws, axis=1)

    def receive_up(level, ws):
        rows = spread(m["wb", level][:, count, :], m["ohf", level][...], NEAR, count)
        return rows - times(ws, kept(("g", level)), 0)

    def near_sum(name):
        arrive(name)
        return jnp.sum(m[name][...], axis=0)

    def send_down(level, full):
        count_tiles, per = tiles_of(level)
        sp = times(full, kept(("g", level)), 1)
        tile = pick(full, m["ohg", level][...])
        for t in range(count_tiles):
            m["bs", level][t] = jnp.concatenate(
                [sp[:, :RANK], sp[:, RANK:], tile[:, t * LANES : (t + 1) * LANES]], axis=0
            )
        bs, ba = m["bs", level], m["ba", level]
        ba[near] = bs[near // per]
        fan_near(("ba", level), lambda q: bs.at[q // per], ba)

    def send_further(level):
        arrive(("ba", level))
        ba = m["ba", level]
        tot = jnp.sum(ba[:, : 2 * count, :], axis=0)
        send_far(level, "s", tot[:count], tot[count:], rows_of(level, "s", ba[:, 2 * count :, :]))

    def receive_down(level, base):
        arrive(("s", level))
        sb = m["sb", level]
        s = jnp.sum(sb[:, :count, :], axis=0) * side[level]
        x = base - times(s, kept(("t", level)), 1)
        xu = spread(sb[:, count, :], m["ohr", level][...], NEAR, count)
        return x, xu

    saved = {}

    def solve_front(level, local):
        arrive(("hb", level))
        hq = jnp.sum(m["hb", level][...], axis=0)
        z = (local + outer(hq, exp[level][...])) * piv[level][...]
        saved[level] = z
        m["za", level][near] = mult(z, exp[level][...])
        spread_own(("za", level), NEAR, 1)

    def pass_zp(level):
        m["zb", level][far % nb[level]] = near_sum(("za", level))
        spread_own(("zb", level), nb[level], NEAR)

    def base_of(level, zp):
        return outer(saved[level], blk[level][...]) + outer(zp * head[level], q_of(level))

    def tail_of(level, wv):
        qm = q_of(level) * jnp.broadcast_to(head[level][:1], (LANES, RANK))
        keep(("t", level), wv + times(qm, kept(("cross", level)), 0))

    def wv_of(level):
        qh, ql = kept(("qw", level))
        return qh[:, RANK:].astype(F32) + ql[:, RANK:].astype(F32)

    arrive("r0")
    r0 = m["r0"][...]
    lane = lax.broadcasted_iota(jnp.int32, (plane, 2 * LANES), 1).astype(F32)
    at = cap * count
    m["oh0"][...] = jnp.concatenate(
        [(lane == r0[:, at + s : at + s + 1]).astype(F32) for s in range(cap)], axis=1
    ).astype(BF16)
    inc = spread(r0, m["oh0"][...], cap, count)
    b1 = src[1][...] + inc[:, :LANES]
    send_up(1, b1, inc[:, LANES:])

    local1 = mult(b1, blk[1][...])
    saved[0] = z0
    arrive("zx")
    base0 = base_of(0, jnp.sum(m["zx"][...], axis=0))
    build(1)
    arrive("xg1")
    keep(("cross", 1), m["xg1"][...].reshape(RANK, RANK))
    build(2)
    kh, kl = kept(("qw", 3))
    hot, gh, gl = m["ohg", 2][...], *kept(("g", 2))
    m["kp"][...] = (once(hot, kh, 1, 0) + once(hot, kl, 1, 0)).reshape(NEAR, fars, 2 * RANK)
    scatter_near("kr", "kp")
    arrive("xb2")
    m["xy"][me // plane] = jnp.sum(m["xb2"][...], axis=0)
    spread_own("xy", total_devices // plane, plane)
    send_on(1)
    both = once(gh, kh, 1, 0) + (once(gl, kh, 1, 0) + once(gh, kl, 1, 0))
    m["yp"][...] = both.reshape(NEAR, 2 * RANK // NEAR, 2 * RANK)
    scatter_near("yr", "yp")
    ks, kb = m["ks"], m["kb"]
    for half in range(2):
        ks[:, half] = m["kp"][:, :, half * RANK : (half + 1) * RANK]
    kb[:, :, pl.ds(far, 1), :] = ks[:, :, pl.ds(far, 1), :]
    fan(
        fars,
        NEAR,
        (
            "kb",
            lambda q: ks.at[:, :, pl.ds(q, 1)],
            lambda i: kb.at[:, :, pl.ds(i, 1)],
            kb.at[:, :, pl.ds(0, fars - 1)],
        ),
    )

    arrive("xy")
    pair = me // plane // 2 * 2
    m["xg2"][near, :slice_rows, :] = jnp.sum(m["xy"][pl.ds(pair, 2), :slice_rows, :], axis=0)
    m["xg2"][near, slice_rows:, :] = jnp.sum(m["xy"][:, slice_rows:, :], axis=0)
    spread_own("xg2", NEAR, 1)
    tail_of(1, wv_of(1))

    inc = receive_up(1, sums_up(1))
    b2 = src[2][...] + inc[:, :LANES]
    send_up(2, b2, inc[:, LANES:])
    m["yg"][near] = near_sum("yr")
    spread_own("yg", NEAR, 1)

    local2 = mult(b2, blk[2][...])
    arrive("xg2")
    keep(("cross", 2), m["xg2"][:, :slice_rows, :].reshape(RANK, RANK))
    rows = send_on(2)
    keep(("cross", 3), m["xg2"][:, slice_rows:, :].reshape(RANK, RANK))
    core = near // across
    per = LANES // fars
    turned = transposed(rows)
    passing = []
    for t in range(NEAR // per):
        group = [turned[(t * per + k) * count : (t * per + k + 1) * count] for k in range(per)]
        passing.append(sum(pltpu.roll(group[k], k * fars, 1) for k in range(1, per)) + group[0])
    arrive("kb")
    pulled = jnp.concatenate([kb[:, half].reshape(NEAR * fars, RANK) for half in range(2)], axis=1)
    sr = times(src[3][...], kept(("qw", 3)), 0)
    sr = sr + times(jnp.concatenate(passing, axis=1), halves(pulled), 0)
    m["sr"][near] = jnp.concatenate([sr[:, :RANK], sr[:, RANK:]], axis=0)
    spread_own("sr", NEAR, 1)
    solve_front(1, local1)
    tail_of(2, wv_of(2))

    arrive("yg")
    y = m["yg"][...].reshape(2 * RANK, 2 * RANK)
    keep("y", y)
    yq = y[:, :RANK] * jnp.broadcast_to(head[3][:1], (2 * RANK, RANK))
    yv = y[:, RANK:] + times(yq, kept(("cross", 3)), 0)
    keep("yh", jnp.where(core == 0, yq, yv))
    tot = near_sum("sr")
    sq = tot[:count] * head[3]
    mine = jnp.where(core == 0, sq, tot[count:] + times(sq, kept(("cross", 3)), 0))
    ws = sums_up(2)
    m["fb"][far] = mine - times(ws, kept("yh"), 0)
    spread_own("fb", fars, NEAR)
    b3 = src[3][...] + receive_up(2, ws)
    early = outer(mult(b3, blk[3][...]) * piv[3][...], blk[3][...])
    send_down(2, early)
    solve_front(2, local2)
    pass_zp(1)
    arrive("c0")
    keep(("cross", 0), jnp.sum(m["c0"][...], axis=0))
    tail_of(0, mult(blk[0][...], v_of(0)))
    arrive(("ba", 2))
    ba = m["ba", 2]
    sums = jnp.sum(ba[:, : 2 * count, :], axis=0)
    early_rows = rows_of(2, "s", ba[:, 2 * count :, :])
    pass_zp(2)
    arrive("kr")
    keep("ka", m["kr"][...].reshape(NEAR * fars, 2 * RANK))
    arrive(("zb", 1))
    base1 = base_of(1, jnp.sum(m["zb", 1][...], axis=0))
    arrive("fb")
    m["fc"][core] = jnp.sum(m["fb"][...], axis=0)
    spread_own("fc", 2, across)
    arrive("fc")
    ends = jnp.concatenate([m["fc"][1] * head[3], m["fc"][0]], axis=1)
    sums = jnp.concatenate([sums[:count], sums[count:]], axis=1) + times(ends, kept("y"), 1)
    late = times(ends, kept("ka"), 1)
    late = [
        pltpu.roll(late[:, k // per * LANES : (k // per + 1) * LANES], (LANES - k % per * fars) % LANES, 1)
        for k in range(NEAR)
    ]
    late = transposed(jnp.concatenate(late, axis=0))[:fars]
    send_far(2, "s", sums[:, :RANK], sums[:, RANK:], early_rows + late)
    spread_own("hx", four, 1)
    outs[3][...] = early + times(ends, kept(("qw", 3)), 1)

    arrive(("zb", 2))
    base2 = base_of(2, jnp.sum(m["zb", 2][...], axis=0))
    x, xu = receive_down(2, base2)
    send_down(1, jnp.concatenate([x, xu], axis=1))
    outs[2][...] = x
    send_further(1)
    arrive("hx")
    for k in range(four):
        at = slice(k * cap * plane, (k + 1) * cap * plane)
        m["hxh"][at, :], m["hxl"][at, :] = halves(m["hx"][k])
    x, xu = receive_down(1, base1)
    full = diagonal(jnp.concatenate([x, xu], axis=1), cap, four)
    rows = leaf_rows((m["oh0"][...], None), full)
    ri = lax.broadcasted_iota(jnp.int32, (plane, LANES), 0)
    li = lax.broadcasted_iota(jnp.int32, (plane, LANES), 1)
    rows = jnp.where(li // (cap * count) == ri % four, rows, 0.0)
    rows = rows + pltpu.roll(rows, plane - 1, 0)
    m["s0b"][...] = rows + pltpu.roll(rows, plane - 2, 0)
    send_leaf("s0b", "r0b", lambda q: q // four * four)
    outs[1][...] = x
    arrive("r0b")
    rows = transposed(m["r0b"][...])
    pieces = [rows[g * count : (g + 1) * count] for g in range(four * cap)]
    pairs = [pieces[2 * g] + pltpu.roll(pieces[2 * g + 1], plane, 1) for g in range(four * cap // 2)]
    s = times(jnp.concatenate(pairs, axis=1), (m["hxh"][...], m["hxl"][...]), 0) * side[0]
    outs[0][...] = base0 - times(s, kept(("t", 0)), 1)

    for name, part in parts.items():
        wait_for(part, send_sem.at[sem_of(name)])


def solution(mesh):
    leaves, across = mesh.shape["leaf"], mesh.shape["grid"]

    def shards(*args):
        levels = [args[8 * i : 8 * i + 8] for i in range(3)]
        root = args[24:30]
        (sl, bl, el, qs, pv, cl, rk, tg) = zip(*levels)
        src = list(sl) + [root[0]]
        blk = list(bl) + [root[1]]
        exp = list(el) + [root[2]]
        bas = list(qs) + [root[3]]
        piv = [v.reshape(1, -1) for v in list(pv) + [root[4]]]
        rnk = [rk[0].T, rk[1].T, rk[2], root[5]]
        tgt = [t.reshape(1, -1) for t in tg]
        count = src[0].shape[0]
        ups = [t.shape[1] for t in tgt]
        fronts = [r.shape[0] for r in rk] + [root[5].shape[0]]
        size = [leaves * across // f for f in fronts]
        cap = ups[0] // size[1]
        nb = [s // NEAR for s in size]
        for v in src:
            assert v.shape == (NEAR, LANES)
        assert ups[1:] == [LANES, LANES] and cap * (count + 1) <= LANES
        assert 2 * size[1] == LANES and size[0] * cap * count == LANES
        assert nb[1] == 8 and across == 4 and size[0] == across
        assert size[2] == 2 * size[1] and size[3] == 2 * size[2] and size[1] % NEAR == 0
        assert NEAR * nb[2] == LANES and NEAR * nb[3] == 2 * LANES
        vm = lambda *s: pltpu.VMEM(s, F32)
        bits = lambda *s: pltpu.VMEM(s, BF16)
        piece = RANK // NEAR
        bufs = {
            "f1": vm(size[0], count, LANES),
            "fv": vm(size[0], count, LANES),
            "c0": vm(size[0], RANK, RANK),
            "zx": vm(size[0], count, LANES),
            "xp1": vm(NEAR, piece, RANK),
            "xr1": vm(NEAR, piece, RANK),
            "xp2": vm(NEAR, 2 * piece, RANK),
            "xr2": vm(NEAR, 2 * piece, RANK),
            "xb1": vm(nb[1], piece, RANK),
            "xb2": vm(nb[1], 2 * piece, RANK),
            "xy": vm(nb[3] // nb[1], 2 * piece, RANK),
            "xg1": vm(NEAR, piece, RANK),
            "xg2": vm(NEAR, 2 * piece, RANK),
            "lows": vm(2, count, LANES),
            "la": vm(NEAR, count, LANES),
            "tl": vm(LANES, LANES),
            "hch": bits(size[1], cap * RANK),
            "hcl": bits(size[1], cap * RANK),
            "low0": vm(size[1], LANES),
            "oh0": bits(size[1], cap * 2 * LANES),
            "fb": vm(nb[3], count, LANES),
            "ks": vm(NEAR, 2, nb[3], RANK),
            "kb": vm(NEAR, 2, nb[3], RANK),
            "sr": vm(NEAR, 2 * count, LANES),
            "kp": vm(NEAR, nb[3], 2 * RANK),
            "kr": vm(NEAR, nb[3], 2 * RANK),
            "yp": vm(NEAR, 2 * RANK // NEAR, 2 * RANK),
            "yr": vm(NEAR, 2 * RANK // NEAR, 2 * RANK),
            "yg": vm(NEAR, 2 * RANK // NEAR, 2 * RANK),
            "fc": vm(2, count, LANES),
            "hx": vm(size[0], cap * size[1], RANK),
            "hxh": bits(size[0] * cap * size[1], RANK),
            "hxl": bits(size[0] * cap * size[1], RANK),
        }
        for name in ("s0", "r0", "s0b", "r0b"):
            bufs[name] = vm(size[1], LANES)
        for half in "hl":
            bufs["ka", half] = bits(NEAR * nb[3], 2 * RANK)
            bufs["y", half] = bits(2 * RANK, 2 * RANK)
            bufs["yh", half] = bits(2 * RANK, RANK)
        for i in range(4):
            for half in "hl":
                bufs[("cross", i), half] = bits(RANK, RANK)
                bufs[("qw", i), half] = bits(LANES, 2 * RANK)
                bufs[("t", i), half] = bits(LANES, RANK)
        for i in (1, 2):
            n = nb[i + 1]
            wide = 2 * LANES if i == 1 else LANES
            tiles = NEAR * n // LANES
            bufs["h", i] = bits(NEAR * n, LANES)
            bufs["ohr", i] = bits(n, NEAR * LANES)
            bufs["ohf", i] = bits(n, NEAR * wide)
            bufs["ohg", i] = bits(NEAR * n, wide)
            bufs["pa", i] = vm(NEAR, n, RANK)
            bufs["ra", i] = vm(NEAR, n, RANK)
            bufs["rb", i] = vm(NEAR, n, RANK)
            bufs["lb", i] = vm(n, LANES)
            for half in "hl":
                bufs[("g", i), half] = bits(2 * RANK, wide)
            bufs["fs", i] = vm(tiles, 3 * count, LANES)
            bufs["fa", i] = vm(NEAR, 3 * count, LANES)
            bufs["bs", i] = vm(tiles, 3 * count, LANES)
            bufs["ba", i] = vm(NEAR, 3 * count, LANES)
            for kind in "ws":
                bufs["t" + kind, i] = vm(LANES, LANES)
                bufs[kind + "s", i] = vm(n, 2 * count, LANES)
                bufs[kind + "b", i] = vm(n, 2 * count, LANES)
            bufs["hb", i] = vm(nb[i], count, LANES)
            bufs["za", i] = vm(NEAR, count, LANES)
            bufs["zb", i] = vm(nb[i], count, LANES)
        arrays = [*src, *blk, *exp, *bas, *piv, *cl, *tgt, *rnk]
        for i, v in enumerate(arrays):
            bufs["in", i] = pltpu.VMEM(v.shape, v.dtype)
        scratch = list(bufs.values())
        scratch += [
            pltpu.SemaphoreType.DMA((56,)),
            pltpu.SemaphoreType.DMA((56,)),
            pltpu.SemaphoreType.DMA((30,)),
            pltpu.SemaphoreType.REGULAR,
        ]
        vspec = pl.BlockSpec(memory_space=pltpu.VMEM)
        whole = pl.pallas_call(
            functools.partial(kernel, (leaves, across, size, ups, count, cap), list(bufs)),
            out_shape=jax.ShapeDtypeStruct((4 * count, LANES), F32),
            in_specs=[pl.BlockSpec(memory_space=pl.ANY)] * 30,
            out_specs=vspec,
            scratch_shapes=scratch,
            compiler_params=pltpu.CompilerParams(
                collective_id=0, has_side_effects=True, vmem_limit_bytes=60 * 1024 * 1024
            ),
        )(*arrays)
        return tuple(whole[i * count : (i + 1) * count] for i in range(4))

    spread_axes = ("leaf", "grid")
    level = (P(None, spread_axes), P(spread_axes, None), P(spread_axes, None), P(spread_axes, None), P(spread_axes))
    mid = level + (P(spread_axes, None), P(), P(spread_axes))
    return jax.shard_map(
        shards,
        mesh=mesh,
        in_specs=mid * 3 + level + (P(),),
        out_specs=(P(None, spread_axes),) * 4,
        check_vma=False,
    )
```

```python
import functools

import jax
import jax.numpy as jnp
from jax import lax
from jax.experimental import pallas as pl
from jax.experimental.pallas import tpu as pltpu
from jax.sharding import PartitionSpec as P

RANK = 128
LANES = 128
NEAR = 8
LOGICAL = pl.DeviceIdType.LOGICAL
F32 = jnp.float32
BF16 = jnp.bfloat16


def once(a, b, ca, cb):
    return lax.dot_general(a, b, (((ca,), (cb,)), ((), ())), preferred_element_type=F32)


def halves(x):
    hi = x.astype(BF16)
    return hi, (x - hi.astype(F32)).astype(BF16)


def stacked(x):
    hi = x.astype(BF16).astype(F32)
    return jnp.concatenate([hi, x - hi], axis=0).astype(BF16)


def times(a, b, cb):
    bh, bl = b
    n = a.shape[0]
    both = once(stacked(a), bh, 1, cb)
    return both[:n] + (both[n:] + once(a.astype(BF16), bl, 1, cb))


def mult(a, b):
    return times(a, halves(b), 0)


def outer(a, b):
    return times(a, halves(b), 1)


def inner(a, b):
    ah, al = halves(a)
    bh, bl = halves(b)
    return once(ah, bh, 0, 0) + (once(al, bh, 0, 0) + once(ah, bl, 0, 0))


def pick(x, onehot):
    n = x.shape[0]
    both = once(stacked(x), onehot, 1, 1)
    return both[:n] + both[n:]


def spread(rows, onehot, groups, count):
    m = groups * count
    wide = onehot.shape[1] // groups
    both = once(stacked(rows.T[:m]), onehot, 1, 0)
    out = None
    for g in range(groups):
        lanes = slice(g * wide, (g + 1) * wide)
        part = both[g * count : (g + 1) * count, lanes] + both[m + g * count : m + (g + 1) * count, lanes]
        out = part if out is None else out + part
    return out


def diagonal(x, groups, again=1):
    count, wide = x.shape
    zero = jnp.zeros((count, wide), F32)
    rows = [
        jnp.concatenate([x if h == g else zero for h in range(groups)], axis=1) for g in range(groups)
    ]
    rows = rows * again
    left = LANES - len(rows) * count
    if left:
        rows.append(jnp.zeros((left, groups * wide), F32))
    return jnp.concatenate(rows, axis=0)


def kernel(cfg, names, *refs):
    leaves, across, size, ups, count, cap = cfg
    total_devices = leaves * across
    count_in = 30
    given, out = refs[:count_in], refs[count_in]
    outs = [out.at[pl.ds(i * count, count)] for i in range(4)]
    m = dict(zip(names, refs[count_in + 1 : -4]))
    send_sem, recv_sem, load_sem, ready = refs[-4:]
    held = [m["in", i] for i in range(count_in)]
    (src, blk, exp, bas, piv) = [held[4 * i : 4 * i + 4] for i in range(5)]
    cpl, tgt, rnk = held[20:23], held[23:26], held[26:30]
    loads = [pltpu.make_async_copy(given[i], held[i], load_sem.at[i]) for i in range(count_in)]
    sems = {}
    parts = {}

    me = lax.axis_index("leaf") * across + lax.axis_index("grid")
    near = me % NEAR
    far = me // NEAR
    nb = [s // NEAR for s in size]
    plane = size[1]
    fars = nb[3]

    def sem_of(name):
        return sems.setdefault(name, len(sems))

    def remote(a, b, sem, peer):
        return pltpu.make_async_remote_copy(
            src_ref=a,
            dst_ref=b,
            send_sem=send_sem.at[sem],
            recv_sem=recv_sem.at[sem],
            device_id=peer,
            device_id_type=LOGICAL,
        )

    def wait_for(part, sem):
        pltpu.make_async_copy(part, part, sem).wait()

    ring = nb[1]

    def farthest(n):
        return sorted(range(n), key=lambda d: -min(d, n - d))

    def fan(group, stride, *sets):
        idx = me // stride % group
        base = me - idx * stride
        for name, source, dest, part in sets:
            sem_of(name)
            parts[name] = part

        def go(q):
            for name, source, dest, part in sets:
                remote(source(q), dest(idx), sem_of(name), base + q * stride).start()

        if stride == NEAR:
            rows = group // ring
            for dy in farthest(rows):
                line = (idx // ring + dy) % rows * ring
                for dz in farthest(ring):
                    if dy or dz:
                        go(line + (idx + dz) % ring)
        elif group == plane:
            for dz in farthest(ring)[:-1]:
                line = (idx // NEAR + dz) % ring * NEAR

                def body(k, carry, line=line):
                    go(line + k)
                    return carry

                lax.fori_loop(0, NEAR, body, 0, unroll=True)
            for k in range(1, NEAR):
                go(idx // NEAR * NEAR + (idx + k) % NEAR)
        elif group == NEAR:
            for dx in farthest(across):
                for dc in (1, 0):
                    if dx or dc:
                        go((idx // across + dc) % 2 * across + (idx + dx) % across)
        else:
            for d in farthest(group)[:-1]:
                go((idx + d) % group)

    def arrive(name):
        wait_for(parts[name], recv_sem.at[sem_of(name)])

    def slots(name, group):
        buf = m[name]
        return buf.at[pl.ds(0, group - 1)]

    def spread_own(name, group, stride):
        buf = m[name]
        idx = me // stride % group
        fan(group, stride, (name, lambda q: buf.at[idx], lambda i: buf.at[i], slots(name, group)))

    barrier = pltpu.get_barrier_semaphore()

    def greet_near(sem):
        def body(k, carry):
            peer = far * NEAR + (near + k) % NEAR
            pl.semaphore_signal(sem, inc=1, device_id=peer, device_id_type=LOGICAL)
            return carry

        lax.fori_loop(1, NEAR, body, 0)

    def greet_ring(sem):
        for dz in farthest(ring)[:-1]:
            peer = (far // ring * ring + (far + dz) % ring) * NEAR + near
            pl.semaphore_signal(sem, inc=1, device_id=peer, device_id_type=LOGICAL)

    def greet_planes():
        for dy in range(1, fars // ring):
            peer = (far + dy * ring) % fars * NEAR + near
            pl.semaphore_signal(barrier, inc=1, device_id=peer, device_id_type=LOGICAL)

    soon = (0, 12)
    for i in soon:
        loads[i].start()
    greet_ring(barrier)
    greet_planes()
    greet_near(barrier)
    rest = [i for i in range(count_in) if i not in soon]
    for i in rest:
        loads[i].start()

    def mask(level, which, front):
        ranks = rnk[level][...].astype(F32)
        axis = 1 if level < 2 else 0
        line = ranks[which : which + 1, :] if level < 2 else ranks[:, which : which + 1]
        here = lax.broadcasted_iota(jnp.int32, line.shape, axis) == front
        rank = jnp.sum(jnp.where(here, line, 0.0), axis=axis, keepdims=True)
        col = lax.broadcasted_iota(jnp.int32, (count, RANK), 1).astype(F32)
        return (col < rank).astype(F32)

    def q_of(level):
        return bas[level][:, :RANK]

    def v_of(level):
        return bas[level][:, RANK:]

    def tiles_of(level):
        n = nb[level + 1]
        return NEAR * n // LANES, LANES // n

    def keep(name, value):
        hi, lo = halves(value)
        m[name, "h"][...] = hi
        m[name, "l"][...] = lo

    def kept(name):
        return m[name, "h"][...], m[name, "l"][...]

    four = size[0]
    my4 = me % four
    for i in soon:
        loads[i].wait()
    s0 = src[0][...]
    m["f1"][my4] = mult(s0, q_of(0))
    pl.semaphore_wait(barrier, NEAR - 1 + ring - 1 + fars // ring - 1)
    spread_own("f1", four, 1)
    greet_near(ready)
    greet_ring(ready)
    for i in rest:
        loads[i].wait()
    front = [me // n for n in size]
    head = [mask(level, 0, front[level]) for level in range(4)]
    side = [mask(level, 1, front[level]) for level in range(3)]
    below = [None] + [
        [mask(level, 1, front[level + 1] * 2 + child) for child in range(2)] for level in (1, 2)
    ]
    local0 = mult(s0, blk[0][...])
    own0 = inner(exp[0][...], v_of(0))
    m["c0"][my4] = own0
    keep("own", own0)
    lv0 = mult(local0, v_of(0))

    slice_rows = RANK // NEAR
    root_piv = jnp.broadcast_to(piv[3][...], (LANES, LANES)).T
    crosses = [
        inner(exp[1][...], v_of(1)),
        inner(exp[2][...], v_of(2)),
        inner(exp[3][...] * root_piv, exp[3][...]),
    ]
    for j, cross in enumerate(crosses):
        buf, at = (m["xp1"], 0) if j == 0 else (m["xp2"], (j - 1) * slice_rows)
        buf[:, at : at + slice_rows, :] = cross.reshape(NEAR, slice_rows, RANK)

    def split_targets(level):
        sep = size[level + 1] * LANES
        t = tgt[level][...]
        upd = t >= sep
        rel = jnp.where(upd, t - sep, t)
        return rel // LANES, rel % LANES + jnp.where(upd, LANES, 0)

    def pack_leaf():
        u = ups[0]
        dst, low = split_targets(0)
        ri = lax.broadcasted_iota(jnp.int32, (u, u), 0)
        ci = lax.broadcasted_iota(jnp.int32, (u, u), 1)
        dst_f = dst.astype(F32)
        dst_c = jnp.sum(jnp.where(ri == ci, jnp.broadcast_to(dst_f, (u, u)), 0.0), axis=1, keepdims=True)
        rank = jnp.sum(
            jnp.where((dst_c == dst_f) & (ri < ci), 1.0, 0.0), axis=0, keepdims=True
        ).astype(jnp.int32)
        slot = rank * plane + dst
        ch, cl = halves(cpl[0][...])
        lowmat = None
        li = lax.broadcasted_iota(jnp.int32, (LANES, u), 0)
        for s in range(cap):
            si = lax.broadcasted_iota(jnp.int32, (plane, u), 0) + s * plane
            hit = (si == slot).astype(F32).astype(BF16)
            lanes = slice(s * RANK, (s + 1) * RANK)
            high, low_part = once(hit, ch, 1, 0), once(hit, cl, 1, 0)
            m["hch"][:, lanes] = high.astype(BF16)
            m["hcl"][:, lanes] = low_part.astype(BF16)
            m["hx"][my4, s * plane : (s + 1) * plane, :] = high + low_part
            mine = jnp.where(li == cap * count + s, low.astype(F32), 0.0).astype(BF16)
            part = once(hit, mine, 1, 1)
            lowmat = part if lowmat is None else lowmat + part
        m["low0"][...] = lowmat

    def pack_couple(level):
        n = nb[level + 1]
        dst, low = split_targets(level)
        slot = dst % NEAR * n + dst // NEAR
        si = lax.broadcasted_iota(jnp.int32, (NEAR * n, LANES), 0)
        h = (si == slot).astype(F32).astype(BF16)
        m["h", level][...] = h
        hi, lo = [once(h, piece, 1, 0) for piece in halves(cpl[level][...])]
        m["pa", level][...] = (hi + lo).reshape(NEAR, n, RANK)
        rows = jnp.broadcast_to(low, (count, LANES)).astype(F32).astype(BF16)
        bi = lax.broadcasted_iota(jnp.int32, (n, LANES), 0) * NEAR
        m["ohr", level][...] = jnp.concatenate(
            [(bi + k == dst).astype(F32) for k in range(NEAR)], axis=1
        ).astype(BF16)
        return once(rows, h, 1, 1)

    low1, low2 = pack_couple(1), pack_couple(2)
    ri = lax.broadcasted_iota(jnp.int32, (count, LANES), 0)
    for t in range(2):
        two = low2[:, t * LANES : (t + 1) * LANES]
        m["lows"][t] = jnp.where(ri == 0, two, jnp.where(ri == 1, low1, 0.0))
    pack_leaf()

    def fan_near(name, source, dest):
        fan(NEAR, 1, (name, source, lambda i: dest.at[i], dest.at[pl.ds(0, NEAR - 1)]))

    def scatter_near(name, source):
        m[name][near] = m[source][near]
        fan_near(name, lambda q: m[source].at[q], m[name])

    scatter_near("xr1", "xp1")
    m["la"][near] = m["lows"][near // 4]
    fan_near("la", lambda q: m["lows"].at[q // 4], m["la"])
    scatter_near(("ra", 1), ("pa", 1))

    for level in (1, 2):
        wv = mult(blk[level][...], v_of(level))
        keep(("qw", level), jnp.concatenate([q_of(level), wv], axis=1))
    wpp = mult(blk[3][...] * piv[3][...], exp[3][...])
    keep(("qw", 3), jnp.concatenate([q_of(3), wpp], axis=1))

    arrive("f1")
    hq0 = jnp.sum(m["f1"][...], axis=0) * head[0]
    m["fv"][my4] = lv0 + times(hq0, kept("own"), 0)
    spread_own("fv", four, 1)
    y0 = local0 + outer(hq0, exp[0][...])
    scatter_near(("ra", 2), ("pa", 2))
    scatter_near("xr2", "xp2")
    z0 = y0 * piv[0][...]
    m["zx"][my4] = mult(z0, exp[0][...])
    arrive("xr1")
    m["xb1"][far % ring] = jnp.sum(m["xr1"][...], axis=0)
    spread_own("xb1", ring, NEAR)
    arrive("fv")
    w0 = jnp.sum(m["fv"][...], axis=0) * side[0]

    def leaf_rows(a, b):
        ah, al = a
        bh, bl = halves(b)
        out = once(ah, bh, 1, 1) + once(ah, bl, 1, 1)
        return out if al is None else out + once(al, bh, 1, 1)

    place = me % plane

    def send_leaf(rows, got, row):
        m[got][pl.ds(place, 1), :] = m[rows][pl.ds(row(place), 1), :]
        fan(
            plane,
            1,
            (
                got,
                lambda q: m[rows].at[pl.ds(row(q), 1)],
                lambda i: m[got].at[pl.ds(i, 1)],
                m[got].at[pl.ds(0, plane - 1)],
            ),
        )

    hc = (m["hch"][...], m["hcl"][...])
    m["s0"][...] = leaf_rows(hc, diagonal(-w0, cap)) + m["low0"][...]
    pl.semaphore_wait(ready, NEAR - 1 + ring - 1)
    send_leaf("s0", "r0", lambda q: q)

    def store_row(buf, i, row):
        buf[pl.ds(i, 1), :] = row

    def forward_rows(level, table, got, name):
        n = nb[level + 1]
        per = tiles_of(level)[1]
        idx = far % n
        first = near % per * n
        store_row(m[got], idx, m[table][pl.ds(first + idx, 1), :])
        return (
            name,
            lambda q: m[table].at[pl.ds(first + q, 1)],
            lambda i: m[got].at[pl.ds(i, 1)],
            m[got].at[pl.ds(0, n - 1)],
        )

    def transposed(x):
        return jnp.concatenate([x, jnp.zeros((LANES - x.shape[0], LANES), F32)], axis=0).T

    def couple_set(level):
        n = nb[level + 1]
        ra, rb = m["ra", level], m["rb", level]
        idx = far % n
        rb[:, pl.ds(idx, 1), :] = ra[:, pl.ds(idx, 1), :]
        return (
            ("rb", level),
            lambda q: ra.at[:, pl.ds(q, 1)],
            lambda i: rb.at[:, pl.ds(i, 1)],
            rb.at[:, pl.ds(0, n - 1)],
        )

    arrive("la")
    m["tl"][...] = transposed(m["la"][...].reshape(NEAR * count, LANES))
    for level in (1, 2):
        arrive(("ra", level))
        sets = [forward_rows(level, "tl", ("lb", level), ("lb", level))]
        if level == 1:
            sets.append(couple_set(level))
        fan(nb[level + 1], NEAR, *sets)
    arrive("xr2")
    m["xb2"][far % ring] = jnp.sum(m["xr2"][...], axis=0)
    spread_own("xb2", ring, NEAR)
    arrive("xb1")
    m["xg1"][near] = jnp.sum(m["xb1"][...], axis=0)
    spread_own("xg1", NEAR, 1)
    spread_own("zx", four, 1)

    def build_hits(level):
        n = nb[level + 1]
        wide = 2 * LANES if level == 1 else LANES
        arrive(("lb", level))
        lb = m["lb", level][...]
        lane = lax.broadcasted_iota(jnp.int32, (n, wide), 1).astype(F32)
        at = 2 - level
        hits = [(lane == lb[:, k * count + at : k * count + at + 1]).astype(F32) for k in range(NEAR)]
        m["ohf", level][...] = jnp.concatenate(hits, axis=1).astype(BF16)
        m["ohg", level][...] = jnp.concatenate(hits, axis=0).astype(BF16)
        return hits

    def build_g(level, hits):
        n = nb[level + 1]
        arrive(("rb", level))
        half = n // 2
        for child in range(2):
            rows = slice(child * half, (child + 1) * half)
            got = m["rb", level][:, rows, :].reshape(NEAR * half, RANK)
            hot = jnp.concatenate([hit[rows] for hit in hits], axis=0).astype(BF16)
            hi, lo = [once(piece, hot, 0, 0) for piece in halves(got)]
            gh, gl = halves(hi + lo)
            out = slice(child * RANK, (child + 1) * RANK)
            m[("g", level), "h"][out, :] = gh
            m[("g", level), "l"][out, :] = gl

    def send_up(level, b, u):
        count_tiles, per = tiles_of(level)
        both = times(b, kept(("qw", level)), 0)
        tile = pick(u, m["h", level][...])
        for t in range(count_tiles):
            m["fs", level][t] = jnp.concatenate(
                [both[:, :RANK], both[:, RANK:], tile[:, t * LANES : (t + 1) * LANES]], axis=0
            )
        fs, fa = m["fs", level], m["fa", level]
        fa[near] = fs[near // per]
        fan_near(("fa", level), lambda q: fs.at[q // per], fa)

    def rows_of(level, kind, tiles):
        n = nb[level + 1]
        table = m["t" + kind, level]
        table[...] = transposed(tiles.reshape(NEAR * count, LANES))
        return table[pl.ds(pl.multiple_of(near % tiles_of(level)[1] * n, 8), n), :]

    def send_far(level, kind, first, second, rows):
        n = nb[level + 1]
        half = n // 2
        idx = far % n
        source, got = m[kind + "s", level], m[kind + "b", level]
        source[:half, :count, :] = jnp.broadcast_to(first[None], (half, count, RANK))
        source[half:, :count, :] = jnp.broadcast_to(second[None], (half, count, RANK))
        source[:, count, :] = rows
        used = pl.ds(0, count + 1)
        got[idx, : count + 1, :] = source[idx, : count + 1, :]
        fan(
            n,
            NEAR,
            (
                (kind, level),
                lambda q: source.at[q, used],
                lambda i: got.at[i, used],
                got.at[pl.ds(0, n - 1), used],
            ),
        )

    def send_on(level):
        arrive(("fa", level))
        fa = m["fa", level]
        tot = jnp.sum(fa[:, : 2 * count, :], axis=0)
        hq = tot[:count] * head[level]
        w = tot[count:] + times(hq, kept(("cross", level)), 0)
        rows = rows_of(level, "w", fa[:, 2 * count :, :])
        send_far(level, "w", w, w, rows)
        m["hb", level][far % nb[level]] = hq
        spread_own(("hb", level), nb[level], NEAR)
        return rows

    def sums_up(level):
        half = nb[level + 1] // 2
        arrive(("w", level))
        wb = m["wb", level]
        ws = [
            jnp.sum(wb[child * half : (child + 1) * half, :count, :], axis=0) * below[level][child]
            for child in range(2)
        ]
        return jnp.concatenate(ws, axis=1)

    def receive_up(level, ws):
        rows = spread(m["wb", level][:, count, :], m["ohf", level][...], NEAR, count)
        return rows - times(ws, kept(("g", level)), 0)

    def near_sum(name):
        arrive(name)
        return jnp.sum(m[name][...], axis=0)

    def send_down(level, full):
        count_tiles, per = tiles_of(level)
        sp = times(full, kept(("g", level)), 1)
        tile = pick(full, m["ohg", level][...])
        for t in range(count_tiles):
            m["bs", level][t] = jnp.concatenate(
                [sp[:, :RANK], sp[:, RANK:], tile[:, t * LANES : (t + 1) * LANES]], axis=0
            )
        bs, ba = m["bs", level], m["ba", level]
        ba[near] = bs[near // per]
        fan_near(("ba", level), lambda q: bs.at[q // per], ba)

    def send_further(level):
        arrive(("ba", level))
        ba = m["ba", level]
        tot = jnp.sum(ba[:, : 2 * count, :], axis=0)
        send_far(level, "s", tot[:count], tot[count:], rows_of(level, "s", ba[:, 2 * count :, :]))

    def receive_down(level, base):
        arrive(("s", level))
        sb = m["sb", level]
        s = jnp.sum(sb[:, :count, :], axis=0) * side[level]
        x = base - times(s, kept(("t", level)), 1)
        xu = spread(sb[:, count, :], m["ohr", level][...], NEAR, count)
        return x, xu

    saved = {}

    def solve_front(level, local):
        arrive(("hb", level))
        hq = jnp.sum(m["hb", level][...], axis=0)
        z = (local + outer(hq, exp[level][...])) * piv[level][...]
        saved[level] = z
        m["za", level][near] = mult(z, exp[level][...])
        spread_own(("za", level), NEAR, 1)

    def pass_zp(level):
        m["zb", level][far % nb[level]] = near_sum(("za", level))
        spread_own(("zb", level), nb[level], NEAR)

    def base_of(level, zp):
        return outer(saved[level], blk[level][...]) + outer(zp * head[level], q_of(level))

    def tail_of(level, wv):
        qm = q_of(level) * jnp.broadcast_to(head[level][:1], (LANES, RANK))
        keep(("t", level), wv + times(qm, kept(("cross", level)), 0))

    def wv_of(level):
        qh, ql = kept(("qw", level))
        return qh[:, RANK:].astype(F32) + ql[:, RANK:].astype(F32)

    arrive("r0")
    r0 = m["r0"][...]
    lane = lax.broadcasted_iota(jnp.int32, (plane, 2 * LANES), 1).astype(F32)
    at = cap * count
    m["oh0"][...] = jnp.concatenate(
        [(lane == r0[:, at + s : at + s + 1]).astype(F32) for s in range(cap)], axis=1
    ).astype(BF16)
    inc = spread(r0, m["oh0"][...], cap, count)
    b1 = src[1][...] + inc[:, :LANES]
    send_up(1, b1, inc[:, LANES:])
    fan(nb[3], NEAR, couple_set(2))

    local1 = mult(b1, blk[1][...])
    saved[0] = z0
    arrive("zx")
    base0 = base_of(0, jnp.sum(m["zx"][...], axis=0))
    build_g(1, build_hits(1))
    arrive("xg1")
    keep(("cross", 1), m["xg1"][...].reshape(RANK, RANK))
    hits = build_hits(2)
    kh, kl = kept(("qw", 3))
    hot = m["ohg", 2][...]
    m["kp"][...] = (once(hot, kh, 1, 0) + once(hot, kl, 1, 0)).reshape(NEAR, fars, 2 * RANK)
    scatter_near("kr", "kp")
    arrive("xb2")
    m["xy"][me // plane] = jnp.sum(m["xb2"][...], axis=0)
    spread_own("xy", total_devices // plane, plane)
    send_on(1)
    ks, kb = m["ks"], m["kb"]
    for half in range(2):
        ks[:, half] = m["kp"][:, :, half * RANK : (half + 1) * RANK]
    kb[:, :, pl.ds(far, 1), :] = ks[:, :, pl.ds(far, 1), :]
    fan(
        fars,
        NEAR,
        (
            "kb",
            lambda q: ks.at[:, :, pl.ds(q, 1)],
            lambda i: kb.at[:, :, pl.ds(i, 1)],
            kb.at[:, :, pl.ds(0, fars - 1)],
        ),
    )

    arrive("xy")
    pair = me // plane // 2 * 2
    m["xg2"][near, :slice_rows, :] = jnp.sum(m["xy"][pl.ds(pair, 2), :slice_rows, :], axis=0)
    m["xg2"][near, slice_rows:, :] = jnp.sum(m["xy"][:, slice_rows:, :], axis=0)
    spread_own("xg2", NEAR, 1)
    build_g(2, hits)
    gh, gl = kept(("g", 2))
    both = once(gh, kh, 1, 0) + (once(gl, kh, 1, 0) + once(gh, kl, 1, 0))
    m["yp"][...] = both.reshape(NEAR, 2 * RANK // NEAR, 2 * RANK)
    scatter_near("yr", "yp")
    tail_of(1, wv_of(1))

    inc = receive_up(1, sums_up(1))
    b2 = src[2][...] + inc[:, :LANES]
    send_up(2, b2, inc[:, LANES:])
    m["yg"][near] = near_sum("yr")
    spread_own("yg", NEAR, 1)

    local2 = mult(b2, blk[2][...])
    arrive("xg2")
    keep(("cross", 2), m["xg2"][:, :slice_rows, :].reshape(RANK, RANK))
    rows = send_on(2)
    keep(("cross", 3), m["xg2"][:, slice_rows:, :].reshape(RANK, RANK))
    core = near // across
    per = LANES // fars
    turned = transposed(rows)
    passing = []
    for t in range(NEAR // per):
        group = [turned[(t * per + k) * count : (t * per + k + 1) * count] for k in range(per)]
        passing.append(sum(pltpu.roll(group[k], k * fars, 1) for k in range(1, per)) + group[0])
    arrive("kb")
    pulled = jnp.concatenate([kb[:, half].reshape(NEAR * fars, RANK) for half in range(2)], axis=1)
    sr = times(src[3][...], kept(("qw", 3)), 0)
    sr = sr + times(jnp.concatenate(passing, axis=1), halves(pulled), 0)
    m["sr"][near] = jnp.concatenate([sr[:, :RANK], sr[:, RANK:]], axis=0)
    spread_own("sr", NEAR, 1)
    spread_own("c0", four, 1)
    solve_front(1, local1)
    tail_of(2, wv_of(2))

    arrive("yg")
    y = m["yg"][...].reshape(2 * RANK, 2 * RANK)
    keep("y", y)
    yq = y[:, :RANK] * jnp.broadcast_to(head[3][:1], (2 * RANK, RANK))
    yv = y[:, RANK:] + times(yq, kept(("cross", 3)), 0)
    keep("yh", jnp.where(core == 0, yq, yv))
    tot = near_sum("sr")
    sq = tot[:count] * head[3]
    mine = jnp.where(core == 0, sq, tot[count:] + times(sq, kept(("cross", 3)), 0))
    ws = sums_up(2)
    m["fb"][far] = mine - times(ws, kept("yh"), 0)
    spread_own("fb", fars, NEAR)
    b3 = src[3][...] + receive_up(2, ws)
    early = outer(mult(b3, blk[3][...]) * piv[3][...], blk[3][...])
    send_down(2, early)
    solve_front(2, local2)
    pass_zp(1)
    arrive("c0")
    keep(("cross", 0), jnp.sum(m["c0"][...], axis=0))
    tail_of(0, mult(blk[0][...], v_of(0)))
    arrive(("ba", 2))
    ba = m["ba", 2]
    sums = jnp.sum(ba[:, : 2 * count, :], axis=0)
    early_rows = rows_of(2, "s", ba[:, 2 * count :, :])
    pass_zp(2)
    arrive("kr")
    keep("ka", m["kr"][...].reshape(NEAR * fars, 2 * RANK))
    arrive("fb")
    m["fc"][core] = jnp.sum(m["fb"][...], axis=0)
    spread_own("fc", 2, across)
    arrive("fc")
    ends = jnp.concatenate([m["fc"][1] * head[3], m["fc"][0]], axis=1)
    sums = jnp.concatenate([sums[:count], sums[count:]], axis=1) + times(ends, kept("y"), 1)
    late = times(ends, kept("ka"), 1)
    late = [
        pltpu.roll(late[:, k // per * LANES : (k // per + 1) * LANES], (LANES - k % per * fars) % LANES, 1)
        for k in range(NEAR)
    ]
    late = transposed(jnp.concatenate(late, axis=0))[:fars]
    send_far(2, "s", sums[:, :RANK], sums[:, RANK:], early_rows + late)
    spread_own("hx", four, 1)
    outs[3][...] = early + times(ends, kept(("qw", 3)), 1)

    arrive(("zb", 1))
    base1 = base_of(1, jnp.sum(m["zb", 1][...], axis=0))
    arrive(("zb", 2))
    base2 = base_of(2, jnp.sum(m["zb", 2][...], axis=0))
    x, xu = receive_down(2, base2)
    send_down(1, jnp.concatenate([x, xu], axis=1))
    outs[2][...] = x
    send_further(1)
    arrive("hx")
    for k in range(four):
        at = slice(k * cap * plane, (k + 1) * cap * plane)
        packed = m["hx"][k] * jnp.broadcast_to(side[0][:1], (cap * plane, RANK))
        m["hxh"][at, :], m["hxl"][at, :] = halves(times(packed, kept(("t", 0)), 1))
    x, xu = receive_down(1, base1)
    full = diagonal(jnp.concatenate([x, xu], axis=1), cap, four)
    rows = leaf_rows((m["oh0"][...], None), full)
    ri = lax.broadcasted_iota(jnp.int32, (plane, LANES), 0)
    li = lax.broadcasted_iota(jnp.int32, (plane, LANES), 1)
    rows = jnp.where(li // (cap * count) == ri % four, rows, 0.0)
    rows = rows + pltpu.roll(rows, plane - 1, 0)
    m["s0b"][...] = rows + pltpu.roll(rows, plane - 2, 0)
    send_leaf("s0b", "r0b", lambda q: q // four * four)
    outs[1][...] = x
    for name, part in parts.items():
        wait_for(part, send_sem.at[sem_of(name)])
    arrive("r0b")
    rows = transposed(m["r0b"][...])
    pieces = [rows[g * count : (g + 1) * count] for g in range(four * cap)]
    pairs = [pieces[2 * g] + pltpu.roll(pieces[2 * g + 1], plane, 1) for g in range(four * cap // 2)]
    outs[0][...] = base0 - times(jnp.concatenate(pairs, axis=1), (m["hxh"][...], m["hxl"][...]), 0)


def solution(mesh):
    leaves, across = mesh.shape["leaf"], mesh.shape["grid"]

    def shards(*args):
        levels = [args[8 * i : 8 * i + 8] for i in range(3)]
        root = args[24:30]
        (sl, bl, el, qs, pv, cl, rk, tg) = zip(*levels)
        src = list(sl) + [root[0]]
        blk = list(bl) + [root[1]]
        exp = list(el) + [root[2]]
        bas = list(qs) + [root[3]]
        piv = [v.reshape(1, -1) for v in list(pv) + [root[4]]]
        rnk = [rk[0].T, rk[1].T, rk[2], root[5]]
        tgt = [t.reshape(1, -1) for t in tg]
        count = src[0].shape[0]
        ups = [t.shape[1] for t in tgt]
        fronts = [r.shape[0] for r in rk] + [root[5].shape[0]]
        size = [leaves * across // f for f in fronts]
        cap = ups[0] // size[1]
        nb = [s // NEAR for s in size]
        for v in src:
            assert v.shape == (NEAR, LANES)
        assert ups[1:] == [LANES, LANES] and cap * (count + 1) <= LANES
        assert 2 * size[1] == LANES and size[0] * cap * count == LANES
        assert nb[1] == 8 and across == 4 and size[0] == across
        assert size[2] == 2 * size[1] and size[3] == 2 * size[2] and size[1] % NEAR == 0
        assert NEAR * nb[2] == LANES and NEAR * nb[3] == 2 * LANES
        vm = lambda *s: pltpu.VMEM(s, F32)
        bits = lambda *s: pltpu.VMEM(s, BF16)
        piece = RANK // NEAR
        bufs = {
            "f1": vm(size[0], count, LANES),
            "fv": vm(size[0], count, LANES),
            "c0": vm(size[0], RANK, RANK),
            "zx": vm(size[0], count, LANES),
            "xp1": vm(NEAR, piece, RANK),
            "xr1": vm(NEAR, piece, RANK),
            "xp2": vm(NEAR, 2 * piece, RANK),
            "xr2": vm(NEAR, 2 * piece, RANK),
            "xb1": vm(nb[1], piece, RANK),
            "xb2": vm(nb[1], 2 * piece, RANK),
            "xy": vm(nb[3] // nb[1], 2 * piece, RANK),
            "xg1": vm(NEAR, piece, RANK),
            "xg2": vm(NEAR, 2 * piece, RANK),
            "lows": vm(2, count, LANES),
            "la": vm(NEAR, count, LANES),
            "tl": vm(LANES, LANES),
            "hch": bits(size[1], cap * RANK),
            "hcl": bits(size[1], cap * RANK),
            "low0": vm(size[1], LANES),
            "oh0": bits(size[1], cap * 2 * LANES),
            "fb": vm(nb[3], count, LANES),
            "ks": vm(NEAR, 2, nb[3], RANK),
            "kb": vm(NEAR, 2, nb[3], RANK),
            "sr": vm(NEAR, 2 * count, LANES),
            "kp": vm(NEAR, nb[3], 2 * RANK),
            "kr": vm(NEAR, nb[3], 2 * RANK),
            "yp": vm(NEAR, 2 * RANK // NEAR, 2 * RANK),
            "yr": vm(NEAR, 2 * RANK // NEAR, 2 * RANK),
            "yg": vm(NEAR, 2 * RANK // NEAR, 2 * RANK),
            "fc": vm(2, count, LANES),
            "hx": vm(size[0], cap * size[1], RANK),
            "hxh": bits(size[0] * cap * size[1], RANK),
            "hxl": bits(size[0] * cap * size[1], RANK),
        }
        for name in ("s0", "r0", "s0b", "r0b"):
            bufs[name] = vm(size[1], LANES)
        for half in "hl":
            bufs["ka", half] = bits(NEAR * nb[3], 2 * RANK)
            bufs["y", half] = bits(2 * RANK, 2 * RANK)
            bufs["yh", half] = bits(2 * RANK, RANK)
        for i in range(4):
            for half in "hl":
                bufs[("cross", i), half] = bits(RANK, RANK)
                bufs[("qw", i), half] = bits(LANES, 2 * RANK)
                bufs[("t", i), half] = bits(LANES, RANK)
                bufs["own", half] = bits(RANK, RANK)
        for i in (1, 2):
            n = nb[i + 1]
            wide = 2 * LANES if i == 1 else LANES
            tiles = NEAR * n // LANES
            bufs["h", i] = bits(NEAR * n, LANES)
            bufs["ohr", i] = bits(n, NEAR * LANES)
            bufs["ohf", i] = bits(n, NEAR * wide)
            bufs["ohg", i] = bits(NEAR * n, wide)
            bufs["pa", i] = vm(NEAR, n, RANK)
            bufs["ra", i] = vm(NEAR, n, RANK)
            bufs["rb", i] = vm(NEAR, n, RANK)
            bufs["lb", i] = vm(n, LANES)
            for half in "hl":
                bufs[("g", i), half] = bits(2 * RANK, wide)
            bufs["fs", i] = vm(tiles, 3 * count, LANES)
            bufs["fa", i] = vm(NEAR, 3 * count, LANES)
            bufs["bs", i] = vm(tiles, 3 * count, LANES)
            bufs["ba", i] = vm(NEAR, 3 * count, LANES)
            for kind in "ws":
                bufs["t" + kind, i] = vm(LANES, LANES)
                bufs[kind + "s", i] = vm(n, 2 * count, LANES)
                bufs[kind + "b", i] = vm(n, 2 * count, LANES)
            bufs["hb", i] = vm(nb[i], count, LANES)
            bufs["za", i] = vm(NEAR, count, LANES)
            bufs["zb", i] = vm(nb[i], count, LANES)
        arrays = [*src, *blk, *exp, *bas, *piv, *cl, *tgt, *rnk]
        for i, v in enumerate(arrays):
            bufs["in", i] = pltpu.VMEM(v.shape, v.dtype)
        scratch = list(bufs.values())
        scratch += [
            pltpu.SemaphoreType.DMA((56,)),
            pltpu.SemaphoreType.DMA((56,)),
            pltpu.SemaphoreType.DMA((30,)),
            pltpu.SemaphoreType.REGULAR,
        ]
        vspec = pl.BlockSpec(memory_space=pltpu.VMEM)
        whole = pl.pallas_call(
            functools.partial(kernel, (leaves, across, size, ups, count, cap), list(bufs)),
            out_shape=jax.ShapeDtypeStruct((4 * count, LANES), F32),
            in_specs=[pl.BlockSpec(memory_space=pl.ANY)] * 30,
            out_specs=vspec,
            scratch_shapes=scratch,
            compiler_params=pltpu.CompilerParams(
                collective_id=0, has_side_effects=True, vmem_limit_bytes=60 * 1024 * 1024
            ),
        )(*arrays)
        return tuple(whole[i * count : (i + 1) * count] for i in range(4))

    spread_axes = ("leaf", "grid")
    level = (P(None, spread_axes), P(spread_axes, None), P(spread_axes, None), P(spread_axes, None), P(spread_axes))
    mid = level + (P(spread_axes, None), P(), P(spread_axes))
    return jax.shard_map(
        shards,
        mesh=mesh,
        in_specs=mid * 3 + level + (P(),),
        out_specs=(P(None, spread_axes),) * 4,
        check_vma=False,
    )
```

```python
import functools

import jax
import jax.numpy as jnp
from jax import lax
from jax.experimental import pallas as pl
from jax.experimental.pallas import tpu as pltpu
from jax.sharding import PartitionSpec as P

RANK = 128
LANES = 128
NEAR = 8
LOGICAL = pl.DeviceIdType.LOGICAL
F32 = jnp.float32
BF16 = jnp.bfloat16


def once(a, b, ca, cb):
    return lax.dot_general(a, b, (((ca,), (cb,)), ((), ())), preferred_element_type=F32)


def halves(x):
    hi = x.astype(BF16)
    return hi, (x - hi.astype(F32)).astype(BF16)


def stacked(x):
    hi = x.astype(BF16).astype(F32)
    return jnp.concatenate([hi, x - hi], axis=0).astype(BF16)


def times(a, b, cb):
    bh, bl = b
    n = a.shape[0]
    both = once(stacked(a), bh, 1, cb)
    return both[:n] + (both[n:] + once(a.astype(BF16), bl, 1, cb))


def mult(a, b):
    return times(a, halves(b), 0)


def outer(a, b):
    return times(a, halves(b), 1)


def inner(a, b):
    ah, al = halves(a)
    bh, bl = halves(b)
    return once(ah, bh, 0, 0) + (once(al, bh, 0, 0) + once(ah, bl, 0, 0))


def pick(x, onehot):
    n = x.shape[0]
    both = once(stacked(x), onehot, 1, 1)
    return both[:n] + both[n:]


def spread(rows, onehot, groups, count):
    m = groups * count
    wide = onehot.shape[1] // groups
    both = once(stacked(rows.T[:m]), onehot, 1, 0)
    out = None
    for g in range(groups):
        lanes = slice(g * wide, (g + 1) * wide)
        part = both[g * count : (g + 1) * count, lanes] + both[m + g * count : m + (g + 1) * count, lanes]
        out = part if out is None else out + part
    return out


def diagonal(x, groups, again=1):
    count, wide = x.shape
    zero = jnp.zeros((count, wide), F32)
    rows = [
        jnp.concatenate([x if h == g else zero for h in range(groups)], axis=1) for g in range(groups)
    ]
    rows = rows * again
    left = LANES - len(rows) * count
    if left:
        rows.append(jnp.zeros((left, groups * wide), F32))
    return jnp.concatenate(rows, axis=0)


def kernel(cfg, names, *refs):
    leaves, across, size, ups, count, cap = cfg
    total_devices = leaves * across
    count_in = 30
    given, out = refs[:count_in], refs[count_in]
    outs = [out.at[pl.ds(i * count, count)] for i in range(4)]
    m = dict(zip(names, refs[count_in + 1 : -4]))
    send_sem, recv_sem, load_sem, ready = refs[-4:]
    held = [m["in", i] for i in range(count_in)]
    (src, blk, exp, bas, piv) = [held[4 * i : 4 * i + 4] for i in range(5)]
    cpl, tgt, rnk = held[20:23], held[23:26], held[26:30]
    loads = [pltpu.make_async_copy(given[i], held[i], load_sem.at[i]) for i in range(count_in)]
    sems = {}
    parts = {}

    me = lax.axis_index("leaf") * across + lax.axis_index("grid")
    near = me % NEAR
    far = me // NEAR
    nb = [s // NEAR for s in size]
    plane = size[1]
    fars = nb[3]

    def sem_of(name):
        return sems.setdefault(name, len(sems))

    def remote(a, b, sem, peer):
        return pltpu.make_async_remote_copy(
            src_ref=a,
            dst_ref=b,
            send_sem=send_sem.at[sem],
            recv_sem=recv_sem.at[sem],
            device_id=peer,
            device_id_type=LOGICAL,
        )

    def wait_for(part, sem):
        pltpu.make_async_copy(part, part, sem).wait()

    ring = nb[1]

    def farthest(n):
        return sorted(range(n), key=lambda d: -min(d, n - d))

    def fan(group, stride, *sets):
        idx = me // stride % group
        base = me - idx * stride
        for name, source, dest, part in sets:
            sem_of(name)
            parts[name] = part

        def go(q):
            for name, source, dest, part in sets:
                remote(source(q), dest(idx), sem_of(name), base + q * stride).start()

        if stride == NEAR:
            rows = group // ring
            for dy in farthest(rows):
                line = (idx // ring + dy) % rows * ring
                for dz in farthest(ring):
                    if dy or dz:
                        go(line + (idx + dz) % ring)
        elif group == plane:
            for dz in farthest(ring)[:-1]:
                line = (idx // NEAR + dz) % ring * NEAR

                def body(k, carry, line=line):
                    go(line + k)
                    return carry

                lax.fori_loop(0, NEAR, body, 0, unroll=True)
            for k in range(1, NEAR):
                go(idx // NEAR * NEAR + (idx + k) % NEAR)
        elif group == NEAR:
            for dx in farthest(across):
                for dc in (1, 0):
                    if dx or dc:
                        go((idx // across + dc) % 2 * across + (idx + dx) % across)
        else:
            for d in farthest(group)[:-1]:
                go((idx + d) % group)

    def arrive(name):
        wait_for(parts[name], recv_sem.at[sem_of(name)])

    def slots(name, group):
        buf = m[name]
        return buf.at[pl.ds(0, group - 1)]

    def spread_own(name, group, stride):
        buf = m[name]
        idx = me // stride % group
        fan(group, stride, (name, lambda q: buf.at[idx], lambda i: buf.at[i], slots(name, group)))

    barrier = pltpu.get_barrier_semaphore()

    def greet_near(sem):
        def body(k, carry):
            peer = far * NEAR + (near + k) % NEAR
            pl.semaphore_signal(sem, inc=1, device_id=peer, device_id_type=LOGICAL)
            return carry

        lax.fori_loop(1, NEAR, body, 0)

    def greet_ring(sem):
        for dz in farthest(ring)[:-1]:
            peer = (far // ring * ring + (far + dz) % ring) * NEAR + near
            pl.semaphore_signal(sem, inc=1, device_id=peer, device_id_type=LOGICAL)

    def greet_z(sem, step):
        for dz in (step, ring - step):
            peer = (far // ring * ring + (far + dz) % ring) * NEAR + near
            pl.semaphore_signal(sem, inc=1, device_id=peer, device_id_type=LOGICAL)

    def greet_y(sem):
        for dy in (1, fars // ring - 1):
            peer = (far + dy * ring) % fars * NEAR + near
            pl.semaphore_signal(sem, inc=1, device_id=peer, device_id_type=LOGICAL)

    soon = (0, 12)
    for i in soon:
        loads[i].start()
    greet_z(barrier, 1)
    greet_y(barrier)
    greet_near(barrier)
    rest = [i for i in range(count_in) if i not in soon]
    for i in rest:
        loads[i].start()

    def mask(level, which, front):
        ranks = rnk[level][...].astype(F32)
        axis = 1 if level < 2 else 0
        line = ranks[which : which + 1, :] if level < 2 else ranks[:, which : which + 1]
        here = lax.broadcasted_iota(jnp.int32, line.shape, axis) == front
        rank = jnp.sum(jnp.where(here, line, 0.0), axis=axis, keepdims=True)
        col = lax.broadcasted_iota(jnp.int32, (count, RANK), 1).astype(F32)
        return (col < rank).astype(F32)

    def q_of(level):
        return bas[level][:, :RANK]

    def v_of(level):
        return bas[level][:, RANK:]

    def tiles_of(level):
        n = nb[level + 1]
        return NEAR * n // LANES, LANES // n

    def keep(name, value):
        hi, lo = halves(value)
        m[name, "h"][...] = hi
        m[name, "l"][...] = lo

    def kept(name):
        return m[name, "h"][...], m[name, "l"][...]

    four = size[0]
    my4 = me % four
    for i in soon:
        loads[i].wait()
    s0 = src[0][...]
    m["f1"][my4] = mult(s0, q_of(0))
    pl.semaphore_wait(barrier, NEAR - 1 + 4)
    spread_own("f1", four, 1)
    greet_z(ready.at[0], 1)
    greet_y(ready.at[0])
    for i in rest:
        loads[i].wait()
    front = [me // n for n in size]
    head = [mask(level, 0, front[level]) for level in range(4)]
    side = [mask(level, 1, front[level]) for level in range(3)]
    below = [None] + [
        [mask(level, 1, front[level + 1] * 2 + child) for child in range(2)] for level in (1, 2)
    ]
    local0 = mult(s0, blk[0][...])
    own0 = inner(exp[0][...], v_of(0))
    m["c0"][my4] = own0
    keep("own", own0)
    lv0 = mult(local0, v_of(0))

    slice_rows = RANK // NEAR
    root_piv = jnp.broadcast_to(piv[3][...], (LANES, LANES)).T
    crosses = [
        inner(exp[1][...], v_of(1)),
        inner(exp[2][...], v_of(2)),
        inner(exp[3][...] * root_piv, exp[3][...]),
    ]
    for j, cross in enumerate(crosses):
        buf, at = (m["xp1"], 0) if j == 0 else (m["xp2"], (j - 1) * slice_rows)
        buf[:, at : at + slice_rows, :] = cross.reshape(NEAR, slice_rows, RANK)

    def split_targets(level):
        sep = size[level + 1] * LANES
        t = tgt[level][...]
        upd = t >= sep
        rel = jnp.where(upd, t - sep, t)
        return rel // LANES, rel % LANES + jnp.where(upd, LANES, 0)

    def pack_leaf():
        u = ups[0]
        dst, low = split_targets(0)
        ri = lax.broadcasted_iota(jnp.int32, (u, u), 0)
        ci = lax.broadcasted_iota(jnp.int32, (u, u), 1)
        dst_f = dst.astype(F32)
        dst_c = jnp.sum(jnp.where(ri == ci, jnp.broadcast_to(dst_f, (u, u)), 0.0), axis=1, keepdims=True)
        rank = jnp.sum(
            jnp.where((dst_c == dst_f) & (ri < ci), 1.0, 0.0), axis=0, keepdims=True
        ).astype(jnp.int32)
        slot = rank * plane + dst
        ch, cl = halves(cpl[0][...])
        lowmat = None
        li = lax.broadcasted_iota(jnp.int32, (LANES, u), 0)
        for s in range(cap):
            si = lax.broadcasted_iota(jnp.int32, (plane, u), 0) + s * plane
            hit = (si == slot).astype(F32).astype(BF16)
            lanes = slice(s * RANK, (s + 1) * RANK)
            high, low_part = once(hit, ch, 1, 0), once(hit, cl, 1, 0)
            m["hch"][:, lanes] = high.astype(BF16)
            m["hcl"][:, lanes] = low_part.astype(BF16)
            m["hx"][my4, s * plane : (s + 1) * plane, :] = high + low_part
            mine = jnp.where(li == cap * count + s, low.astype(F32), 0.0).astype(BF16)
            part = once(hit, mine, 1, 1)
            lowmat = part if lowmat is None else lowmat + part
        m["low0"][...] = lowmat

    def pack_couple(level):
        n = nb[level + 1]
        dst, low = split_targets(level)
        slot = dst % NEAR * n + dst // NEAR
        si = lax.broadcasted_iota(jnp.int32, (NEAR * n, LANES), 0)
        h = (si == slot).astype(F32).astype(BF16)
        m["h", level][...] = h
        hi, lo = [once(h, piece, 1, 0) for piece in halves(cpl[level][...])]
        m["pa", level][...] = (hi + lo).reshape(NEAR, n, RANK)
        rows = jnp.broadcast_to(low, (count, LANES)).astype(F32).astype(BF16)
        bi = lax.broadcasted_iota(jnp.int32, (n, LANES), 0) * NEAR
        m["ohr", level][...] = jnp.concatenate(
            [(bi + k == dst).astype(F32) for k in range(NEAR)], axis=1
        ).astype(BF16)
        return once(rows, h, 1, 1)

    low1, low2 = pack_couple(1), pack_couple(2)
    ri = lax.broadcasted_iota(jnp.int32, (count, LANES), 0)
    for t in range(2):
        two = low2[:, t * LANES : (t + 1) * LANES]
        m["lows"][t] = jnp.where(ri == 0, two, jnp.where(ri == 1, low1, 0.0))
    pack_leaf()

    def fan_near(name, source, dest):
        fan(NEAR, 1, (name, source, lambda i: dest.at[i], dest.at[pl.ds(0, NEAR - 1)]))

    def scatter_near(name, source):
        m[name][near] = m[source][near]
        fan_near(name, lambda q: m[source].at[q], m[name])

    pl.semaphore_wait(ready.at[0], 4)
    greet_z(ready.at[1], 2)
    scatter_near("xr1", "xp1")
    m["la"][near] = m["lows"][near // 4]
    fan_near("la", lambda q: m["lows"].at[q // 4], m["la"])
    scatter_near(("ra", 1), ("pa", 1))

    for level in (1, 2):
        wv = mult(blk[level][...], v_of(level))
        keep(("qw", level), jnp.concatenate([q_of(level), wv], axis=1))
    wpp = mult(blk[3][...] * piv[3][...], exp[3][...])
    keep(("qw", 3), jnp.concatenate([q_of(3), wpp], axis=1))

    pl.semaphore_wait(ready.at[1], 2)
    greet_near(ready.at[2])
    greet_ring(ready.at[2])
    arrive("f1")
    hq0 = jnp.sum(m["f1"][...], axis=0) * head[0]
    m["fv"][my4] = lv0 + times(hq0, kept("own"), 0)
    spread_own("fv", four, 1)
    y0 = local0 + outer(hq0, exp[0][...])
    scatter_near(("ra", 2), ("pa", 2))
    scatter_near("xr2", "xp2")
    z0 = y0 * piv[0][...]
    m["zx"][my4] = mult(z0, exp[0][...])
    arrive("xr1")
    m["xb1"][far % ring] = jnp.sum(m["xr1"][...], axis=0)
    spread_own("xb1", ring, NEAR)
    arrive("fv")
    w0 = jnp.sum(m["fv"][...], axis=0) * side[0]

    def leaf_rows(a, b):
        ah, al = a
        bh, bl = halves(b)
        out = once(ah, bh, 1, 1) + once(ah, bl, 1, 1)
        return out if al is None else out + once(al, bh, 1, 1)

    place = me % plane

    def send_leaf(rows, got, row):
        m[got][pl.ds(place, 1), :] = m[rows][pl.ds(row(place), 1), :]
        fan(
            plane,
            1,
            (
                got,
                lambda q: m[rows].at[pl.ds(row(q), 1)],
                lambda i: m[got].at[pl.ds(i, 1)],
                m[got].at[pl.ds(0, plane - 1)],
            ),
        )

    hc = (m["hch"][...], m["hcl"][...])
    m["s0"][...] = leaf_rows(hc, diagonal(-w0, cap)) + m["low0"][...]
    pl.semaphore_wait(ready.at[2], NEAR - 1 + ring - 1)
    send_leaf("s0", "r0", lambda q: q)

    def store_row(buf, i, row):
        buf[pl.ds(i, 1), :] = row

    def forward_rows(level, table, got, name):
        n = nb[level + 1]
        per = tiles_of(level)[1]
        idx = far % n
        first = near % per * n
        store_row(m[got], idx, m[table][pl.ds(first + idx, 1), :])
        return (
            name,
            lambda q: m[table].at[pl.ds(first + q, 1)],
            lambda i: m[got].at[pl.ds(i, 1)],
            m[got].at[pl.ds(0, n - 1)],
        )

    def transposed(x):
        return jnp.concatenate([x, jnp.zeros((LANES - x.shape[0], LANES), F32)], axis=0).T

    def couple_set(level):
        n = nb[level + 1]
        ra, rb = m["ra", level], m["rb", level]
        idx = far % n
        rb[:, pl.ds(idx, 1), :] = ra[:, pl.ds(idx, 1), :]
        return (
            ("rb", level),
            lambda q: ra.at[:, pl.ds(q, 1)],
            lambda i: rb.at[:, pl.ds(i, 1)],
            rb.at[:, pl.ds(0, n - 1)],
        )

    arrive("la")
    m["tl"][...] = transposed(m["la"][...].reshape(NEAR * count, LANES))
    for level in (1, 2):
        arrive(("ra", level))
        sets = [forward_rows(level, "tl", ("lb", level), ("lb", level))]
        if level == 1:
            sets.append(couple_set(level))
        fan(nb[level + 1], NEAR, *sets)
    arrive("xr2")
    m["xb2"][far % ring] = jnp.sum(m["xr2"][...], axis=0)
    spread_own("xb2", ring, NEAR)
    arrive("xb1")
    m["xg1"][near] = jnp.sum(m["xb1"][...], axis=0)
    spread_own("xg1", NEAR, 1)
    spread_own("zx", four, 1)

    def build_hits(level):
        n = nb[level + 1]
        wide = 2 * LANES if level == 1 else LANES
        arrive(("lb", level))
        lb = m["lb", level][...]
        lane = lax.broadcasted_iota(jnp.int32, (n, wide), 1).astype(F32)
        at = 2 - level
        hits = [(lane == lb[:, k * count + at : k * count + at + 1]).astype(F32) for k in range(NEAR)]
        m["ohf", level][...] = jnp.concatenate(hits, axis=1).astype(BF16)
        m["ohg", level][...] = jnp.concatenate(hits, axis=0).astype(BF16)
        return hits

    def build_g(level, hits):
        n = nb[level + 1]
        arrive(("rb", level))
        half = n // 2
        for child in range(2):
            rows = slice(child * half, (child + 1) * half)
            got = m["rb", level][:, rows, :].reshape(NEAR * half, RANK)
            hot = jnp.concatenate([hit[rows] for hit in hits], axis=0).astype(BF16)
            hi, lo = [once(piece, hot, 0, 0) for piece in halves(got)]
            gh, gl = halves(hi + lo)
            out = slice(child * RANK, (child + 1) * RANK)
            m[("g", level), "h"][out, :] = gh
            m[("g", level), "l"][out, :] = gl

    def send_up(level, b, u):
        count_tiles, per = tiles_of(level)
        both = times(b, kept(("qw", level)), 0)
        tile = pick(u, m["h", level][...])
        for t in range(count_tiles):
            m["fs", level][t] = jnp.concatenate(
                [both[:, :RANK], both[:, RANK:], tile[:, t * LANES : (t + 1) * LANES]], axis=0
            )
        fs, fa = m["fs", level], m["fa", level]
        fa[near] = fs[near // per]
        fan_near(("fa", level), lambda q: fs.at[q // per], fa)

    def rows_of(level, kind, tiles):
        n = nb[level + 1]
        table = m["t" + kind, level]
        table[...] = transposed(tiles.reshape(NEAR * count, LANES))
        return table[pl.ds(pl.multiple_of(near % tiles_of(level)[1] * n, 8), n), :]

    def send_far(level, kind, first, second, rows):
        n = nb[level + 1]
        half = n // 2
        idx = far % n
        source, got = m[kind + "s", level], m[kind + "b", level]
        source[:half, :count, :] = jnp.broadcast_to(first[None], (half, count, RANK))
        source[half:, :count, :] = jnp.broadcast_to(second[None], (half, count, RANK))
        source[:, count, :] = rows
        used = pl.ds(0, count + 1)
        got[idx, : count + 1, :] = source[idx, : count + 1, :]
        fan(
            n,
            NEAR,
            (
                (kind, level),
                lambda q: source.at[q, used],
                lambda i: got.at[i, used],
                got.at[pl.ds(0, n - 1), used],
            ),
        )

    def send_on(level):
        arrive(("fa", level))
        fa = m["fa", level]
        tot = jnp.sum(fa[:, : 2 * count, :], axis=0)
        hq = tot[:count] * head[level]
        w = tot[count:] + times(hq, kept(("cross", level)), 0)
        rows = rows_of(level, "w", fa[:, 2 * count :, :])
        send_far(level, "w", w, w, rows)
        m["hb", level][far % nb[level]] = hq
        spread_own(("hb", level), nb[level], NEAR)
        return rows

    def sums_up(level):
        half = nb[level + 1] // 2
        arrive(("w", level))
        wb = m["wb", level]
        ws = [
            jnp.sum(wb[child * half : (child + 1) * half, :count, :], axis=0) * below[level][child]
            for child in range(2)
        ]
        return jnp.concatenate(ws, axis=1)

    def receive_up(level, ws):
        rows = spread(m["wb", level][:, count, :], m["ohf", level][...], NEAR, count)
        return rows - times(ws, kept(("g", level)), 0)

    def near_sum(name):
        arrive(name)
        return jnp.sum(m[name][...], axis=0)

    def send_down(level, full):
        count_tiles, per = tiles_of(level)
        sp = times(full, kept(("g", level)), 1)
        tile = pick(full, m["ohg", level][...])
        for t in range(count_tiles):
            m["bs", level][t] = jnp.concatenate(
                [sp[:, :RANK], sp[:, RANK:], tile[:, t * LANES : (t + 1) * LANES]], axis=0
            )
        bs, ba = m["bs", level], m["ba", level]
        ba[near] = bs[near // per]
        fan_near(("ba", level), lambda q: bs.at[q // per], ba)

    def send_further(level):
        arrive(("ba", level))
        ba = m["ba", level]
        tot = jnp.sum(ba[:, : 2 * count, :], axis=0)
        send_far(level, "s", tot[:count], tot[count:], rows_of(level, "s", ba[:, 2 * count :, :]))

    def receive_down(level, base):
        arrive(("s", level))
        sb = m["sb", level]
        s = jnp.sum(sb[:, :count, :], axis=0) * side[level]
        x = base - times(s, kept(("t", level)), 1)
        xu = spread(sb[:, count, :], m["ohr", level][...], NEAR, count)
        return x, xu

    saved = {}

    def solve_front(level, local):
        arrive(("hb", level))
        hq = jnp.sum(m["hb", level][...], axis=0)
        z = (local + outer(hq, exp[level][...])) * piv[level][...]
        saved[level] = z
        m["za", level][near] = mult(z, exp[level][...])
        spread_own(("za", level), NEAR, 1)

    def pass_zp(level):
        m["zb", level][far % nb[level]] = near_sum(("za", level))
        spread_own(("zb", level), nb[level], NEAR)

    def base_of(level, zp):
        return outer(saved[level], blk[level][...]) + outer(zp * head[level], q_of(level))

    def tail_of(level, wv):
        qm = q_of(level) * jnp.broadcast_to(head[level][:1], (LANES, RANK))
        keep(("t", level), wv + times(qm, kept(("cross", level)), 0))

    def wv_of(level):
        qh, ql = kept(("qw", level))
        return qh[:, RANK:].astype(F32) + ql[:, RANK:].astype(F32)

    arrive("r0")
    r0 = m["r0"][...]
    lane = lax.broadcasted_iota(jnp.int32, (plane, 2 * LANES), 1).astype(F32)
    at = cap * count
    m["oh0"][...] = jnp.concatenate(
        [(lane == r0[:, at + s : at + s + 1]).astype(F32) for s in range(cap)], axis=1
    ).astype(BF16)
    inc = spread(r0, m["oh0"][...], cap, count)
    b1 = src[1][...] + inc[:, :LANES]
    send_up(1, b1, inc[:, LANES:])
    fan(nb[3], NEAR, couple_set(2))

    local1 = mult(b1, blk[1][...])
    saved[0] = z0
    arrive("zx")
    base0 = base_of(0, jnp.sum(m["zx"][...], axis=0))
    build_g(1, build_hits(1))
    arrive("xg1")
    keep(("cross", 1), m["xg1"][...].reshape(RANK, RANK))
    hits = build_hits(2)
    kh, kl = kept(("qw", 3))
    hot = m["ohg", 2][...]
    m["kp"][...] = (once(hot, kh, 1, 0) + once(hot, kl, 1, 0)).reshape(NEAR, fars, 2 * RANK)
    scatter_near("kr", "kp")
    arrive("xb2")
    m["xy"][me // plane] = jnp.sum(m["xb2"][...], axis=0)
    spread_own("xy", total_devices // plane, plane)
    send_on(1)
    ks, kb = m["ks"], m["kb"]
    for half in range(2):
        ks[:, half] = m["kp"][:, :, half * RANK : (half + 1) * RANK]
    kb[:, :, pl.ds(far, 1), :] = ks[:, :, pl.ds(far, 1), :]
    fan(
        fars,
        NEAR,
        (
            "kb",
            lambda q: ks.at[:, :, pl.ds(q, 1)],
            lambda i: kb.at[:, :, pl.ds(i, 1)],
            kb.at[:, :, pl.ds(0, fars - 1)],
        ),
    )

    arrive("xy")
    pair = me // plane // 2 * 2
    m["xg2"][near, :slice_rows, :] = jnp.sum(m["xy"][pl.ds(pair, 2), :slice_rows, :], axis=0)
    m["xg2"][near, slice_rows:, :] = jnp.sum(m["xy"][:, slice_rows:, :], axis=0)
    spread_own("xg2", NEAR, 1)
    build_g(2, hits)
    gh, gl = kept(("g", 2))
    both = once(gh, kh, 1, 0) + (once(gl, kh, 1, 0) + once(gh, kl, 1, 0))
    m["yp"][...] = both.reshape(NEAR, 2 * RANK // NEAR, 2 * RANK)
    scatter_near("yr", "yp")
    tail_of(1, wv_of(1))

    inc = receive_up(1, sums_up(1))
    b2 = src[2][...] + inc[:, :LANES]
    send_up(2, b2, inc[:, LANES:])
    m["yg"][near] = near_sum("yr")
    spread_own("yg", NEAR, 1)

    local2 = mult(b2, blk[2][...])
    arrive("xg2")
    keep(("cross", 2), m["xg2"][:, :slice_rows, :].reshape(RANK, RANK))
    rows = send_on(2)
    keep(("cross", 3), m["xg2"][:, slice_rows:, :].reshape(RANK, RANK))
    core = near // across
    per = LANES // fars
    turned = transposed(rows)
    passing = []
    for t in range(NEAR // per):
        group = [turned[(t * per + k) * count : (t * per + k + 1) * count] for k in range(per)]
        passing.append(sum(pltpu.roll(group[k], k * fars, 1) for k in range(1, per)) + group[0])
    arrive("kb")
    pulled = jnp.concatenate([kb[:, half].reshape(NEAR * fars, RANK) for half in range(2)], axis=1)
    sr = times(src[3][...], kept(("qw", 3)), 0)
    sr = sr + times(jnp.concatenate(passing, axis=1), halves(pulled), 0)
    m["sr"][near] = jnp.concatenate([sr[:, :RANK], sr[:, RANK:]], axis=0)
    spread_own("sr", NEAR, 1)
    spread_own("c0", four, 1)
    solve_front(1, local1)
    tail_of(2, wv_of(2))

    arrive("yg")
    y = m["yg"][...].reshape(2 * RANK, 2 * RANK)
    keep("y", y)
    yq = y[:, :RANK] * jnp.broadcast_to(head[3][:1], (2 * RANK, RANK))
    yv = y[:, RANK:] + times(yq, kept(("cross", 3)), 0)
    keep("yh", jnp.where(core == 0, yq, yv))
    tot = near_sum("sr")
    sq = tot[:count] * head[3]
    mine = jnp.where(core == 0, sq, tot[count:] + times(sq, kept(("cross", 3)), 0))
    ws = sums_up(2)
    m["fb"][far] = mine - times(ws, kept("yh"), 0)
    spread_own("fb", fars, NEAR)
    b3 = src[3][...] + receive_up(2, ws)
    early = outer(mult(b3, blk[3][...]) * piv[3][...], blk[3][...])
    send_down(2, early)
    solve_front(2, local2)
    pass_zp(1)
    arrive("c0")
    keep(("cross", 0), jnp.sum(m["c0"][...], axis=0))
    tail_of(0, mult(blk[0][...], v_of(0)))
    arrive(("ba", 2))
    ba = m["ba", 2]
    sums = jnp.sum(ba[:, : 2 * count, :], axis=0)
    early_rows = rows_of(2, "s", ba[:, 2 * count :, :])
    pass_zp(2)
    arrive("kr")
    keep("ka", m["kr"][...].reshape(NEAR * fars, 2 * RANK))
    arrive("fb")
    m["fc"][core] = jnp.sum(m["fb"][...], axis=0)
    spread_own("fc", 2, across)
    arrive("fc")
    ends = jnp.concatenate([m["fc"][1] * head[3], m["fc"][0]], axis=1)
    sums = jnp.concatenate([sums[:count], sums[count:]], axis=1) + times(ends, kept("y"), 1)
    late = times(ends, kept("ka"), 1)
    late = [
        pltpu.roll(late[:, k // per * LANES : (k // per + 1) * LANES], (LANES - k % per * fars) % LANES, 1)
        for k in range(NEAR)
    ]
    late = transposed(jnp.concatenate(late, axis=0))[:fars]
    send_far(2, "s", sums[:, :RANK], sums[:, RANK:], early_rows + late)
    spread_own("hx", four, 1)
    outs[3][...] = early + times(ends, kept(("qw", 3)), 1)

    arrive(("zb", 1))
    base1 = base_of(1, jnp.sum(m["zb", 1][...], axis=0))
    arrive(("zb", 2))
    base2 = base_of(2, jnp.sum(m["zb", 2][...], axis=0))
    x, xu = receive_down(2, base2)
    send_down(1, jnp.concatenate([x, xu], axis=1))
    outs[2][...] = x
    send_further(1)
    arrive("hx")
    for k in range(four):
        at = slice(k * cap * plane, (k + 1) * cap * plane)
        packed = m["hx"][k] * jnp.broadcast_to(side[0][:1], (cap * plane, RANK))
        m["hxh"][at, :], m["hxl"][at, :] = halves(times(packed, kept(("t", 0)), 1))
    x, xu = receive_down(1, base1)
    full = diagonal(jnp.concatenate([x, xu], axis=1), cap, four)
    rows = leaf_rows((m["oh0"][...], None), full)
    ri = lax.broadcasted_iota(jnp.int32, (plane, LANES), 0)
    li = lax.broadcasted_iota(jnp.int32, (plane, LANES), 1)
    rows = jnp.where(li // (cap * count) == ri % four, rows, 0.0)
    rows = rows + pltpu.roll(rows, plane - 1, 0)
    m["s0b"][...] = rows + pltpu.roll(rows, plane - 2, 0)
    send_leaf("s0b", "r0b", lambda q: q // four * four)
    outs[1][...] = x
    for name, part in parts.items():
        wait_for(part, send_sem.at[sem_of(name)])
    arrive("r0b")
    rows = transposed(m["r0b"][...])
    pieces = [rows[g * count : (g + 1) * count] for g in range(four * cap)]
    pairs = [pieces[2 * g] + pltpu.roll(pieces[2 * g + 1], plane, 1) for g in range(four * cap // 2)]
    outs[0][...] = base0 - times(jnp.concatenate(pairs, axis=1), (m["hxh"][...], m["hxl"][...]), 0)


def solution(mesh):
    leaves, across = mesh.shape["leaf"], mesh.shape["grid"]

    def shards(*args):
        levels = [args[8 * i : 8 * i + 8] for i in range(3)]
        root = args[24:30]
        (sl, bl, el, qs, pv, cl, rk, tg) = zip(*levels)
        src = list(sl) + [root[0]]
        blk = list(bl) + [root[1]]
        exp = list(el) + [root[2]]
        bas = list(qs) + [root[3]]
        piv = [v.reshape(1, -1) for v in list(pv) + [root[4]]]
        rnk = [rk[0].T, rk[1].T, rk[2], root[5]]
        tgt = [t.reshape(1, -1) for t in tg]
        count = src[0].shape[0]
        ups = [t.shape[1] for t in tgt]
        fronts = [r.shape[0] for r in rk] + [root[5].shape[0]]
        size = [leaves * across // f for f in fronts]
        cap = ups[0] // size[1]
        nb = [s // NEAR for s in size]
        for v in src:
            assert v.shape == (NEAR, LANES)
        assert ups[1:] == [LANES, LANES] and cap * (count + 1) <= LANES
        assert 2 * size[1] == LANES and size[0] * cap * count == LANES
        assert nb[1] == 8 and across == 4 and size[0] == across
        assert size[2] == 2 * size[1] and size[3] == 2 * size[2] and size[1] % NEAR == 0
        assert NEAR * nb[2] == LANES and NEAR * nb[3] == 2 * LANES
        vm = lambda *s: pltpu.VMEM(s, F32)
        bits = lambda *s: pltpu.VMEM(s, BF16)
        piece = RANK // NEAR
        bufs = {
            "f1": vm(size[0], count, LANES),
            "fv": vm(size[0], count, LANES),
            "c0": vm(size[0], RANK, RANK),
            "zx": vm(size[0], count, LANES),
            "xp1": vm(NEAR, piece, RANK),
            "xr1": vm(NEAR, piece, RANK),
            "xp2": vm(NEAR, 2 * piece, RANK),
            "xr2": vm(NEAR, 2 * piece, RANK),
            "xb1": vm(nb[1], piece, RANK),
            "xb2": vm(nb[1], 2 * piece, RANK),
            "xy": vm(nb[3] // nb[1], 2 * piece, RANK),
            "xg1": vm(NEAR, piece, RANK),
            "xg2": vm(NEAR, 2 * piece, RANK),
            "lows": vm(2, count, LANES),
            "la": vm(NEAR, count, LANES),
            "tl": vm(LANES, LANES),
            "hch": bits(size[1], cap * RANK),
            "hcl": bits(size[1], cap * RANK),
            "low0": vm(size[1], LANES),
            "oh0": bits(size[1], cap * 2 * LANES),
            "fb": vm(nb[3], count, LANES),
            "ks": vm(NEAR, 2, nb[3], RANK),
            "kb": vm(NEAR, 2, nb[3], RANK),
            "sr": vm(NEAR, 2 * count, LANES),
            "kp": vm(NEAR, nb[3], 2 * RANK),
            "kr": vm(NEAR, nb[3], 2 * RANK),
            "yp": vm(NEAR, 2 * RANK // NEAR, 2 * RANK),
            "yr": vm(NEAR, 2 * RANK // NEAR, 2 * RANK),
            "yg": vm(NEAR, 2 * RANK // NEAR, 2 * RANK),
            "fc": vm(2, count, LANES),
            "hx": vm(size[0], cap * size[1], RANK),
            "hxh": bits(size[0] * cap * size[1], RANK),
            "hxl": bits(size[0] * cap * size[1], RANK),
        }
        for name in ("s0", "r0", "s0b", "r0b"):
            bufs[name] = vm(size[1], LANES)
        for half in "hl":
            bufs["ka", half] = bits(NEAR * nb[3], 2 * RANK)
            bufs["y", half] = bits(2 * RANK, 2 * RANK)
            bufs["yh", half] = bits(2 * RANK, RANK)
        for i in range(4):
            for half in "hl":
                bufs[("cross", i), half] = bits(RANK, RANK)
                bufs[("qw", i), half] = bits(LANES, 2 * RANK)
                bufs[("t", i), half] = bits(LANES, RANK)
                bufs["own", half] = bits(RANK, RANK)
        for i in (1, 2):
            n = nb[i + 1]
            wide = 2 * LANES if i == 1 else LANES
            tiles = NEAR * n // LANES
            bufs["h", i] = bits(NEAR * n, LANES)
            bufs["ohr", i] = bits(n, NEAR * LANES)
            bufs["ohf", i] = bits(n, NEAR * wide)
            bufs["ohg", i] = bits(NEAR * n, wide)
            bufs["pa", i] = vm(NEAR, n, RANK)
            bufs["ra", i] = vm(NEAR, n, RANK)
            bufs["rb", i] = vm(NEAR, n, RANK)
            bufs["lb", i] = vm(n, LANES)
            for half in "hl":
                bufs[("g", i), half] = bits(2 * RANK, wide)
            bufs["fs", i] = vm(tiles, 3 * count, LANES)
            bufs["fa", i] = vm(NEAR, 3 * count, LANES)
            bufs["bs", i] = vm(tiles, 3 * count, LANES)
            bufs["ba", i] = vm(NEAR, 3 * count, LANES)
            for kind in "ws":
                bufs["t" + kind, i] = vm(LANES, LANES)
                bufs[kind + "s", i] = vm(n, 2 * count, LANES)
                bufs[kind + "b", i] = vm(n, 2 * count, LANES)
            bufs["hb", i] = vm(nb[i], count, LANES)
            bufs["za", i] = vm(NEAR, count, LANES)
            bufs["zb", i] = vm(nb[i], count, LANES)
        arrays = [*src, *blk, *exp, *bas, *piv, *cl, *tgt, *rnk]
        for i, v in enumerate(arrays):
            bufs["in", i] = pltpu.VMEM(v.shape, v.dtype)
        scratch = list(bufs.values())
        scratch += [
            pltpu.SemaphoreType.DMA((56,)),
            pltpu.SemaphoreType.DMA((56,)),
            pltpu.SemaphoreType.DMA((30,)),
            pltpu.SemaphoreType.REGULAR((3,)),
        ]
        vspec = pl.BlockSpec(memory_space=pltpu.VMEM)
        whole = pl.pallas_call(
            functools.partial(kernel, (leaves, across, size, ups, count, cap), list(bufs)),
            out_shape=jax.ShapeDtypeStruct((4 * count, LANES), F32),
            in_specs=[pl.BlockSpec(memory_space=pl.ANY)] * 30,
            out_specs=vspec,
            scratch_shapes=scratch,
            compiler_params=pltpu.CompilerParams(
                collective_id=0, has_side_effects=True, vmem_limit_bytes=60 * 1024 * 1024
            ),
        )(*arrays)
        return tuple(whole[i * count : (i + 1) * count] for i in range(4))

    spread_axes = ("leaf", "grid")
    level = (P(None, spread_axes), P(spread_axes, None), P(spread_axes, None), P(spread_axes, None), P(spread_axes))
    mid = level + (P(spread_axes, None), P(), P(spread_axes))
    return jax.shard_map(
        shards,
        mesh=mesh,
        in_specs=mid * 3 + level + (P(),),
        out_specs=(P(None, spread_axes),) * 4,
        check_vma=False,
    )
```

```python
import functools

import jax
import jax.numpy as jnp
from jax import lax
from jax.experimental import pallas as pl
from jax.experimental.pallas import tpu as pltpu
from jax.sharding import PartitionSpec as P

RANK = 128
LANES = 128
NEAR = 8
LOGICAL = pl.DeviceIdType.LOGICAL
F32 = jnp.float32
BF16 = jnp.bfloat16


def once(a, b, ca, cb):
    return lax.dot_general(a, b, (((ca,), (cb,)), ((), ())), preferred_element_type=F32)


def halves(x):
    hi = x.astype(BF16)
    return hi, (x - hi.astype(F32)).astype(BF16)


def stacked(x):
    hi = x.astype(BF16).astype(F32)
    return jnp.concatenate([hi, x - hi], axis=0).astype(BF16)


def times(a, b, cb):
    bh, bl = b
    n = a.shape[0]
    both = once(stacked(a), bh, 1, cb)
    return both[:n] + (both[n:] + once(a.astype(BF16), bl, 1, cb))


def mult(a, b):
    return times(a, halves(b), 0)


def outer(a, b):
    return times(a, halves(b), 1)


def inner(a, b):
    ah, al = halves(a)
    bh, bl = halves(b)
    return once(ah, bh, 0, 0) + (once(al, bh, 0, 0) + once(ah, bl, 0, 0))


def pick(x, onehot):
    n = x.shape[0]
    both = once(stacked(x), onehot, 1, 1)
    return both[:n] + both[n:]


def spread(rows, onehot, groups, count):
    m = groups * count
    wide = onehot.shape[1] // groups
    both = once(stacked(rows.T[:m]), onehot, 1, 0)
    out = None
    for g in range(groups):
        lanes = slice(g * wide, (g + 1) * wide)
        part = both[g * count : (g + 1) * count, lanes] + both[m + g * count : m + (g + 1) * count, lanes]
        out = part if out is None else out + part
    return out


def diagonal(x, groups, again=1):
    count, wide = x.shape
    zero = jnp.zeros((count, wide), F32)
    rows = [
        jnp.concatenate([x if h == g else zero for h in range(groups)], axis=1) for g in range(groups)
    ]
    rows = rows * again
    left = LANES - len(rows) * count
    if left:
        rows.append(jnp.zeros((left, groups * wide), F32))
    return jnp.concatenate(rows, axis=0)


def kernel(cfg, names, *refs):
    leaves, across, size, ups, count, cap = cfg
    total_devices = leaves * across
    count_in = 30
    given, out = refs[:count_in], refs[count_in]
    outs = [out.at[pl.ds(i * count, count)] for i in range(4)]
    m = dict(zip(names, refs[count_in + 1 : -4]))
    send_sem, recv_sem, load_sem, ready = refs[-4:]
    held = [m["in", i] for i in range(count_in)]
    (src, blk, exp, bas, piv) = [held[4 * i : 4 * i + 4] for i in range(5)]
    cpl, tgt, rnk = held[20:23], held[23:26], held[26:30]
    loads = [pltpu.make_async_copy(given[i], held[i], load_sem.at[i]) for i in range(count_in)]
    sems = {}
    parts = {}

    me = lax.axis_index("leaf") * across + lax.axis_index("grid")
    near = me % NEAR
    far = me // NEAR
    nb = [s // NEAR for s in size]
    plane = size[1]
    fars = nb[3]

    def sem_of(name):
        return sems.setdefault(name, len(sems))

    def remote(a, b, sem, peer):
        return pltpu.make_async_remote_copy(
            src_ref=a,
            dst_ref=b,
            send_sem=send_sem.at[sem],
            recv_sem=recv_sem.at[sem],
            device_id=peer,
            device_id_type=LOGICAL,
        )

    def wait_for(part, sem):
        pltpu.make_async_copy(part, part, sem).wait()

    ring = nb[1]

    def farthest(n):
        return sorted(range(n), key=lambda d: -min(d, n - d))

    def fan(group, stride, *sets):
        idx = me // stride % group
        base = me - idx * stride
        for name, source, dest, part in sets:
            sem_of(name)
            parts[name] = part

        def go(q):
            for name, source, dest, part in sets:
                remote(source(q), dest(idx), sem_of(name), base + q * stride).start()

        if stride == NEAR:
            rows = group // ring
            for dy in farthest(rows):
                line = (idx // ring + dy) % rows * ring
                for dz in farthest(ring):
                    if dy or dz:
                        go(line + (idx + dz) % ring)
        elif group == plane:
            for dz in farthest(ring)[:-1]:
                line = (idx // NEAR + dz) % ring * NEAR

                def body(k, carry, line=line):
                    go(line + k)
                    return carry

                lax.fori_loop(0, NEAR, body, 0, unroll=True)
            for k in range(1, NEAR):
                go(idx // NEAR * NEAR + (idx + k) % NEAR)
        elif group == NEAR:
            for dx in farthest(across):
                for dc in (1, 0):
                    if dx or dc:
                        go((idx // across + dc) % 2 * across + (idx + dx) % across)
        else:
            for d in farthest(group)[:-1]:
                go((idx + d) % group)

    def arrive(name):
        wait_for(parts[name], recv_sem.at[sem_of(name)])

    def slots(name, group):
        buf = m[name]
        return buf.at[pl.ds(0, group - 1)]

    def spread_own(name, group, stride):
        buf = m[name]
        idx = me // stride % group
        fan(group, stride, (name, lambda q: buf.at[idx], lambda i: buf.at[i], slots(name, group)))

    barrier = pltpu.get_barrier_semaphore()

    def greet_near(sem):
        def body(k, carry):
            peer = far * NEAR + (near + k) % NEAR
            pl.semaphore_signal(sem, inc=1, device_id=peer, device_id_type=LOGICAL)
            return carry

        lax.fori_loop(1, NEAR, body, 0)

    def greet_ring(sem):
        for dz in farthest(ring)[:-1]:
            peer = (far // ring * ring + (far + dz) % ring) * NEAR + near
            pl.semaphore_signal(sem, inc=1, device_id=peer, device_id_type=LOGICAL)

    def greet_z(sem, step):
        for dz in (step, ring - step):
            peer = (far // ring * ring + (far + dz) % ring) * NEAR + near
            pl.semaphore_signal(sem, inc=1, device_id=peer, device_id_type=LOGICAL)

    def greet_y(sem):
        for dy in (1, fars // ring - 1):
            peer = (far + dy * ring) % fars * NEAR + near
            pl.semaphore_signal(sem, inc=1, device_id=peer, device_id_type=LOGICAL)

    soon = (0, 12)
    for i in soon:
        loads[i].start()
    greet_z(barrier, 1)
    greet_y(barrier)
    greet_near(barrier)
    rest = [i for i in range(count_in) if i not in soon]
    for i in rest:
        loads[i].start()

    def mask(level, which, front):
        ranks = rnk[level][...].astype(F32)
        axis = 1 if level < 2 else 0
        line = ranks[which : which + 1, :] if level < 2 else ranks[:, which : which + 1]
        here = lax.broadcasted_iota(jnp.int32, line.shape, axis) == front
        rank = jnp.sum(jnp.where(here, line, 0.0), axis=axis, keepdims=True)
        col = lax.broadcasted_iota(jnp.int32, (count, RANK), 1).astype(F32)
        return (col < rank).astype(F32)

    def q_of(level):
        return bas[level][:, :RANK]

    def v_of(level):
        return bas[level][:, RANK:]

    def tiles_of(level):
        n = nb[level + 1]
        return NEAR * n // LANES, LANES // n

    def keep(name, value):
        hi, lo = halves(value)
        m[name, "h"][...] = hi
        m[name, "l"][...] = lo

    def kept(name):
        return m[name, "h"][...], m[name, "l"][...]

    four = size[0]
    my4 = me % four
    for i in soon:
        loads[i].wait()
    s0 = src[0][...]
    m["f1"][my4] = mult(s0, q_of(0))
    pl.semaphore_wait(barrier, NEAR - 1 + 4)
    spread_own("f1", four, 1)
    greet_z(ready.at[0], 1)
    greet_y(ready.at[0])
    for i in rest:
        loads[i].wait()
    front = [me // n for n in size]
    head = [mask(level, 0, front[level]) for level in range(4)]
    side = [mask(level, 1, front[level]) for level in range(3)]
    below = [None] + [
        [mask(level, 1, front[level + 1] * 2 + child) for child in range(2)] for level in (1, 2)
    ]
    local0 = mult(s0, blk[0][...])
    own0 = inner(exp[0][...], v_of(0))
    m["c0"][my4] = own0
    keep("own", own0)
    lv0 = mult(local0, v_of(0))

    slice_rows = RANK // NEAR
    root_piv = jnp.broadcast_to(piv[3][...], (LANES, LANES)).T
    crosses = [
        inner(exp[1][...], v_of(1)),
        inner(exp[2][...], v_of(2)),
        inner(exp[3][...] * root_piv, exp[3][...]),
    ]
    for j, cross in enumerate(crosses):
        buf, at = (m["xp1"], 0) if j == 0 else (m["xp2"], (j - 1) * slice_rows)
        buf[:, at : at + slice_rows, :] = cross.reshape(NEAR, slice_rows, RANK)

    def split_targets(level):
        sep = size[level + 1] * LANES
        t = tgt[level][...]
        upd = t >= sep
        rel = jnp.where(upd, t - sep, t)
        return rel // LANES, rel % LANES + jnp.where(upd, LANES, 0)

    def pack_leaf():
        u = ups[0]
        dst, low = split_targets(0)
        ri = lax.broadcasted_iota(jnp.int32, (u, u), 0)
        ci = lax.broadcasted_iota(jnp.int32, (u, u), 1)
        dst_f = dst.astype(F32)
        dst_c = jnp.sum(jnp.where(ri == ci, jnp.broadcast_to(dst_f, (u, u)), 0.0), axis=1, keepdims=True)
        rank = jnp.sum(
            jnp.where((dst_c == dst_f) & (ri < ci), 1.0, 0.0), axis=0, keepdims=True
        ).astype(jnp.int32)
        slot = rank * plane + dst
        ch, cl = halves(cpl[0][...])
        lowmat = None
        li = lax.broadcasted_iota(jnp.int32, (LANES, u), 0)
        for s in range(cap):
            si = lax.broadcasted_iota(jnp.int32, (plane, u), 0) + s * plane
            hit = (si == slot).astype(F32).astype(BF16)
            lanes = slice(s * RANK, (s + 1) * RANK)
            high, low_part = once(hit, ch, 1, 0), once(hit, cl, 1, 0)
            m["hch"][:, lanes] = high.astype(BF16)
            m["hcl"][:, lanes] = low_part.astype(BF16)
            m["hx"][my4, s * plane : (s + 1) * plane, :] = high + low_part
            mine = jnp.where(li == cap * count + s, low.astype(F32), 0.0).astype(BF16)
            part = once(hit, mine, 1, 1)
            lowmat = part if lowmat is None else lowmat + part
        m["low0"][...] = lowmat

    def pack_couple(level):
        n = nb[level + 1]
        dst, low = split_targets(level)
        slot = dst % NEAR * n + dst // NEAR
        si = lax.broadcasted_iota(jnp.int32, (NEAR * n, LANES), 0)
        h = (si == slot).astype(F32).astype(BF16)
        m["h", level][...] = h
        hi, lo = [once(h, piece, 1, 0) for piece in halves(cpl[level][...])]
        m["pa", level][...] = (hi + lo).reshape(NEAR, n, RANK)
        rows = jnp.broadcast_to(low, (count, LANES)).astype(F32).astype(BF16)
        bi = lax.broadcasted_iota(jnp.int32, (n, LANES), 0) * NEAR
        m["ohr", level][...] = jnp.concatenate(
            [(bi + k == dst).astype(F32) for k in range(NEAR)], axis=1
        ).astype(BF16)
        return once(rows, h, 1, 1)

    low1, low2 = pack_couple(1), pack_couple(2)
    ri = lax.broadcasted_iota(jnp.int32, (count, LANES), 0)
    for t in range(2):
        two = low2[:, t * LANES : (t + 1) * LANES]
        m["lows"][t] = jnp.where(ri == 0, two, jnp.where(ri == 1, low1, 0.0))
    pack_leaf()

    def fan_near(name, source, dest):
        fan(NEAR, 1, (name, source, lambda i: dest.at[i], dest.at[pl.ds(0, NEAR - 1)]))

    def scatter_near(name, source):
        m[name][near] = m[source][near]
        fan_near(name, lambda q: m[source].at[q], m[name])

    pl.semaphore_wait(ready.at[0], 4)
    greet_z(ready.at[1], 2)
    scatter_near("xr1", "xp1")
    m["la"][near] = m["lows"][near // 4]
    fan_near("la", lambda q: m["lows"].at[q // 4], m["la"])
    scatter_near(("ra", 1), ("pa", 1))

    for level in (1, 2):
        wv = mult(blk[level][...], v_of(level))
        keep(("qw", level), jnp.concatenate([q_of(level), wv], axis=1))
    wpp = mult(blk[3][...] * piv[3][...], exp[3][...])
    keep(("qw", 3), jnp.concatenate([q_of(3), wpp], axis=1))

    pl.semaphore_wait(ready.at[1], 2)
    greet_near(ready.at[2])
    greet_ring(ready.at[2])
    arrive("f1")
    hq0 = jnp.sum(m["f1"][...], axis=0) * head[0]
    m["fv"][my4] = lv0 + times(hq0, kept("own"), 0)
    spread_own("fv", four, 1)
    y0 = local0 + outer(hq0, exp[0][...])
    scatter_near(("ra", 2), ("pa", 2))
    scatter_near("xr2", "xp2")
    z0 = y0 * piv[0][...]
    m["zx"][my4] = mult(z0, exp[0][...])
    arrive("xr1")
    m["xb1"][far % ring] = jnp.sum(m["xr1"][...], axis=0)
    spread_own("xb1", ring, NEAR)
    arrive("fv")
    w0 = jnp.sum(m["fv"][...], axis=0) * side[0]

    def leaf_rows(a, b):
        ah, al = a
        bh, bl = halves(b)
        out = once(ah, bh, 1, 1) + once(ah, bl, 1, 1)
        return out if al is None else out + once(al, bh, 1, 1)

    place = me % plane

    def send_leaf(rows, got, row):
        m[got][pl.ds(place, 1), :] = m[rows][pl.ds(row(place), 1), :]
        fan(
            plane,
            1,
            (
                got,
                lambda q: m[rows].at[pl.ds(row(q), 1)],
                lambda i: m[got].at[pl.ds(i, 1)],
                m[got].at[pl.ds(0, plane - 1)],
            ),
        )

    hc = (m["hch"][...], m["hcl"][...])
    m["s0"][...] = leaf_rows(hc, diagonal(-w0, cap)) + m["low0"][...]
    pl.semaphore_wait(ready.at[2], NEAR - 1 + ring - 1)
    send_leaf("s0", "r0", lambda q: q)

    def store_row(buf, i, row):
        buf[pl.ds(i, 1), :] = row

    def forward_rows(level, table, got, name):
        n = nb[level + 1]
        per = tiles_of(level)[1]
        idx = far % n
        first = near % per * n
        store_row(m[got], idx, m[table][pl.ds(first + idx, 1), :])
        return (
            name,
            lambda q: m[table].at[pl.ds(first + q, 1)],
            lambda i: m[got].at[pl.ds(i, 1)],
            m[got].at[pl.ds(0, n - 1)],
        )

    def transposed(x):
        return jnp.concatenate([x, jnp.zeros((LANES - x.shape[0], LANES), F32)], axis=0).T

    def couple_set(level):
        n = nb[level + 1]
        ra, rb = m["ra", level], m["rb", level]
        idx = far % n
        rb[:, pl.ds(idx, 1), :] = ra[:, pl.ds(idx, 1), :]
        return (
            ("rb", level),
            lambda q: ra.at[:, pl.ds(q, 1)],
            lambda i: rb.at[:, pl.ds(i, 1)],
            rb.at[:, pl.ds(0, n - 1)],
        )

    arrive("la")
    m["tl"][...] = transposed(m["la"][...].reshape(NEAR * count, LANES))
    for level in (1, 2):
        arrive(("ra", level))
        sets = [forward_rows(level, "tl", ("lb", level), ("lb", level))]
        if level == 1:
            sets.append(couple_set(level))
        fan(nb[level + 1], NEAR, *sets)
    arrive("xr2")
    m["xb2"][far % ring] = jnp.sum(m["xr2"][...], axis=0)
    spread_own("xb2", ring, NEAR)
    arrive("xb1")
    m["xg1"][near] = jnp.sum(m["xb1"][...], axis=0)
    spread_own("xg1", NEAR, 1)
    spread_own("zx", four, 1)

    def build_hits(level):
        n = nb[level + 1]
        wide = 2 * LANES if level == 1 else LANES
        arrive(("lb", level))
        lb = m["lb", level][...]
        lane = lax.broadcasted_iota(jnp.int32, (n, wide), 1).astype(F32)
        at = 2 - level
        hits = [(lane == lb[:, k * count + at : k * count + at + 1]).astype(F32) for k in range(NEAR)]
        m["ohf", level][...] = jnp.concatenate(hits, axis=1).astype(BF16)
        m["ohg", level][...] = jnp.concatenate(hits, axis=0).astype(BF16)
        return hits

    def build_g(level, hits):
        n = nb[level + 1]
        arrive(("rb", level))
        half = n // 2
        for child in range(2):
            rows = slice(child * half, (child + 1) * half)
            got = m["rb", level][:, rows, :].reshape(NEAR * half, RANK)
            hot = jnp.concatenate([hit[rows] for hit in hits], axis=0).astype(BF16)
            hi, lo = [once(piece, hot, 0, 0) for piece in halves(got)]
            gh, gl = halves(hi + lo)
            out = slice(child * RANK, (child + 1) * RANK)
            m[("g", level), "h"][out, :] = gh
            m[("g", level), "l"][out, :] = gl

    def send_up(level, b, u):
        count_tiles, per = tiles_of(level)
        both = times(b, kept(("qw", level)), 0)
        tile = pick(u, m["h", level][...])
        for t in range(count_tiles):
            m["fs", level][t] = jnp.concatenate(
                [both[:, :RANK], both[:, RANK:], tile[:, t * LANES : (t + 1) * LANES]], axis=0
            )
        fs, fa = m["fs", level], m["fa", level]
        fa[near] = fs[near // per]
        fan_near(("fa", level), lambda q: fs.at[q // per], fa)

    def rows_of(level, kind, tiles):
        n = nb[level + 1]
        table = m["t" + kind, level]
        table[...] = transposed(tiles.reshape(NEAR * count, LANES))
        return table[pl.ds(pl.multiple_of(near % tiles_of(level)[1] * n, 8), n), :]

    def send_far(level, kind, first, second, rows):
        n = nb[level + 1]
        half = n // 2
        idx = far % n
        source, got = m[kind + "s", level], m[kind + "b", level]
        source[:half, :count, :] = jnp.broadcast_to(first[None], (half, count, RANK))
        source[half:, :count, :] = jnp.broadcast_to(second[None], (half, count, RANK))
        source[:, count, :] = rows
        used = pl.ds(0, count + 1)
        got[idx, : count + 1, :] = source[idx, : count + 1, :]
        fan(
            n,
            NEAR,
            (
                (kind, level),
                lambda q: source.at[q, used],
                lambda i: got.at[i, used],
                got.at[pl.ds(0, n - 1), used],
            ),
        )

    def send_on(level):
        arrive(("fa", level))
        fa = m["fa", level]
        tot = jnp.sum(fa[:, : 2 * count, :], axis=0)
        hq = tot[:count] * head[level]
        w = tot[count:] + times(hq, kept(("cross", level)), 0)
        rows = rows_of(level, "w", fa[:, 2 * count :, :])
        send_far(level, "w", w, w, rows)
        m["hb", level][far % nb[level]] = hq
        spread_own(("hb", level), nb[level], NEAR)
        return rows

    def sums_up(level):
        half = nb[level + 1] // 2
        arrive(("w", level))
        wb = m["wb", level]
        ws = [
            jnp.sum(wb[child * half : (child + 1) * half, :count, :], axis=0) * below[level][child]
            for child in range(2)
        ]
        return jnp.concatenate(ws, axis=1)

    def receive_up(level, ws):
        rows = spread(m["wb", level][:, count, :], m["ohf", level][...], NEAR, count)
        return rows - times(ws, kept(("g", level)), 0)

    def near_sum(name):
        arrive(name)
        return jnp.sum(m[name][...], axis=0)

    def send_down(level, full):
        count_tiles, per = tiles_of(level)
        sp = times(full, kept(("g", level)), 1)
        tile = pick(full, m["ohg", level][...])
        for t in range(count_tiles):
            m["bs", level][t] = jnp.concatenate(
                [sp[:, :RANK], sp[:, RANK:], tile[:, t * LANES : (t + 1) * LANES]], axis=0
            )
        bs, ba = m["bs", level], m["ba", level]
        ba[near] = bs[near // per]
        fan_near(("ba", level), lambda q: bs.at[q // per], ba)

    def send_further(level):
        arrive(("ba", level))
        ba = m["ba", level]
        tot = jnp.sum(ba[:, : 2 * count, :], axis=0)
        send_far(level, "s", tot[:count], tot[count:], rows_of(level, "s", ba[:, 2 * count :, :]))

    def receive_down(level, base):
        arrive(("s", level))
        sb = m["sb", level]
        s = jnp.sum(sb[:, :count, :], axis=0) * side[level]
        x = base - times(s, kept(("t", level)), 1)
        xu = spread(sb[:, count, :], m["ohr", level][...], NEAR, count)
        return x, xu

    saved = {}

    def solve_front(level, local):
        arrive(("hb", level))
        hq = jnp.sum(m["hb", level][...], axis=0)
        z = (local + outer(hq, exp[level][...])) * piv[level][...]
        saved[level] = z
        m["za", level][near] = mult(z, exp[level][...])
        spread_own(("za", level), NEAR, 1)

    def pass_zp(level):
        m["zb", level][far % nb[level]] = near_sum(("za", level))
        spread_own(("zb", level), nb[level], NEAR)

    def base_of(level, zp):
        return outer(saved[level], blk[level][...]) + outer(zp * head[level], q_of(level))

    def tail_of(level, wv):
        qm = q_of(level) * jnp.broadcast_to(head[level][:1], (LANES, RANK))
        keep(("t", level), wv + times(qm, kept(("cross", level)), 0))

    def wv_of(level):
        qh, ql = kept(("qw", level))
        return qh[:, RANK:].astype(F32) + ql[:, RANK:].astype(F32)

    arrive("r0")
    r0 = m["r0"][...]
    lane = lax.broadcasted_iota(jnp.int32, (plane, 2 * LANES), 1).astype(F32)
    at = cap * count
    m["oh0"][...] = jnp.concatenate(
        [(lane == r0[:, at + s : at + s + 1]).astype(F32) for s in range(cap)], axis=1
    ).astype(BF16)
    inc = spread(r0, m["oh0"][...], cap, count)
    b1 = src[1][...] + inc[:, :LANES]
    send_up(1, b1, inc[:, LANES:])
    fan(nb[3], NEAR, couple_set(2))

    local1 = mult(b1, blk[1][...])
    saved[0] = z0
    arrive("zx")
    base0 = base_of(0, jnp.sum(m["zx"][...], axis=0))
    build_g(1, build_hits(1))
    arrive("xg1")
    keep(("cross", 1), m["xg1"][...].reshape(RANK, RANK))
    hits = build_hits(2)
    kh, kl = kept(("qw", 3))
    hot = m["ohg", 2][...]
    m["kp"][...] = (once(hot, kh, 1, 0) + once(hot, kl, 1, 0)).reshape(NEAR, fars, 2 * RANK)
    scatter_near("kr", "kp")
    arrive("xb2")
    m["xy"][me // plane] = jnp.sum(m["xb2"][...], axis=0)
    spread_own("xy", total_devices // plane, plane)
    send_on(1)
    ks, kb = m["ks"], m["kb"]
    for half in range(2):
        ks[:, half] = m["kp"][:, :, half * RANK : (half + 1) * RANK]
    kb[:, :, pl.ds(far, 1), :] = ks[:, :, pl.ds(far, 1), :]
    fan(
        fars,
        NEAR,
        (
            "kb",
            lambda q: ks.at[:, :, pl.ds(q, 1)],
            lambda i: kb.at[:, :, pl.ds(i, 1)],
            kb.at[:, :, pl.ds(0, fars - 1)],
        ),
    )

    arrive("xy")
    pair = me // plane // 2 * 2
    m["xg2"][near, :slice_rows, :] = jnp.sum(m["xy"][pl.ds(pair, 2), :slice_rows, :], axis=0)
    m["xg2"][near, slice_rows:, :] = jnp.sum(m["xy"][:, slice_rows:, :], axis=0)
    spread_own("xg2", NEAR, 1)
    build_g(2, hits)
    gh, gl = kept(("g", 2))
    both = once(gh, kh, 1, 0) + (once(gl, kh, 1, 0) + once(gh, kl, 1, 0))
    m["yp"][...] = both.reshape(NEAR, 2 * RANK // NEAR, 2 * RANK)
    scatter_near("yr", "yp")
    tail_of(1, wv_of(1))

    inc = receive_up(1, sums_up(1))
    b2 = src[2][...] + inc[:, :LANES]
    send_up(2, b2, inc[:, LANES:])

    local2 = mult(b2, blk[2][...])
    arrive("xg2")
    keep(("cross", 2), m["xg2"][:, :slice_rows, :].reshape(RANK, RANK))
    rows = send_on(2)
    keep(("cross", 3), m["xg2"][:, slice_rows:, :].reshape(RANK, RANK))
    core = near // across
    per = LANES // fars
    turned = transposed(rows)
    passing = []
    for t in range(NEAR // per):
        group = [turned[(t * per + k) * count : (t * per + k + 1) * count] for k in range(per)]
        passing.append(sum(pltpu.roll(group[k], k * fars, 1) for k in range(1, per)) + group[0])
    arrive("kb")
    pulled = jnp.concatenate([kb[:, half].reshape(NEAR * fars, RANK) for half in range(2)], axis=1)
    sr = times(src[3][...], kept(("qw", 3)), 0)
    sr = sr + times(jnp.concatenate(passing, axis=1), halves(pulled), 0)
    m["sr"][near] = jnp.concatenate([sr[:, :RANK], sr[:, RANK:]], axis=0)
    spread_own("sr", NEAR, 1)
    m["yg"][near] = near_sum("yr")
    spread_own("yg", NEAR, 1)
    spread_own("c0", four, 1)
    solve_front(1, local1)
    tail_of(2, wv_of(2))

    arrive("yg")
    y = m["yg"][...].reshape(2 * RANK, 2 * RANK)
    keep("y", y)
    yq = y[:, :RANK] * jnp.broadcast_to(head[3][:1], (2 * RANK, RANK))
    yv = y[:, RANK:] + times(yq, kept(("cross", 3)), 0)
    keep("yh", jnp.where(core == 0, yq, yv))
    tot = near_sum("sr")
    sq = tot[:count] * head[3]
    mine = jnp.where(core == 0, sq, tot[count:] + times(sq, kept(("cross", 3)), 0))
    ws = sums_up(2)
    m["fb"][far] = mine - times(ws, kept("yh"), 0)
    spread_own("fb", fars, NEAR)
    b3 = src[3][...] + receive_up(2, ws)
    early = outer(mult(b3, blk[3][...]) * piv[3][...], blk[3][...])
    send_down(2, early)
    solve_front(2, local2)
    pass_zp(1)
    arrive("c0")
    keep(("cross", 0), jnp.sum(m["c0"][...], axis=0))
    tail_of(0, mult(blk[0][...], v_of(0)))
    arrive(("ba", 2))
    ba = m["ba", 2]
    sums = jnp.sum(ba[:, : 2 * count, :], axis=0)
    early_rows = rows_of(2, "s", ba[:, 2 * count :, :])
    pass_zp(2)
    arrive("kr")
    keep("ka", m["kr"][...].reshape(NEAR * fars, 2 * RANK))
    arrive("fb")
    m["fc"][core] = jnp.sum(m["fb"][...], axis=0)
    spread_own("fc", 2, across)
    arrive("fc")
    ends = jnp.concatenate([m["fc"][1] * head[3], m["fc"][0]], axis=1)
    sums = jnp.concatenate([sums[:count], sums[count:]], axis=1) + times(ends, kept("y"), 1)
    late = times(ends, kept("ka"), 1)
    late = [
        pltpu.roll(late[:, k // per * LANES : (k // per + 1) * LANES], (LANES - k % per * fars) % LANES, 1)
        for k in range(NEAR)
    ]
    late = transposed(jnp.concatenate(late, axis=0))[:fars]
    send_far(2, "s", sums[:, :RANK], sums[:, RANK:], early_rows + late)
    spread_own("hx", four, 1)
    outs[3][...] = early + times(ends, kept(("qw", 3)), 1)

    arrive(("zb", 1))
    base1 = base_of(1, jnp.sum(m["zb", 1][...], axis=0))
    arrive(("zb", 2))
    base2 = base_of(2, jnp.sum(m["zb", 2][...], axis=0))
    x, xu = receive_down(2, base2)
    send_down(1, jnp.concatenate([x, xu], axis=1))
    outs[2][...] = x
    send_further(1)
    arrive("hx")
    for k in range(four):
        at = slice(k * cap * plane, (k + 1) * cap * plane)
        packed = m["hx"][k] * jnp.broadcast_to(side[0][:1], (cap * plane, RANK))
        m["hxh"][at, :], m["hxl"][at, :] = halves(times(packed, kept(("t", 0)), 1))
    x, xu = receive_down(1, base1)
    full = diagonal(jnp.concatenate([x, xu], axis=1), cap, four)
    rows = leaf_rows((m["oh0"][...], None), full)
    ri = lax.broadcasted_iota(jnp.int32, (plane, LANES), 0)
    li = lax.broadcasted_iota(jnp.int32, (plane, LANES), 1)
    rows = jnp.where(li // (cap * count) == ri % four, rows, 0.0)
    rows = rows + pltpu.roll(rows, plane - 1, 0)
    m["s0b"][...] = rows + pltpu.roll(rows, plane - 2, 0)
    send_leaf("s0b", "r0b", lambda q: q // four * four)
    outs[1][...] = x
    for name, part in parts.items():
        wait_for(part, send_sem.at[sem_of(name)])
    arrive("r0b")
    rows = transposed(m["r0b"][...])
    pieces = [rows[g * count : (g + 1) * count] for g in range(four * cap)]
    pairs = [pieces[2 * g] + pltpu.roll(pieces[2 * g + 1], plane, 1) for g in range(four * cap // 2)]
    outs[0][...] = base0 - times(jnp.concatenate(pairs, axis=1), (m["hxh"][...], m["hxl"][...]), 0)


def solution(mesh):
    leaves, across = mesh.shape["leaf"], mesh.shape["grid"]

    def shards(*args):
        levels = [args[8 * i : 8 * i + 8] for i in range(3)]
        root = args[24:30]
        (sl, bl, el, qs, pv, cl, rk, tg) = zip(*levels)
        src = list(sl) + [root[0]]
        blk = list(bl) + [root[1]]
        exp = list(el) + [root[2]]
        bas = list(qs) + [root[3]]
        piv = [v.reshape(1, -1) for v in list(pv) + [root[4]]]
        rnk = [rk[0].T, rk[1].T, rk[2], root[5]]
        tgt = [t.reshape(1, -1) for t in tg]
        count = src[0].shape[0]
        ups = [t.shape[1] for t in tgt]
        fronts = [r.shape[0] for r in rk] + [root[5].shape[0]]
        size = [leaves * across // f for f in fronts]
        cap = ups[0] // size[1]
        nb = [s // NEAR for s in size]
        for v in src:
            assert v.shape == (NEAR, LANES)
        assert ups[1:] == [LANES, LANES] and cap * (count + 1) <= LANES
        assert 2 * size[1] == LANES and size[0] * cap * count == LANES
        assert nb[1] == 8 and across == 4 and size[0] == across
        assert size[2] == 2 * size[1] and size[3] == 2 * size[2] and size[1] % NEAR == 0
        assert NEAR * nb[2] == LANES and NEAR * nb[3] == 2 * LANES
        vm = lambda *s: pltpu.VMEM(s, F32)
        bits = lambda *s: pltpu.VMEM(s, BF16)
        piece = RANK // NEAR
        bufs = {
            "f1": vm(size[0], count, LANES),
            "fv": vm(size[0], count, LANES),
            "c0": vm(size[0], RANK, RANK),
            "zx": vm(size[0], count, LANES),
            "xp1": vm(NEAR, piece, RANK),
            "xr1": vm(NEAR, piece, RANK),
            "xp2": vm(NEAR, 2 * piece, RANK),
            "xr2": vm(NEAR, 2 * piece, RANK),
            "xb1": vm(nb[1], piece, RANK),
            "xb2": vm(nb[1], 2 * piece, RANK),
            "xy": vm(nb[3] // nb[1], 2 * piece, RANK),
            "xg1": vm(NEAR, piece, RANK),
            "xg2": vm(NEAR, 2 * piece, RANK),
            "lows": vm(2, count, LANES),
            "la": vm(NEAR, count, LANES),
            "tl": vm(LANES, LANES),
            "hch": bits(size[1], cap * RANK),
            "hcl": bits(size[1], cap * RANK),
            "low0": vm(size[1], LANES),
            "oh0": bits(size[1], cap * 2 * LANES),
            "fb": vm(nb[3], count, LANES),
            "ks": vm(NEAR, 2, nb[3], RANK),
            "kb": vm(NEAR, 2, nb[3], RANK),
            "sr": vm(NEAR, 2 * count, LANES),
            "kp": vm(NEAR, nb[3], 2 * RANK),
            "kr": vm(NEAR, nb[3], 2 * RANK),
            "yp": vm(NEAR, 2 * RANK // NEAR, 2 * RANK),
            "yr": vm(NEAR, 2 * RANK // NEAR, 2 * RANK),
            "yg": vm(NEAR, 2 * RANK // NEAR, 2 * RANK),
            "fc": vm(2, count, LANES),
            "hx": vm(size[0], cap * size[1], RANK),
            "hxh": bits(size[0] * cap * size[1], RANK),
            "hxl": bits(size[0] * cap * size[1], RANK),
        }
        for name in ("s0", "r0", "s0b", "r0b"):
            bufs[name] = vm(size[1], LANES)
        for half in "hl":
            bufs["ka", half] = bits(NEAR * nb[3], 2 * RANK)
            bufs["y", half] = bits(2 * RANK, 2 * RANK)
            bufs["yh", half] = bits(2 * RANK, RANK)
        for i in range(4):
            for half in "hl":
                bufs[("cross", i), half] = bits(RANK, RANK)
                bufs[("qw", i), half] = bits(LANES, 2 * RANK)
                bufs[("t", i), half] = bits(LANES, RANK)
                bufs["own", half] = bits(RANK, RANK)
        for i in (1, 2):
            n = nb[i + 1]
            wide = 2 * LANES if i == 1 else LANES
            tiles = NEAR * n // LANES
            bufs["h", i] = bits(NEAR * n, LANES)
            bufs["ohr", i] = bits(n, NEAR * LANES)
            bufs["ohf", i] = bits(n, NEAR * wide)
            bufs["ohg", i] = bits(NEAR * n, wide)
            bufs["pa", i] = vm(NEAR, n, RANK)
            bufs["ra", i] = vm(NEAR, n, RANK)
            bufs["rb", i] = vm(NEAR, n, RANK)
            bufs["lb", i] = vm(n, LANES)
            for half in "hl":
                bufs[("g", i), half] = bits(2 * RANK, wide)
            bufs["fs", i] = vm(tiles, 3 * count, LANES)
            bufs["fa", i] = vm(NEAR, 3 * count, LANES)
            bufs["bs", i] = vm(tiles, 3 * count, LANES)
            bufs["ba", i] = vm(NEAR, 3 * count, LANES)
            for kind in "ws":
                bufs["t" + kind, i] = vm(LANES, LANES)
                bufs[kind + "s", i] = vm(n, 2 * count, LANES)
                bufs[kind + "b", i] = vm(n, 2 * count, LANES)
            bufs["hb", i] = vm(nb[i], count, LANES)
            bufs["za", i] = vm(NEAR, count, LANES)
            bufs["zb", i] = vm(nb[i], count, LANES)
        arrays = [*src, *blk, *exp, *bas, *piv, *cl, *tgt, *rnk]
        for i, v in enumerate(arrays):
            bufs["in", i] = pltpu.VMEM(v.shape, v.dtype)
        scratch = list(bufs.values())
        scratch += [
            pltpu.SemaphoreType.DMA((56,)),
            pltpu.SemaphoreType.DMA((56,)),
            pltpu.SemaphoreType.DMA((30,)),
            pltpu.SemaphoreType.REGULAR((3,)),
        ]
        vspec = pl.BlockSpec(memory_space=pltpu.VMEM)
        whole = pl.pallas_call(
            functools.partial(kernel, (leaves, across, size, ups, count, cap), list(bufs)),
            out_shape=jax.ShapeDtypeStruct((4 * count, LANES), F32),
            in_specs=[pl.BlockSpec(memory_space=pl.ANY)] * 30,
            out_specs=vspec,
            scratch_shapes=scratch,
            compiler_params=pltpu.CompilerParams(
                collective_id=0, has_side_effects=True, vmem_limit_bytes=60 * 1024 * 1024
            ),
        )(*arrays)
        return tuple(whole[i * count : (i + 1) * count] for i in range(4))

    spread_axes = ("leaf", "grid")
    level = (P(None, spread_axes), P(spread_axes, None), P(spread_axes, None), P(spread_axes, None), P(spread_axes))
    mid = level + (P(spread_axes, None), P(), P(spread_axes))
    return jax.shard_map(
        shards,
        mesh=mesh,
        in_specs=mid * 3 + level + (P(),),
        out_specs=(P(None, spread_axes),) * 4,
        check_vma=False,
    )
```
